512 devices in a mesh: tex: 16 (over z_lo, core), smp: 32 (over z_hi, y, x).
Axes of the slice: x: 4, y: 4, z: 16 (z_hi: 2, z_lo: 8; z = z_hi * 8 + z_lo), core: 2. Of those that a mesh axis runs over, the one named last changes fastest.
Arguments:
- blocks: int32 [16, 32, 2, 2], P('tex', 'smp'), may hold values from -1 to 3, as said below
- observed: float32 [16, 32, 512, 256], P('tex', 'smp'), may hold values from 0.05 to 1.5
- w_factor: float32 [64, 16384], P('smp', 'tex'), may hold values from 0.03 to 0.5
- h_factor: float32 [64, 32768], P('tex', 'smp'), may hold values from 0.03 to 0.5
Outputs:
- w_final: float32 [64, 16384], P('smp', 'tex')
- h_final: float32 [64, 32768], P('tex', 'smp')
The draws below stay inside these ranges and needn't reach their ends.
Inputs may be any that keep to these rules, and one draw needn't show every extreme that they name: blocks[t, s, 0, j] is a block row (below 4) and blocks[t, s, 1, j] a block column (below 4) of device (t, s)'s tile, or both are -1 for an empty slot; live slots come first and name different blocks; each device has at least one live slot and some device has 2; every block row of texels is observed on some device along smp, and every block column of samples on some device along tex.
All inputs are finite; a program needn't handle non-finite values.
Results may differ from the reference program's by a relative error of at most 0.0003.
Values sent between devices are 32-bit elements; how exact they have to be, the bound alone decides.
No kernel may reach another device: no remote copies, remote signals or barrier semaphores. Data moves between devices by JAX's collectives and lax.ppermute only.
A program may use at most 64 MiB of HBM per device.

```python
import math
import jax
import jax.numpy as jnp
from jax import lax

K = 64
BS = 256
RB = 4
CB = 4
CAP = 2
ITERS = 2
M = 16384
N = 32768
N_TEX = 16
N_SMP = 32


def draw_blocks(key, part):
    key_count = jax.random.fold_in(key, 11)
    key_score = jax.random.fold_in(key, 12)
    key_full = jax.random.fold_in(key, 13)
    devices_all = N_TEX * N_SMP
    tile_blocks = RB * CB
    counts = jax.random.randint(key_count, (N_TEX, N_SMP), max(1, CAP // 4), CAP + 1)
    full_at = jax.random.randint(key_full, (), 0, devices_all)
    counts = jnp.where(jnp.arange(devices_all).reshape(N_TEX, N_SMP) == full_at, CAP, counts)
    scores = jax.random.randint(key_score, (N_TEX, N_SMP, tile_blocks), 0, 1 << 20) * tile_blocks + jnp.arange(tile_blocks)
    texels = jnp.arange(N_TEX)[:, None]
    samples = jnp.arange(N_SMP)[None, :]
    forced = samples % RB * CB + texels % CB
    scores = jnp.where(jnp.arange(tile_blocks)[None, None, :] == forced[:, :, None], -1, scores)
    chosen = jnp.argsort(scores, axis=-1)[:, :, :CAP].astype(jnp.int32)
    live = jnp.arange(CAP)[None, None, :] < counts[:, :, None]
    rows = jnp.where(live, chosen // CB, -1)
    cols = jnp.where(live, chosen % CB, -1)
    return jnp.stack([rows, cols], axis=2).astype(jnp.int32)


def level_of(own_key, extent, pieces, low, largest):
    def one(position, parts):
        steps = jax.random.uniform(jax.random.fold_in(jax.random.fold_in(own_key, 6), position), (parts,), jnp.float32, low / len(pieces), largest / len(pieces))
        return jnp.repeat(jnp.exp(steps), extent[position] // parts).reshape((-1,) + (1,) * (len(extent) - position - 1))

    factor_of = one(*pieces[0])
    for cut in pieces[1:]:
        factor_of = factor_of * one(*cut)
    return factor_of


def setup_inputs(seed: int = 0) -> dict:
    key_list = jax.random.split(jax.random.key(seed), 5)
    blocks = draw_blocks(jax.random.fold_in(key_list[4], 71), 0)
    observed = jnp.clip(0.05 + 1.45 * jax.random.uniform(key_list[1], (N_TEX, N_SMP, CAP * BS, BS), jnp.float32) ** level_of(key_list[1], (N_TEX, N_SMP, CAP * BS, BS), ((0, 16), (1, 32)), -0.2, 0.2), 0.05, 1.5)
    w_factor = jnp.clip(jnp.exp(math.log(0.5) - 2.8134107 * jax.random.uniform(key_list[2], (K, M), jnp.float32) ** level_of(key_list[2], (K, M), ((0, 32), (1, 16)), -0.2, 0.2)), 0.03, 0.5)
    h_factor = jnp.clip(jnp.exp(math.log(0.5) - 2.8134107 * jax.random.uniform(key_list[3], (K, N), jnp.float32) ** level_of(key_list[3], (K, N), ((0, 16), (1, 32)), -0.2, 0.2)), 0.03, 0.5)
    return dict(blocks=blocks, observed=observed, w_factor=w_factor, h_factor=h_factor)


highest = lax.Precision.HIGHEST


def pick_tables(listing, rows_count, cols_count):
    rows = listing[0]
    cols = listing[1]
    live = (rows >= 0).astype(jnp.float32)
    row_pick = (jnp.maximum(rows, 0)[:, None] == jnp.arange(rows_count)[None, :]).astype(jnp.float32) * live[:, None]
    col_pick = (jnp.maximum(cols, 0)[:, None] == jnp.arange(cols_count)[None, :]).astype(jnp.float32)
    return row_pick, col_pick


def block_factors(w_tile, h_tile, row_pick, col_pick):
    rank = w_tile.shape[0]
    w_blocks = jnp.einsum('sr,krb->skb', row_pick, w_tile.reshape(rank, row_pick.shape[1], -1), precision=highest)
    h_blocks = jnp.einsum('sc,kcb->skb', col_pick, h_tile.reshape(rank, col_pick.shape[1], -1), precision=highest)
    approx = jnp.einsum('ska,skb->sab', w_blocks, h_blocks, precision=highest)
    return w_blocks, h_blocks, approx


def basis_terms(w_tile, h_tile, row_pick, col_pick, values):
    w_blocks, h_blocks, approx = block_factors(w_tile, h_tile, row_pick, col_pick)
    upper = jnp.einsum('ska,sab->skb', w_blocks, values, precision=highest)
    lower = jnp.einsum('ska,sab->skb', w_blocks, approx, precision=highest)
    upper = jnp.einsum('sc,skb->kcb', col_pick, upper, precision=highest)
    lower = jnp.einsum('sc,skb->kcb', col_pick, lower, precision=highest)
    return upper.reshape(h_tile.shape), lower.reshape(h_tile.shape)


def weight_terms(w_tile, h_tile, row_pick, col_pick, values):
    w_blocks, h_blocks, approx = block_factors(w_tile, h_tile, row_pick, col_pick)
    upper = jnp.einsum('skb,sab->ska', h_blocks, values, precision=highest)
    lower = jnp.einsum('skb,sab->ska', h_blocks, approx, precision=highest)
    upper = jnp.einsum('sr,ska->kra', row_pick, upper, precision=highest)
    lower = jnp.einsum('sr,ska->kra', row_pick, lower, precision=highest)
    return upper.reshape(w_tile.shape), lower.reshape(w_tile.shape)


def reference(blocks, observed, w_factor, h_factor):
    tiles_w = jnp.moveaxis(w_factor.reshape(K, N_TEX, RB * BS), 1, 0)
    tiles_h = jnp.moveaxis(h_factor.reshape(K, N_SMP, CB * BS), 1, 0)
    values_all = observed.reshape(N_TEX, N_SMP, CAP, BS, BS)
    for sweep in range(ITERS):
        def over_tex(carry, inputs):
            w_tile, listing_row, value_row = inputs

            def per_sample(items):
                h_tile, listing, values = items
                row_pick, col_pick = pick_tables(listing, RB, CB)
                return basis_terms(w_tile, h_tile, row_pick, col_pick, values)

            upper, lower = lax.map(per_sample, (tiles_h, listing_row, value_row))
            return (carry[0] + upper, carry[1] + lower), None

        start = jnp.zeros(tiles_h.shape, jnp.float32)
        (upper, lower), _ = lax.scan(over_tex, (start, start), (tiles_w, blocks, values_all))
        tiles_h = tiles_h * upper / lower

        def texel_sums(inputs):
            w_tile, listing_row, value_row = inputs

            def per_sample(items):
                h_tile, listing, values = items
                row_pick, col_pick = pick_tables(listing, RB, CB)
                return weight_terms(w_tile, h_tile, row_pick, col_pick, values)

            upper, lower = lax.map(per_sample, (tiles_h, listing_row, value_row))
            return jnp.sum(upper, axis=0), jnp.sum(lower, axis=0)

        upper, lower = lax.map(texel_sums, (tiles_w, blocks, values_all))
        tiles_w = tiles_w * upper / lower
    w_final = jnp.moveaxis(tiles_w, 0, 1).reshape(K, N_TEX * RB * BS)
    h_final = jnp.moveaxis(tiles_h, 0, 1).reshape(K, N_SMP * CB * BS)
    return w_final, h_final
```

```python
import jax
import jax.numpy as jnp
from jax import lax
from jax.experimental import pallas as pl
from jax.experimental.pallas import tpu as pltpu
from jax.sharding import Mesh, PartitionSpec as P

RANK = 64
BS = 256
CAP = 2
NB = 4
TAB = 128

FINE = ("z4", "z2", "z1", "core", "zh", "y", "x")
HALF = ("z2", "z1", "core")
PLANE = ("y", "x")
TEX = HALF + ("z4",)
SMP = PLANE + ("zh",)
NH = 8
NP = 16

NN = (((1,), (0,)), ((), ()))
NT = (((1,), (1,)), ((), ()))


def exchange(x, axes):
    return lax.all_to_all(x, axes, split_axis=0, concat_axis=0, tiled=True)


def swap(x, axis):
    return lax.ppermute(x, axis, [(0, 1), (1, 0)])


def halves(x):
    hi = x.astype(jnp.bfloat16)
    lo = (x - hi.astype(jnp.float32)).astype(jnp.bfloat16)
    return hi, lo


def product(a, b, dims):
    dot = lambda x, y: lax.dot_general(x, y, dims, preferred_element_type=jnp.float32)
    return dot(a[0], b[0]) + (dot(a[0], b[1]) + dot(a[1], b[0]))


def sums(left, right, values, dims, live):
    whole = halves(left)
    left = halves(left * live)
    upper = product(left, halves(values), dims)
    gram = product(left, whole, NT)
    lower = product(halves(gram), halves(right), NN)
    return upper, lower


def live_of(blk, j):
    return jnp.where(blk[0, j] >= 0, 1.0, 0.0).astype(jnp.float32)


def block_of(blk, d, j):
    return jnp.maximum(blk[d, j], 0)


def send_h(out, j, upper, lower):
    for q in range(NH):
        out[q, 16 * j : 16 * j + 8, :] = upper[8 * q : 8 * q + 8, :]
        out[q, 16 * j + 8 : 16 * j + 16, :] = lower[8 * q : 8 * q + 8, :]


def first_kernel(blk, pos, w0, h0, values, w_slots, h_own, w_own, out):
    for j in range(CAP):
        at = pl.multiple_of(block_of(blk, 0, j) * BS, BS)
        for q in range(2 * NP):
            w_slots[j, 2 * q : 2 * q + 2, :] = w0[q, :, pl.ds(at, BS)]
        at = pl.multiple_of(block_of(blk, 1, j) * BS, BS)
        rows = []
        for q in range(NH):
            for high in range(2):
                for z in range(2):
                    rows.append(h0[2 * q + z, 2 * high : 2 * high + 2, pl.ds(at, BS)])
        upper, lower = sums(
            w_slots[j], jnp.concatenate(rows, axis=0), values[j * BS : (j + 1) * BS, :], NN, live_of(blk, j)
        )
        send_h(out, j, upper, lower)
    for b in range(NB):
        for z in range(2):
            w_own[b, 2 * z : 2 * z + 2, :] = w0[2 * pos[1] + z, :, b * BS : (b + 1) * BS]
            for high in range(2):
                h_own[b, 4 * high + 2 * z : 4 * high + 2 * z + 2, :] = h0[
                    2 * pos[0] + z, 2 * high : 2 * high + 2, b * BS : (b + 1) * BS
                ]


def h_slot(got, j):
    return got[:, 8 * j : 8 * j + 8, :].reshape(RANK, BS)


def w_slot(got, j):
    return jnp.concatenate([got[q, 4 * j : 4 * j + 4, :] for q in range(NP)], axis=0)


def w_terms_kernel(blk, h_got, w_slots, values, out):
    share = out.shape[1] // (2 * CAP)
    for j in range(CAP):
        upper, lower = sums(h_slot(h_got, j), w_slots[j], values[j * BS : (j + 1) * BS, :], NT, live_of(blk, j))
        for q in range(out.shape[0]):
            at = 2 * share * j
            out[q, at : at + share, :] = upper[share * q : share * (q + 1), :]
            out[q, at + share : at + 2 * share, :] = lower[share * q : share * (q + 1), :]


def h_terms_kernel(blk, w_got, h_got, values, w_slots, out):
    for j in range(CAP):
        w_slots[j] = w_slot(w_got, j)
        upper, lower = sums(w_slots[j], h_slot(h_got, j), values[j * BS : (j + 1) * BS, :], NN, live_of(blk, j))
        send_h(out, j, upper, lower)


def peer_block(table, pos, which, q, j):
    return jnp.maximum(table[(2 * q + pos[which]) * CAP + j], 0)


def collect_kernel(which, table, pos, got, out):
    rows = out.shape[1]
    out[...] = jnp.zeros(out.shape, out.dtype)
    for q in range(got.shape[0]):
        for j in range(CAP):
            b = peer_block(table, pos, which, q, j)
            out[b] = out[b] + got[q, rows * j : rows * (j + 1), :]


def updated(own, mine, theirs):
    rows = own.shape[1]
    upper = mine[:, :rows, :] + theirs[:, :rows, :]
    lower = mine[:, rows:, :] + theirs[:, rows:, :]
    return own[...] * upper / lower


def update_kernel(which, table, pos, own, mine, theirs, new, out):
    rows = own.shape[1]
    new[...] = updated(own, mine, theirs)
    for q in range(out.shape[0]):
        for j in range(CAP):
            out[q, rows * j : rows * (j + 1), :] = new[peer_block(table, pos, which, q, j)]


def last_kernel(table, pos, own, got, out, acc):
    acc[...] = jnp.zeros(acc.shape, acc.dtype)
    for q in range(2 * NP):
        for j in range(CAP):
            b = jnp.maximum(table[q * CAP + j], 0)
            acc[b] = acc[b] + got[q, 4 * j : 4 * j + 4, :]
    z = pos[3]
    for b in range(NB):
        mine = jnp.where(z == 0, own[b, 0:2, :], own[b, 2:4, :])
        out[:, b * BS : (b + 1) * BS] = mine * acc[b, 0:2, :] / acc[b, 2:4, :]


def call(body, scalars, arrays, outs, scratch=(), name=None):
    smem = pl.BlockSpec(memory_space=pltpu.SMEM)
    vmem = pl.BlockSpec(memory_space=pltpu.VMEM)
    shapes = [jax.ShapeDtypeStruct(s, jnp.float32) for s in outs]
    return pl.pallas_call(
        body,
        in_specs=[smem] * len(scalars) + [vmem] * len(arrays),
        out_specs=[vmem] * len(outs),
        out_shape=shapes,
        scratch_shapes=[pltpu.VMEM(s, jnp.float32) for s in scratch],
        name=name,
    )(*scalars, *arrays)


def with_list(factor, listing, copies):
    listed = jnp.zeros((factor.shape[0], TAB), jnp.float32)
    listed = listed.at[:, :CAP].set(listing.astype(jnp.float32)[None, :])
    message = jnp.concatenate([factor, listed], axis=1)
    return jnp.broadcast_to(message, (copies, *message.shape))


def table_of(got):
    return got[:, 0, NB * BS : NB * BS + CAP].astype(jnp.int32).reshape(-1)


def per_device(blocks, observed, w_factor, h_factor):
    blk = blocks[0, 0]
    values = observed[0, 0]
    half = lax.axis_index(HALF)
    plane = lax.axis_index(PLANE)
    pos = jnp.stack([half, plane, lax.axis_index("z4"), lax.axis_index("zh")]).astype(jnp.int32)

    h_got0 = exchange(with_list(h_factor, blk[1], 2 * NH), TEX)
    w_got0 = exchange(with_list(w_factor, blk[0], 2 * NP), SMP)
    cols = table_of(h_got0)
    rows = table_of(w_got0)

    def h_round(sent, own, name):
        got = exchange(sent, HALF)
        (mine,) = call(lambda *r: collect_kernel(2, *r), (cols, pos), (got,), [(NB, 16, BS)], name=name + "_collect")
        theirs = swap(mine, "z4")
        own, out = call(
            lambda *r: update_kernel(2, *r),
            (cols, pos),
            (own, mine, theirs),
            [(NB, 8, BS), (NH, 16, BS)],
            name=name + "_update",
        )
        return own, exchange(out, HALF)

    w_slots, h_own, w_own, sent = call(
        first_kernel,
        (blk, pos),
        (w_got0, h_got0, values),
        [(CAP, RANK, BS), (NB, 8, BS), (NB, 4, BS), (NH, 32, BS)],
        name="h1_terms",
    )
    h_own, h_got = h_round(sent, h_own, "h1")

    (sent,) = call(w_terms_kernel, (blk,), (h_got, w_slots, values), [(NP, 16, BS)], name="w1_terms")
    got = exchange(sent, PLANE)
    (mine,) = call(lambda *r: collect_kernel(3, *r), (rows, pos), (got,), [(NB, 8, BS)], name="w1_collect")
    theirs = swap(mine, "zh")
    w_own, out = call(
        lambda *r: update_kernel(3, *r),
        (rows, pos),
        (w_own, mine, theirs),
        [(NB, 4, BS), (NP, 8, BS)],
        name="w1_update",
    )
    w_got = exchange(out, PLANE)

    w_slots, sent = call(
        h_terms_kernel,
        (blk,),
        (w_got, h_got, values),
        [(CAP, RANK, BS), (NH, 32, BS)],
        name="h2_terms",
    )
    h_own, h_got = h_round(sent, h_own, "h2")

    (sent,) = call(w_terms_kernel, (blk,), (h_got, w_slots, values), [(2 * NP, 8, BS)], name="w2_terms")
    got = exchange(sent, SMP)
    (w_final,) = call(
        last_kernel, (rows, pos), (w_own, got), [(2, NB * BS)], scratch=[(NB, 4, BS)], name="w2_update"
    )
    z = lax.axis_index("z4")
    h_rows = h_own.reshape(NB, 2, 2, 2, BS)
    h_rows = lax.dynamic_index_in_dim(h_rows, z, axis=2, keepdims=False)
    h_final = jnp.moveaxis(h_rows.reshape(NB, 4, BS), 0, 1).reshape(4, NB * BS)
    return w_final, h_final


def solution(mesh):
    fine = Mesh(mesh.devices.reshape(2, 2, 2, 2, 2, 4, 4), FINE)
    tex = ("z4",) + HALF
    smp = ("zh",) + PLANE
    in_specs = (P(tex, smp, None, None), P(tex, smp, None, None), P(smp, tex), P(tex, smp))
    out_specs = (P(smp, tex), P(tex, smp))
    return jax.shard_map(per_device, mesh=fine, in_specs=in_specs, out_specs=out_specs, check_vma=False)
```

```python
import jax
import jax.numpy as jnp
from jax import lax
from jax.experimental import pallas as pl
from jax.experimental.pallas import tpu as pltpu
from jax.sharding import Mesh, PartitionSpec as P

RANK = 64
BS = 256
CAP = 2
NB = 4
TAB = 128

FINE = ("z4", "z2", "z1", "core", "zh", "y", "x")
HALF = ("z2", "z1", "core")
PLANE = ("y", "x")
SMP = PLANE + ("zh",)
NH = 8
NP = 16

NN = (((1,), (0,)), ((), ()))
NT = (((1,), (1,)), ((), ()))


def exchange(x, axes):
    return lax.all_to_all(x, axes, split_axis=0, concat_axis=0, tiled=True)


def swap(x, axis):
    return lax.ppermute(x, axis, [(0, 1), (1, 0)])


def halves(x):
    hi = x.astype(jnp.bfloat16)
    lo = (x - hi.astype(jnp.float32)).astype(jnp.bfloat16)
    return hi, lo


def product(a, b, dims):
    dot = lambda x, y: lax.dot_general(x, y, dims, preferred_element_type=jnp.float32)
    return dot(a[0], b[0]) + (dot(a[0], b[1]) + dot(a[1], b[0]))


def sums(left, right, values, dims, live):
    whole = halves(left)
    left = halves(left * live)
    upper = product(left, halves(values), dims)
    gram = product(left, whole, NT)
    lower = product(halves(gram), halves(right), NN)
    return upper, lower


def live_of(blk, j):
    return jnp.where(blk[0, j] >= 0, 1.0, 0.0).astype(jnp.float32)


def block_of(blk, d, j):
    return jnp.maximum(blk[d, j], 0)


def send_h(out, j, upper, lower):
    for q in range(NH):
        out[q, 16 * j : 16 * j + 8, :] = upper[8 * q : 8 * q + 8, :]
        out[q, 16 * j + 8 : 16 * j + 16, :] = lower[8 * q : 8 * q + 8, :]


def pack_kernel(blk, w, h, w_msg, h_msg):
    for d, factor, message in ((0, w, w_msg), (1, h, h_msg)):
        rows = factor.shape[0]
        message[:, : NB * BS] = factor[...]
        lane = lax.broadcasted_iota(jnp.int32, (rows, TAB), 1)
        message[:, NB * BS :] = jnp.where(lane == 0, blk[d, 0], blk[d, 1]).astype(jnp.float32)


def w_pair_kernel(pos, mine, theirs, out):
    first = pos[3] == 0
    both = jnp.concatenate(
        [jnp.where(first, mine[...], theirs[...]), jnp.where(first, theirs[...], mine[...])], axis=0
    )
    for q in range(NP):
        out[q] = both


def h_pair_kernel(pos, mine, theirs, out):
    first = pos[2] == 0
    low = jnp.where(first, mine[...], theirs[...])
    high = jnp.where(first, theirs[...], mine[...])
    both = jnp.concatenate([low[0:2], high[0:2], low[2:4], high[2:4]], axis=0)
    for q in range(NH):
        out[q] = both


def first_kernel(blk, pos, w0, h0, values, w_slots, h_own, w_own, out):
    for j in range(CAP):
        at = pl.multiple_of(block_of(blk, 0, j) * BS, BS)
        for q in range(NP):
            w_slots[j, 4 * q : 4 * q + 4, :] = w0[q, :, pl.ds(at, BS)]
        at = pl.multiple_of(block_of(blk, 1, j) * BS, BS)
        right = h0[:, :, pl.ds(at, BS)].reshape(RANK, BS)
        upper, lower = sums(w_slots[j], right, values[j * BS : (j + 1) * BS, :], NN, live_of(blk, j))
        send_h(out, j, upper, lower)
    for b in range(NB):
        w_own[b] = w0[pos[1], :, b * BS : (b + 1) * BS]
        h_own[b] = h0[pos[0], :, b * BS : (b + 1) * BS]


def h_slot(got, j):
    return got[:, 8 * j : 8 * j + 8, :].reshape(RANK, BS)


def w_slot(got, j):
    return jnp.concatenate([got[q, 4 * j : 4 * j + 4, :] for q in range(NP)], axis=0)


def w_terms_kernel(blk, h_got, w_slots, values, out):
    share = out.shape[1] // (2 * CAP)
    for j in range(CAP):
        upper, lower = sums(h_slot(h_got, j), w_slots[j], values[j * BS : (j + 1) * BS, :], NT, live_of(blk, j))
        for q in range(out.shape[0]):
            at = 2 * share * j
            out[q, at : at + share, :] = upper[share * q : share * (q + 1), :]
            out[q, at + share : at + 2 * share, :] = lower[share * q : share * (q + 1), :]


def h_terms_kernel(blk, w_got, h_got, values, w_slots, out):
    for j in range(CAP):
        w_slots[j] = w_slot(w_got, j)
        upper, lower = sums(w_slots[j], h_slot(h_got, j), values[j * BS : (j + 1) * BS, :], NN, live_of(blk, j))
        send_h(out, j, upper, lower)


def peer_block(table, pos, which, q, j):
    return jnp.maximum(table[(2 * q + pos[which]) * CAP + j], 0)


def collect_kernel(which, table, pos, got, out):
    rows = out.shape[1]
    out[...] = jnp.zeros(out.shape, out.dtype)
    for q in range(got.shape[0]):
        for j in range(CAP):
            b = peer_block(table, pos, which, q, j)
            out[b] = out[b] + got[q, rows * j : rows * (j + 1), :]


def updated(own, mine, theirs):
    rows = own.shape[1]
    upper = mine[:, :rows, :] + theirs[:, :rows, :]
    lower = mine[:, rows:, :] + theirs[:, rows:, :]
    return own[...] * upper / lower


def update_kernel(which, table, pos, own, mine, theirs, new, out):
    rows = own.shape[1]
    new[...] = updated(own, mine, theirs)
    for q in range(out.shape[0]):
        for j in range(CAP):
            out[q, rows * j : rows * (j + 1), :] = new[peer_block(table, pos, which, q, j)]


def last_kernel(table, pos, own, got, out, acc):
    acc[...] = jnp.zeros(acc.shape, acc.dtype)
    for q in range(2 * NP):
        for j in range(CAP):
            b = jnp.maximum(table[q * CAP + j], 0)
            acc[b] = acc[b] + got[q, 4 * j : 4 * j + 4, :]
    z = pos[3]
    for b in range(NB):
        mine = jnp.where(z == 0, own[b, 0:2, :], own[b, 2:4, :])
        out[:, b * BS : (b + 1) * BS] = mine * acc[b, 0:2, :] / acc[b, 2:4, :]


def call(body, scalars, arrays, outs, scratch=(), last=False, name=None):
    smem = pl.BlockSpec(memory_space=pltpu.SMEM)
    vmem = pl.BlockSpec(memory_space=pltpu.VMEM)
    kind = jax.ShapeDtypeStruct if last else pltpu.VMEM
    return pl.pallas_call(
        body,
        in_specs=[smem] * len(scalars) + [vmem] * len(arrays),
        out_specs=[vmem] * len(outs),
        out_shape=[kind(s, jnp.float32) for s in outs],
        scratch_shapes=[pltpu.VMEM(s, jnp.float32) for s in scratch],
        name=name,
    )(*scalars, *(pltpu.with_memory_space_constraint(a, pltpu.VMEM) for a in arrays))


def table_of(got):
    return got[:, 0:4:2, NB * BS : NB * BS + CAP].astype(jnp.int32).reshape(-1)


def per_device(blocks, observed, w_factor, h_factor):
    blk = blocks[0, 0]
    values = observed[0, 0]
    half = lax.axis_index(HALF)
    plane = lax.axis_index(PLANE)
    pos = jnp.stack([half, plane, lax.axis_index("z4"), lax.axis_index("zh")]).astype(jnp.int32)

    w_msg, h_msg = call(
        pack_kernel, (blk,), (w_factor, h_factor), [(2, NB * BS + TAB), (4, NB * BS + TAB)], name="pack"
    )
    w_other = swap(w_msg, "zh")
    h_other = swap(h_msg, "z4")
    (h_pair,) = call(h_pair_kernel, (pos,), (h_msg, h_other), [(NH, 8, NB * BS + TAB)], name="h_pair")
    h_got0 = exchange(h_pair, HALF)
    (w_pair,) = call(w_pair_kernel, (pos,), (w_msg, w_other), [(NP, 4, NB * BS + TAB)], name="w_pair")
    w_got0 = exchange(w_pair, PLANE)
    cols = table_of(h_got0)
    rows = table_of(w_got0)

    def h_round(sent, own, name):
        got = exchange(sent, HALF)
        (mine,) = call(lambda *r: collect_kernel(2, *r), (cols, pos), (got,), [(NB, 16, BS)], name=name + "_collect")
        theirs = swap(mine, "z4")
        own, out = call(
            lambda *r: update_kernel(2, *r),
            (cols, pos),
            (own, mine, theirs),
            [(NB, 8, BS), (NH, 16, BS)],
            name=name + "_update",
        )
        return own, exchange(out, HALF)

    w_slots, h_own, w_own, sent = call(
        first_kernel,
        (blk, pos),
        (w_got0, h_got0, values),
        [(CAP, RANK, BS), (NB, 8, BS), (NB, 4, BS), (NH, 32, BS)],
        name="h1_terms",
    )
    h_own, h_got = h_round(sent, h_own, "h1")

    (sent,) = call(w_terms_kernel, (blk,), (h_got, w_slots, values), [(NP, 16, BS)], name="w1_terms")
    got = exchange(sent, PLANE)
    (mine,) = call(lambda *r: collect_kernel(3, *r), (rows, pos), (got,), [(NB, 8, BS)], name="w1_collect")
    theirs = swap(mine, "zh")
    w_own, out = call(
        lambda *r: update_kernel(3, *r),
        (rows, pos),
        (w_own, mine, theirs),
        [(NB, 4, BS), (NP, 8, BS)],
        name="w1_update",
    )
    w_got = exchange(out, PLANE)

    w_slots, sent = call(
        h_terms_kernel,
        (blk,),
        (w_got, h_got, values),
        [(CAP, RANK, BS), (NH, 32, BS)],
        name="h2_terms",
    )
    h_own, h_got = h_round(sent, h_own, "h2")

    (sent,) = call(w_terms_kernel, (blk,), (h_got, w_slots, values), [(2 * NP, 8, BS)], name="w2_terms")
    got = exchange(sent, SMP)
    (w_final,) = call(
        last_kernel, (rows, pos), (w_own, got), [(2, NB * BS)], scratch=[(NB, 4, BS)], last=True, name="w2_update"
    )
    z = lax.axis_index("z4")
    h_rows = h_own.reshape(NB, 2, 2, 2, BS)
    h_rows = lax.dynamic_index_in_dim(h_rows, z, axis=2, keepdims=False)
    h_final = jnp.moveaxis(h_rows.reshape(NB, 4, BS), 0, 1).reshape(4, NB * BS)
    return w_final, h_final


def solution(mesh):
    fine = Mesh(mesh.devices.reshape(2, 2, 2, 2, 2, 4, 4), FINE)
    tex = ("z4",) + HALF
    smp = ("zh",) + PLANE
    in_specs = (P(tex, smp, None, None), P(tex, smp, None, None), P(smp, tex), P(tex, smp))
    out_specs = (P(smp, tex), P(tex, smp))
    return jax.shard_map(per_device, mesh=fine, in_specs=in_specs, out_specs=out_specs, check_vma=False)
```

```python
import jax
import jax.numpy as jnp
from jax import lax
from jax.experimental import pallas as pl
from jax.experimental.pallas import tpu as pltpu
from jax.sharding import Mesh, PartitionSpec as P


RANK = 64
BS = 256
CAP = 2
NB = 4
TAB = 128

FINE = ("z4", "z2", "z1", "core", "zh", "y", "x")
HALF = ("z2", "z1", "core")
PLANE = ("y", "x")
NH = 8
NP = 16

NN = (((1,), (0,)), ((), ()))
NT = (((1,), (1,)), ((), ()))


def exchange(x, axes):
    return lax.all_to_all(x, axes, split_axis=0, concat_axis=0, tiled=True)


def swap(x, axis):
    return lax.ppermute(x, axis, [(0, 1), (1, 0)])


def halves(x):
    hi = x.astype(jnp.bfloat16)
    lo = (x - hi.astype(jnp.float32)).astype(jnp.bfloat16)
    return hi, lo


def product(a, b, dims):
    dot = lambda x, y: lax.dot_general(x, y, dims, preferred_element_type=jnp.float32)
    return dot(a[0], b[0]) + (dot(a[0], b[1]) + dot(a[1], b[0]))


def sums(left, right, values, dims, live):
    whole = halves(left)
    left = halves(left * live)
    upper = product(left, halves(values), dims)
    gram = product(left, whole, NT)
    lower = product(halves(gram), halves(right), NN)
    return upper, lower


def live_of(blk, j):
    return jnp.where(blk[0, j] >= 0, 1.0, 0.0).astype(jnp.float32)


def block_of(blk, d, j):
    return jnp.maximum(blk[d, j], 0)


def send_h(out, j, upper, lower):
    for q in range(NH):
        out[q, 16 * j : 16 * j + 8, :] = upper[8 * q : 8 * q + 8, :]
        out[q, 16 * j + 8 : 16 * j + 16, :] = lower[8 * q : 8 * q + 8, :]


def with_list(rows, blk, d, lists):
    lane = lax.broadcasted_iota(jnp.int32, (rows.shape[0], TAB), 1)
    lists[:, : NB * BS] = rows
    lists[:, NB * BS :] = jnp.where(lane == 0, blk[d, 0], blk[d, 1]).astype(jnp.float32)


def w_pair_kernel(blk, mine, theirs, out, message):
    first = lax.axis_index("zh") == 0
    low = jnp.where(first, mine[...], theirs[...])
    high = jnp.where(first, theirs[...], mine[...])
    with_list(jnp.concatenate([low, high], axis=0), blk, 0, message)
    for q in range(NP):
        out[q] = message[...]


def h_pair_kernel(blk, mine, theirs, out, message):
    first = lax.axis_index("z4") == 0
    low = jnp.where(first, mine[...], theirs[...])
    high = jnp.where(first, theirs[...], mine[...])
    with_list(jnp.concatenate([low[0:2], high[0:2], low[2:4], high[2:4]], axis=0), blk, 1, message)
    for q in range(NH):
        out[q] = message[...]


def first_kernel(blk, w0, h0, values, w_slots, h_own, w_own, out, rows, cols):
    for j in range(CAP):
        at = pl.multiple_of(block_of(blk, 0, j) * BS, BS)
        for q in range(NP):
            w_slots[j, 4 * q : 4 * q + 4, :] = w0[q, :, pl.ds(at, BS)]
        at = pl.multiple_of(block_of(blk, 1, j) * BS, BS)
        right = h0[:, :, pl.ds(at, BS)].reshape(RANK, BS)
        upper, lower = sums(w_slots[j], right, values[j * BS : (j + 1) * BS, :], NN, live_of(blk, j))
        send_h(out, j, upper, lower)
    half = lax.axis_index(HALF)
    plane = lax.axis_index(PLANE)
    for b in range(NB):
        w_own[b] = w0[plane, :, b * BS : (b + 1) * BS]
        h_own[b] = h0[half, :, b * BS : (b + 1) * BS]
    for got, table in ((w0, rows), (h0, cols)):
        for q in range(got.shape[0]):
            for j in range(CAP):
                at = NB * BS + j
                table[q * CAP + j] = jnp.maximum(got[q, 0:1, at : at + 1].astype(jnp.int32)[0, 0], 0)


def h_slot(got, j):
    return got[:, 8 * j : 8 * j + 8, :].reshape(RANK, BS)


def w_slot(got, j):
    return jnp.concatenate([got[q, 4 * j : 4 * j + 4, :] for q in range(NP)], axis=0)


def w_terms_kernel(blk, h_got, w_slots, values, out):
    share = out.shape[1] // (2 * CAP)
    for j in range(CAP):
        upper, lower = sums(h_slot(h_got, j), w_slots[j], values[j * BS : (j + 1) * BS, :], NT, live_of(blk, j))
        for q in range(out.shape[0]):
            at = 2 * share * j
            out[q, at : at + share, :] = upper[share * q : share * (q + 1), :]
            out[q, at + share : at + 2 * share, :] = lower[share * q : share * (q + 1), :]


def h_terms_kernel(blk, w_got, h_got, values, w_slots, out):
    for j in range(CAP):
        w_slots[j] = w_slot(w_got, j)
        upper, lower = sums(w_slots[j], h_slot(h_got, j), values[j * BS : (j + 1) * BS, :], NN, live_of(blk, j))
        send_h(out, j, upper, lower)


def collect_kernel(table, got, out):
    rows = out.shape[1]
    out[...] = jnp.zeros(out.shape, out.dtype)
    for q in range(got.shape[0]):
        for j in range(CAP):
            b = table[q * CAP + j]
            out[b] = out[b] + got[q, rows * j : rows * (j + 1), :]


def updated(own, mine, theirs):
    rows = own.shape[1]
    upper = mine[:, :rows, :] + theirs[:, :rows, :]
    lower = mine[:, rows:, :] + theirs[:, rows:, :]
    return own[...] * upper / lower


def update_kernel(table, own, mine, theirs, new, out):
    rows = own.shape[1]
    new[...] = updated(own, mine, theirs)
    for q in range(out.shape[0]):
        for j in range(CAP):
            out[q, rows * j : rows * (j + 1), :] = new[table[q * CAP + j]]


def last_h_kernel(table, own, mine, theirs, final, out, new):
    update_kernel(table, own, mine, theirs, new, out)
    first = lax.axis_index("z4") == 0
    for b in range(NB):
        for high in range(2):
            pair = new[b, 4 * high : 4 * high + 4, :]
            final[2 * high : 2 * high + 2, b * BS : (b + 1) * BS] = jnp.where(first, pair[0:2], pair[2:4])


def last_w_kernel(own, mine, theirs, final, new):
    new[...] = updated(own, mine, theirs)
    first = lax.axis_index("zh") == 0
    for b in range(NB):
        final[:, b * BS : (b + 1) * BS] = jnp.where(first, new[b, 0:2, :], new[b, 2:4, :])


def call(body, scalars, arrays, outs, tables=(), scratch=()):
    smem = pl.BlockSpec(memory_space=pltpu.SMEM)
    vmem = pl.BlockSpec(memory_space=pltpu.VMEM)
    return pl.pallas_call(
        body,
        in_specs=[smem] * len(scalars) + [vmem] * len(arrays),
        out_specs=[vmem] * len(outs) + [smem] * len(tables),
        out_shape=[pltpu.VMEM(s, jnp.float32) for s in outs] + [pltpu.SMEM(s, jnp.int32) for s in tables],
        scratch_shapes=[pltpu.VMEM(s, jnp.float32) for s in scratch],
    )(
        *(pltpu.with_memory_space_constraint(a, pltpu.SMEM) for a in scalars),
        *(pltpu.with_memory_space_constraint(a, pltpu.VMEM) for a in arrays),
    )


def per_device(blocks, observed, w_factor, h_factor):
    blk = blocks[0, 0]
    values = observed[0, 0]
    wide = NB * BS + TAB

    w_other = swap(w_factor, "zh")
    h_other = swap(h_factor, "z4")
    (h_pair,) = call(h_pair_kernel, (blk,), (h_factor, h_other), [(NH, 8, wide)], scratch=[(8, wide)])
    h_got0 = exchange(h_pair, HALF)
    w_other, h_got0 = lax.optimization_barrier((w_other, h_got0))
    (w_pair,) = call(w_pair_kernel, (blk,), (w_factor, w_other), [(NP, 4, wide)], scratch=[(4, wide)])
    w_got0 = exchange(w_pair, PLANE)

    w_slots, h_own, w_own, sent, rows, cols = call(
        first_kernel,
        (blk,),
        (w_got0, h_got0, values),
        [(CAP, RANK, BS), (NB, 8, BS), (NB, 4, BS), (NH, 32, BS)],
        tables=[(NP * CAP,), (NH * CAP,)],
    )
    got = exchange(sent, HALF)
    (mine,) = call(collect_kernel, (cols,), (got,), [(NB, 16, BS)])
    theirs = swap(mine, "z4")
    h_own, out = call(update_kernel, (cols,), (h_own, mine, theirs), [(NB, 8, BS), (NH, 16, BS)])
    h_got = exchange(out, HALF)

    (sent,) = call(w_terms_kernel, (blk,), (h_got, w_slots, values), [(NP, 16, BS)])
    got = exchange(sent, PLANE)
    (mine,) = call(collect_kernel, (rows,), (got,), [(NB, 8, BS)])
    theirs = swap(mine, "zh")
    w_own, out = call(update_kernel, (rows,), (w_own, mine, theirs), [(NB, 4, BS), (NP, 8, BS)])
    w_got = exchange(out, PLANE)

    w_slots, sent = call(h_terms_kernel, (blk,), (w_got, h_got, values), [(CAP, RANK, BS), (NH, 32, BS)])
    got = exchange(sent, HALF)
    (mine,) = call(collect_kernel, (cols,), (got,), [(NB, 16, BS)])
    theirs = swap(mine, "z4")
    h_final, out = call(
        last_h_kernel, (cols,), (h_own, mine, theirs), [(4, NB * BS), (NH, 16, BS)], scratch=[(NB, 8, BS)]
    )
    h_got = exchange(out, HALF)

    (sent,) = call(w_terms_kernel, (blk,), (h_got, w_slots, values), [(NP, 16, BS)])
    got = exchange(sent, PLANE)
    (mine,) = call(collect_kernel, (rows,), (got,), [(NB, 8, BS)])
    theirs = swap(mine, "zh")
    (w_final,) = call(last_w_kernel, (), (w_own, mine, theirs), [(2, NB * BS)], scratch=[(NB, 4, BS)])
    return w_final, h_final


def solution(mesh):
    fine = Mesh(mesh.devices.reshape(2, 2, 2, 2, 2, 4, 4), FINE)
    tex = ("z4",) + HALF
    smp = ("zh",) + PLANE
    in_specs = (P(tex, smp, None, None), P(tex, smp, None, None), P(smp, tex), P(tex, smp))
    out_specs = (P(smp, tex), P(tex, smp))
    return jax.shard_map(per_device, mesh=fine, in_specs=in_specs, out_specs=out_specs, check_vma=False)
```

```python
import jax
import jax.numpy as jnp
from jax import lax
from jax.experimental import pallas as pl
from jax.experimental.pallas import tpu as pltpu
from jax.sharding import Mesh, PartitionSpec as P

RANK = 64
BS = 256
CAP = 2
NB = 4
TAB = 128

FINE = ("z4", "z2", "z1", "core", "zh", "y", "x")
HALF = ("z2", "z1", "core")
PLANE = ("y", "x")
NH = 8
COLS = NB * BS // NH
NP = 16

NN = (((1,), (0,)), ((), ()))
NT = (((1,), (1,)), ((), ()))


def exchange(x, axes):
    return lax.all_to_all(x, axes, split_axis=0, concat_axis=0, tiled=True)


def swap(x, axis):
    return lax.ppermute(x, axis, [(0, 1), (1, 0)])


def halves(x):
    hi = x.astype(jnp.bfloat16)
    lo = (x - hi.astype(jnp.float32)).astype(jnp.bfloat16)
    return hi, lo


def product(a, b, dims):
    dot = lambda x, y: lax.dot_general(x, y, dims, preferred_element_type=jnp.float32)
    return dot(a[0], b[0]) + (dot(a[0], b[1]) + dot(a[1], b[0]))


def grams(left, values, dims, live):
    whole = halves(left)
    left = halves(left * live)
    return product(left, halves(values), dims), product(left, whole, NT)


def sums(left, right, values, dims, live):
    upper, gram = grams(left, values, dims, live)
    return upper, product(halves(gram), halves(right), NN)


def live_of(blk, j):
    return jnp.where(blk[0, j] >= 0, 1.0, 0.0).astype(jnp.float32)


def block_of(blk, d, j):
    return jnp.maximum(blk[d, j], 0)


def with_list(rows, blk, d, lists):
    lane = lax.broadcasted_iota(jnp.int32, (rows.shape[0], TAB), 1)
    lists[:, : NB * BS] = rows
    lists[:, NB * BS :] = jnp.where(lane == 0, blk[d, 0], blk[d, 1]).astype(jnp.float32)


def w_pair_kernel(blk, mine, theirs, out, message):
    first = lax.axis_index("zh") == 0
    low = jnp.where(first, mine[...], theirs[...])
    high = jnp.where(first, theirs[...], mine[...])
    with_list(jnp.concatenate([low, high], axis=0), blk, 0, message)
    for q in range(NP):
        out[q] = message[...]


def read_list(table, q, listed):
    for j in range(CAP):
        table[q * CAP + j] = jnp.maximum(listed[:, j : j + 1].astype(jnp.int32)[0, 0], 0)


def h1_terms_kernel(blk, w0, h, values, w_slots, w_own, out, rows):
    out[:, :96, :] = jnp.zeros((NH, 96, COLS), jnp.float32)
    for j in range(CAP):
        at = pl.multiple_of(block_of(blk, 0, j) * BS, BS)
        for q in range(NP):
            w_slots[j, 4 * q : 4 * q + 4, :] = w0[q, :, pl.ds(at, BS)]
        upper, gram = grams(w_slots[j], values[j * BS : (j + 1) * BS, :], NN, live_of(blk, j))
        gram = jnp.concatenate([gram[:32], gram[32:]], axis=1)
        for side in range(2):
            q = 2 * block_of(blk, 1, j) + side
            out[q, :64, :] = out[q, :64, :] + upper[:, COLS * side : COLS * (side + 1)]
            out[q, 64:96, :] = out[q, 64:96, :] + gram
    lane = lax.broadcasted_iota(jnp.int32, (4, COLS), 1)
    listed = jnp.where(lane == 0, blk[1, 0], blk[1, 1]).astype(jnp.float32)
    for q in range(NH):
        out[q, 96:100, :] = h[:, COLS * q : COLS * (q + 1)]
        out[q, 100:104, :] = listed
    plane = lax.axis_index(PLANE)
    for b in range(NB):
        w_own[b] = w0[plane, :, b * BS : (b + 1) * BS]
    for q in range(NP):
        read_list(rows, q, w0[q, 0:1, NB * BS :])


def h1_collect_kernel(got, out, cols):
    total = got[0, :96, :]
    for q in range(1, NH):
        total = total + got[q, :96, :]
    out[:96, :] = total
    for q in range(NH):
        out[96 + 4 * q : 100 + 4 * q, :] = got[q, 96:100, :]
        read_list(cols, q, got[q, 100:101, :])


def h1_update_kernel(mine, theirs, out):
    total = mine[:96, :] + theirs[:96, :]
    gram = jnp.concatenate([total[64:, :64], total[64:, 64:]], axis=0)
    first = lax.axis_index("z4") == 0
    low = jnp.where(first, mine[96:, :], theirs[96:, :])
    high = jnp.where(first, theirs[96:, :], mine[96:, :])
    pairs = []
    for k in range(16):
        pairs += [low[2 * k : 2 * k + 2], high[2 * k : 2 * k + 2]]
    old = jnp.concatenate(pairs, axis=0)
    new = old * total[:64] / product(halves(gram), halves(old), NN)
    for q in range(NH):
        out[q] = new


def whole_block(h_all, b):
    return jnp.concatenate([h_all[2 * b], h_all[2 * b + 1]], axis=1)


def send_w(out, j, upper, lower):
    for q in range(NP):
        out[q, 8 * j : 8 * j + 4, :] = upper[4 * q : 4 * q + 4, :]
        out[q, 8 * j + 4 : 8 * j + 8, :] = lower[4 * q : 4 * q + 4, :]


def w1_terms_kernel(blk, h_all, w_slots, values, out):
    for j in range(CAP):
        h_slot = whole_block(h_all, block_of(blk, 1, j))
        send_w(out, j, *sums(h_slot, w_slots[j], values[j * BS : (j + 1) * BS, :], NT, live_of(blk, j)))


def w2_terms_kernel(blk, h_got, w_slots, values, out):
    for j in range(CAP):
        h_slot = h_got[:, 8 * j : 8 * j + 8, :].reshape(RANK, BS)
        send_w(out, j, *sums(h_slot, w_slots[j], values[j * BS : (j + 1) * BS, :], NT, live_of(blk, j)))


def w_slot(got, j):
    return jnp.concatenate([got[q, 4 * j : 4 * j + 4, :] for q in range(NP)], axis=0)


def h2_terms_kernel(blk, w_got, values, w_slots, out):
    both = []
    for j in range(CAP):
        w_slots[j] = w_slot(w_got, j)
        upper, gram = grams(w_slots[j], values[j * BS : (j + 1) * BS, :], NN, live_of(blk, j))
        both.append(gram)
        for q in range(NH):
            out[q, :, BS * j : BS * (j + 1)] = upper[8 * q : 8 * q + 8, :]
    both = jnp.concatenate(both, axis=1)
    for q in range(NH):
        out[q, :, CAP * BS :] = both[8 * q : 8 * q + 8, :]


def h2_collect_kernel(table, got, out):
    out[...] = jnp.zeros(out.shape, out.dtype)
    lane = lax.broadcasted_iota(jnp.int32, (8, CAP * RANK), 1)
    for q in range(NH):
        gram = got[q, :, CAP * BS :]
        for j in range(CAP):
            b = table[q * CAP + j]
            out[b, :, :BS] = out[b, :, :BS] + got[q, :, BS * j : BS * (j + 1)]
            out[b, :, BS:] = out[b, :, BS:] + jnp.where(lane // RANK == j, gram, 0.0)


def h2_update_kernel(table, h_all, mine, theirs, final, out, new):
    half = lax.axis_index(HALF)
    first = lax.axis_index("z4") == 0
    for b in range(NB):
        total = mine[b] + theirs[b]
        gram = total[:, BS:]
        high = gram.astype(jnp.bfloat16).astype(jnp.float32)
        gram = jnp.concatenate([high, gram - high], axis=0).astype(jnp.bfloat16)
        block = whole_block(h_all, b)
        block = halves(jnp.concatenate([block, block], axis=0))
        most = lax.dot_general(gram, block[0], NN, preferred_element_type=jnp.float32)
        rest = lax.dot_general(gram, block[1], NN, preferred_element_type=jnp.float32)
        lower = most[:8] + (most[8:] + rest[:8])
        at = pl.multiple_of(8 * half, 8)
        own = jnp.concatenate([h_all[2 * b, pl.ds(at, 8), :], h_all[2 * b + 1, pl.ds(at, 8), :]], axis=1)
        rows = own * total[:, :BS] / lower
        new[b] = rows
        for high in range(2):
            pair = rows[4 * high : 4 * high + 4]
            final[2 * high : 2 * high + 2, b * BS : (b + 1) * BS] = jnp.where(first, pair[0:2], pair[2:4])
    for q in range(NH):
        for j in range(CAP):
            out[q, 8 * j : 8 * (j + 1), :] = new[table[q * CAP + j]]


def collect_kernel(table, got, out):
    rows = out.shape[1]
    out[...] = jnp.zeros(out.shape, out.dtype)
    for q in range(got.shape[0]):
        for j in range(CAP):
            b = table[q * CAP + j]
            out[b] = out[b] + got[q, rows * j : rows * (j + 1), :]


def updated(own, mine, theirs):
    rows = own.shape[1]
    upper = mine[:, :rows, :] + theirs[:, :rows, :]
    lower = mine[:, rows:, :] + theirs[:, rows:, :]
    return own[...] * upper / lower


def update_kernel(table, own, mine, theirs, new, out):
    rows = own.shape[1]
    new[...] = updated(own, mine, theirs)
    for q in range(out.shape[0]):
        for j in range(CAP):
            out[q, rows * j : rows * (j + 1), :] = new[table[q * CAP + j]]


def last_w_kernel(own, mine, theirs, final, new):
    new[...] = updated(own, mine, theirs)
    first = lax.axis_index("zh") == 0
    for b in range(NB):
        final[:, b * BS : (b + 1) * BS] = jnp.where(first, new[b, 0:2, :], new[b, 2:4, :])


def call(body, scalars, arrays, outs, tables=(), scratch=(), name=None):
    smem = pl.BlockSpec(memory_space=pltpu.SMEM)
    vmem = pl.BlockSpec(memory_space=pltpu.VMEM)
    return pl.pallas_call(
        body,
        in_specs=[smem] * len(scalars) + [vmem] * len(arrays),
        out_specs=[vmem] * len(outs) + [smem] * len(tables),
        out_shape=[pltpu.VMEM(s, jnp.float32) for s in outs] + [pltpu.SMEM(s, jnp.int32) for s in tables],
        scratch_shapes=[pltpu.VMEM(s, jnp.float32) for s in scratch],
        name=name,
    )(
        *(pltpu.with_memory_space_constraint(a, pltpu.SMEM) for a in scalars),
        *(pltpu.with_memory_space_constraint(a, pltpu.VMEM) for a in arrays),
    )


def per_device(blocks, observed, w_factor, h_factor):
    blk = blocks[0, 0]
    values = observed[0, 0]
    wide = NB * BS + TAB

    w_other = swap(w_factor, "zh")
    (w_pair,) = call(w_pair_kernel, (blk,), (w_factor, w_other), [(NP, 4, wide)], scratch=[(4, wide)], name="w_pair")
    w_got = exchange(w_pair, PLANE)

    w_slots, w_own, sent, rows = call(
        h1_terms_kernel,
        (blk,),
        (w_got, h_factor, values),
        [(CAP, RANK, BS), (NB, 4, BS), (NH, 104, COLS)],
        tables=[(NP * CAP,)],
        name="h1_terms",
    )
    got = exchange(sent, HALF)
    mine, cols = call(h1_collect_kernel, (), (got,), [(128, COLS)], tables=[(NH * CAP,)], name="h1_collect")
    theirs = swap(mine, "z4")
    (out,) = call(h1_update_kernel, (), (mine, theirs), [(NH, RANK, COLS)], name="h1_update")
    h_all = exchange(out, HALF)

    (sent,) = call(w1_terms_kernel, (blk,), (h_all, w_slots, values), [(NP, 16, BS)], name="w1_terms")
    got = exchange(sent, PLANE)
    (mine,) = call(collect_kernel, (rows,), (got,), [(NB, 8, BS)], name="w1_collect")
    theirs = swap(mine, "zh")
    w_own, out = call(
        update_kernel, (rows,), (w_own, mine, theirs), [(NB, 4, BS), (NP, 8, BS)], name="w1_update"
    )
    w_got = exchange(out, PLANE)

    w_slots, sent = call(
        h2_terms_kernel, (blk,), (w_got, values), [(CAP, RANK, BS), (NH, 8, CAP * (BS + RANK))], name="h2_terms"
    )
    got = exchange(sent, HALF)
    (mine,) = call(h2_collect_kernel, (cols,), (got,), [(NB, 8, BS + CAP * RANK)], name="h2_collect")
    theirs = swap(mine, "z4")
    h_final, out = call(
        h2_update_kernel,
        (cols,),
        (h_all, mine, theirs),
        [(4, NB * BS), (NH, 16, BS)],
        scratch=[(NB, 8, BS)],
        name="h2_update",
    )
    h_got = exchange(out, HALF)

    (sent,) = call(w2_terms_kernel, (blk,), (h_got, w_slots, values), [(NP, 16, BS)], name="w2_terms")
    got = exchange(sent, PLANE)
    (mine,) = call(collect_kernel, (rows,), (got,), [(NB, 8, BS)], name="w2_collect")
    theirs = swap(mine, "zh")
    (w_final,) = call(
        last_w_kernel, (), (w_own, mine, theirs), [(2, NB * BS)], scratch=[(NB, 4, BS)], name="w2_update"
    )
    return w_final, h_final


def solution(mesh):
    fine = Mesh(mesh.devices.reshape(2, 2, 2, 2, 2, 4, 4), FINE)
    tex = ("z4",) + HALF
    smp = ("zh",) + PLANE
    in_specs = (P(tex, smp, None, None), P(tex, smp, None, None), P(smp, tex), P(tex, smp))
    out_specs = (P(smp, tex), P(tex, smp))
    return jax.shard_map(per_device, mesh=fine, in_specs=in_specs, out_specs=out_specs, check_vma=False)
```

```python
import jax
import jax.numpy as jnp
from jax import lax
from jax.experimental import pallas as pl
from jax.experimental.pallas import tpu as pltpu
from jax.sharding import Mesh, PartitionSpec as P


RANK = 64
BS = 256
CAP = 2
NB = 4
TAB = 128

FINE = ("z4", "z2", "z1", "core", "zh", "y", "x")
HALF = ("z2", "z1", "core")
PLANE = ("y", "x")
QUAD = ("z2", "z1")
NH = 8
NQ = 4
NP = 16

NN = (((1,), (0,)), ((), ()))
NT = (((1,), (1,)), ((), ()))


def exchange(x, axes):
    return lax.all_to_all(x, axes, split_axis=0, concat_axis=0, tiled=True)


def swap(x, axis):
    return lax.ppermute(x, axis, [(0, 1), (1, 0)])


def halves(x):
    hi = x.astype(jnp.bfloat16)
    lo = (x - hi.astype(jnp.float32)).astype(jnp.bfloat16)
    return hi, lo


def product(a, b, dims):
    dot = lambda x, y: lax.dot_general(x, y, dims, preferred_element_type=jnp.float32)
    return dot(a[0], b[0]) + (dot(a[0], b[1]) + dot(a[1], b[0]))


def grams(left, values, dims, live):
    whole = halves(left)
    left = halves(left * live)
    return product(left, halves(values), dims), product(left, whole, NT)


def sums(left, right, values, dims, live):
    upper, gram = grams(left, values, dims, live)
    return upper, product(halves(gram), halves(right), NN)


def live_of(blk, j):
    return jnp.where(blk[0, j] >= 0, 1.0, 0.0).astype(jnp.float32)


def block_of(blk, d, j):
    return jnp.maximum(blk[d, j], 0)


def with_list(rows, blk, d, lists):
    lane = lax.broadcasted_iota(jnp.int32, (rows.shape[0], TAB), 1)
    lists[:, : NB * BS] = rows
    lists[:, NB * BS :] = jnp.where(lane == 0, blk[d, 0], blk[d, 1]).astype(jnp.float32)


def w_pair_kernel(blk, mine, theirs, out, message):
    first = lax.axis_index("zh") == 0
    low = jnp.where(first, mine[...], theirs[...])
    high = jnp.where(first, theirs[...], mine[...])
    with_list(jnp.concatenate([low, high], axis=0), blk, 0, message)
    for q in range(NP):
        out[q] = message[...]


def read_list(table, q, listed):
    for j in range(CAP):
        table[q * CAP + j] = jnp.maximum(listed[:, j : j + 1].astype(jnp.int32)[0, 0], 0)


def h_pack_kernel(blk, h, out, message):
    with_list(h[...], blk, 1, message)
    for q in range(NQ):
        out[q] = message[...]


def h_arrange_kernel(mine, theirs, h_all):
    first = lax.axis_index("z4") == 0
    for b in range(NB):
        lanes = slice(b * BS, (b + 1) * BS)
        for q in range(NH):
            at = 8 * q
            for high in range(2):
                pair = slice(2 * high, 2 * high + 2)
                here = mine[q % 2, q // 2, pair, lanes]
                there = theirs[q % 2, q // 2, pair, lanes]
                h_all[b, at + 4 * high : at + 4 * high + 2, :] = jnp.where(first, here, there)
                h_all[b, at + 4 * high + 2 : at + 4 * high + 4, :] = jnp.where(first, there, here)


def send_grams(out, uppers, both):
    both = jnp.concatenate(both, axis=1)
    for q in range(NH):
        for j in range(CAP):
            out[q, :, BS * j : BS * (j + 1)] = uppers[j][8 * q : 8 * q + 8, :]
        out[q, :, CAP * BS :] = both[8 * q : 8 * q + 8, :]


def h1_terms_kernel(blk, w0, h_half, values, w_slots, w_own, out, rows, cols):
    terms = []
    for j in range(CAP):
        at = pl.multiple_of(block_of(blk, 0, j) * BS, BS)
        for q in range(NP):
            w_slots[j, 4 * q : 4 * q + 4, :] = w0[q, :, pl.ds(at, BS)]
        terms.append(grams(w_slots[j], values[j * BS : (j + 1) * BS, :], NN, live_of(blk, j)))
    send_grams(out, *zip(*terms))
    plane = lax.axis_index(PLANE)
    for b in range(NB):
        w_own[b] = w0[plane, :, b * BS : (b + 1) * BS]
    for q in range(NP):
        read_list(rows, q, w0[q, 0:1, NB * BS :])
    for q in range(NH):
        read_list(cols, q, h_half[q % 2, q // 2, 0:1, NB * BS :])


def h_updated(h_all, mine, theirs, b, half):
    total = mine[b] + theirs[b]
    gram = total[:, BS:]
    high = gram.astype(jnp.bfloat16).astype(jnp.float32)
    gram = jnp.concatenate([high, gram - high], axis=0).astype(jnp.bfloat16)
    block = h_all[b]
    block = halves(jnp.concatenate([block, block], axis=0))
    most = lax.dot_general(gram, block[0], NN, preferred_element_type=jnp.float32)
    rest = lax.dot_general(gram, block[1], NN, preferred_element_type=jnp.float32)
    own = h_all[b, pl.ds(pl.multiple_of(8 * half, 8), 8), :]
    return own * total[:, :BS] / (most[:8] + (most[8:] + rest[:8]))


def h1_update_kernel(h_all, mine, theirs, out):
    half = lax.axis_index(HALF)
    for b in range(NB):
        rows = h_updated(h_all, mine, theirs, b, half)
        for q in range(NQ):
            out[q, b] = rows


def send_w(out, j, upper, lower):
    for q in range(NP):
        out[q, 8 * j : 8 * j + 4, :] = upper[4 * q : 4 * q + 4, :]
        out[q, 8 * j + 4 : 8 * j + 8, :] = lower[4 * q : 4 * q + 4, :]


def w1_terms_kernel(blk, h_got, w_slots, values, h_all, out):
    for b in range(NB):
        for q in range(NH):
            h_all[b, 8 * q : 8 * q + 8, :] = h_got[q % 2, q // 2, b]
    for j in range(CAP):
        h_slot = h_all[block_of(blk, 1, j)]
        send_w(out, j, *sums(h_slot, w_slots[j], values[j * BS : (j + 1) * BS, :], NT, live_of(blk, j)))


def w2_terms_kernel(blk, h_got, w_slots, values, out):
    for j in range(CAP):
        h_slot = h_got[:, 8 * j : 8 * j + 8, :].reshape(RANK, BS)
        send_w(out, j, *sums(h_slot, w_slots[j], values[j * BS : (j + 1) * BS, :], NT, live_of(blk, j)))


def w_slot(got, j):
    return jnp.concatenate([got[q, 4 * j : 4 * j + 4, :] for q in range(NP)], axis=0)


def h2_terms_kernel(blk, w_got, values, w_slots, out):
    terms = []
    for j in range(CAP):
        w_slots[j] = w_slot(w_got, j)
        terms.append(grams(w_slots[j], values[j * BS : (j + 1) * BS, :], NN, live_of(blk, j)))
    send_grams(out, *zip(*terms))


def h_collect_kernel(table, got, out):
    out[...] = jnp.zeros(out.shape, out.dtype)
    lane = lax.broadcasted_iota(jnp.int32, (8, CAP * RANK), 1)
    for q in range(NH):
        gram = got[q, :, CAP * BS :]
        for j in range(CAP):
            b = table[q * CAP + j]
            out[b, :, :BS] = out[b, :, :BS] + got[q, :, BS * j : BS * (j + 1)]
            out[b, :, BS:] = out[b, :, BS:] + jnp.where(lane // RANK == j, gram, 0.0)


def h2_update_kernel(table, h_all, mine, theirs, final, out, new):
    half = lax.axis_index(HALF)
    first = lax.axis_index("z4") == 0
    for b in range(NB):
        rows = h_updated(h_all, mine, theirs, b, half)
        new[b] = rows
        for high in range(2):
            pair = rows[4 * high : 4 * high + 4]
            final[2 * high : 2 * high + 2, b * BS : (b + 1) * BS] = jnp.where(first, pair[0:2], pair[2:4])
    for q in range(NH):
        for j in range(CAP):
            out[q, 8 * j : 8 * (j + 1), :] = new[table[q * CAP + j]]


def collect_kernel(table, got, out):
    rows = out.shape[1]
    out[...] = jnp.zeros(out.shape, out.dtype)
    for q in range(got.shape[0]):
        for j in range(CAP):
            b = table[q * CAP + j]
            out[b] = out[b] + got[q, rows * j : rows * (j + 1), :]


def updated(own, mine, theirs):
    rows = own.shape[1]
    upper = mine[:, :rows, :] + theirs[:, :rows, :]
    lower = mine[:, rows:, :] + theirs[:, rows:, :]
    return own[...] * upper / lower


def update_kernel(table, own, mine, theirs, new, out):
    rows = own.shape[1]
    new[...] = updated(own, mine, theirs)
    for q in range(out.shape[0]):
        for j in range(CAP):
            out[q, rows * j : rows * (j + 1), :] = new[table[q * CAP + j]]


def last_w_kernel(own, mine, theirs, final, new):
    new[...] = updated(own, mine, theirs)
    first = lax.axis_index("zh") == 0
    for b in range(NB):
        final[:, b * BS : (b + 1) * BS] = jnp.where(first, new[b, 0:2, :], new[b, 2:4, :])


def call(body, scalars, arrays, outs, tables=(), scratch=()):
    smem = pl.BlockSpec(memory_space=pltpu.SMEM)
    vmem = pl.BlockSpec(memory_space=pltpu.VMEM)
    return pl.pallas_call(
        body,
        in_specs=[smem] * len(scalars) + [vmem] * len(arrays),
        out_specs=[vmem] * len(outs) + [smem] * len(tables),
        out_shape=[pltpu.VMEM(s, jnp.float32) for s in outs] + [pltpu.SMEM(s, jnp.int32) for s in tables],
        scratch_shapes=[pltpu.VMEM(s, jnp.float32) for s in scratch],
    )(
        *(pltpu.with_memory_space_constraint(a, pltpu.SMEM) for a in scalars),
        *(pltpu.with_memory_space_constraint(a, pltpu.VMEM) for a in arrays),
    )


def per_device(blocks, observed, w_factor, h_factor):
    blk = blocks[0, 0]
    values = observed[0, 0]
    wide = NB * BS + TAB

    w_other = swap(w_factor, "zh")
    (h_pack,) = call(h_pack_kernel, (blk,), (h_factor,), [(NQ, 4, wide)], scratch=[(4, wide)])
    h_quad = exchange(h_pack, QUAD)
    h_half = lax.all_gather(h_quad, "core", axis=0)
    h_other = swap(h_half, "z4")
    (w_pair,) = call(w_pair_kernel, (blk,), (w_factor, w_other), [(NP, 4, wide)], scratch=[(4, wide)])
    w_got = exchange(w_pair, PLANE)

    grams_out = (NH, 8, CAP * (BS + RANK))
    w_slots, w_own, sent, rows, cols = call(
        h1_terms_kernel,
        (blk,),
        (w_got, h_half, values),
        [(CAP, RANK, BS), (NB, 4, BS), grams_out],
        tables=[(NP * CAP,), (NH * CAP,)],
    )
    got = exchange(sent, HALF)
    (mine,) = call(h_collect_kernel, (cols,), (got,), [(NB, 8, BS + CAP * RANK)])
    theirs = swap(mine, "z4")
    (h_all,) = call(h_arrange_kernel, (), (h_half, h_other), [(NB, RANK, BS)])
    (out,) = call(h1_update_kernel, (), (h_all, mine, theirs), [(NQ, NB, 8, BS)])
    h_got = lax.all_gather(exchange(out, QUAD), "core", axis=0)

    h_all, sent = call(w1_terms_kernel, (blk,), (h_got, w_slots, values), [(NB, RANK, BS), (NP, 16, BS)])
    got = exchange(sent, PLANE)
    (mine,) = call(collect_kernel, (rows,), (got,), [(NB, 8, BS)])
    theirs = swap(mine, "zh")
    w_own, out = call(update_kernel, (rows,), (w_own, mine, theirs), [(NB, 4, BS), (NP, 8, BS)])
    w_got = exchange(out, PLANE)

    w_slots, sent = call(h2_terms_kernel, (blk,), (w_got, values), [(CAP, RANK, BS), grams_out])
    got = exchange(sent, HALF)
    (mine,) = call(h_collect_kernel, (cols,), (got,), [(NB, 8, BS + CAP * RANK)])
    theirs = swap(mine, "z4")
    h_final, out = call(
        h2_update_kernel, (cols,), (h_all, mine, theirs), [(4, NB * BS), (NH, 16, BS)], scratch=[(NB, 8, BS)]
    )
    h_got = exchange(out, HALF)

    (sent,) = call(w2_terms_kernel, (blk,), (h_got, w_slots, values), [(NP, 16, BS)])
    got = exchange(sent, PLANE)
    (mine,) = call(collect_kernel, (rows,), (got,), [(NB, 8, BS)])
    theirs = swap(mine, "zh")
    (w_final,) = call(last_w_kernel, (), (w_own, mine, theirs), [(2, NB * BS)], scratch=[(NB, 4, BS)])
    return w_final, h_final


def solution(mesh):
    fine = Mesh(mesh.devices.reshape(2, 2, 2, 2, 2, 4, 4), FINE)
    tex = ("z4",) + HALF
    smp = ("zh",) + PLANE
    in_specs = (P(tex, smp, None, None), P(tex, smp, None, None), P(smp, tex), P(tex, smp))
    out_specs = (P(smp, tex), P(tex, smp))
    return jax.shard_map(per_device, mesh=fine, in_specs=in_specs, out_specs=out_specs, check_vma=False)
```

```python
import jax
import jax.numpy as jnp
from jax import lax
from jax.experimental import pallas as pl
from jax.experimental.pallas import tpu as pltpu
from jax.sharding import Mesh, PartitionSpec as P


RANK = 64
BS = 256
CAP = 2
NB = 4
TAB = 128

FINE = ("z4", "z2", "z1", "core", "zh", "y", "x")
HALF = ("z2", "z1", "core")
QUAD = ("z2", "z1")
PLANE = ("y", "x")
NH = 8
NQ = 4
COLS = NB * BS // NH
NP = 16

NN = (((1,), (0,)), ((), ()))
NT = (((1,), (1,)), ((), ()))


def exchange(x, axes):
    return lax.all_to_all(x, axes, split_axis=0, concat_axis=0, tiled=True)


def swap(x, axis):
    return lax.ppermute(x, axis, [(0, 1), (1, 0)])


def halves(x):
    hi = x.astype(jnp.bfloat16)
    lo = (x - hi.astype(jnp.float32)).astype(jnp.bfloat16)
    return hi, lo


def product(a, b, dims=NN):
    dot = lambda x, y: lax.dot_general(x, y, dims, preferred_element_type=jnp.float32)
    return dot(a[0], b[0]) + (dot(a[0], b[1]) + dot(a[1], b[0]))


def grams(left, values, live):
    whole = halves(left)
    left = halves(left * live)
    return product(left, values), product(left, whole, NT)


def sums(left, right, values, live):
    upper, gram = grams(left, values, live)
    return upper, product(halves(gram), halves(right))


def prepare_kernel(values, w, parts, turned, w_mine):
    w_mine[...] = w[...]
    for j in range(CAP):
        block = values[j * BS : (j + 1) * BS, :]
        parts[j, 0], parts[j, 1] = halves(block)
        turned[j, 0], turned[j, 1] = halves(block.T)


def both_of(parts, j):
    return parts[j, 0], parts[j, 1]


def live_of(blk, j):
    return jnp.where(blk[0, j] >= 0, 1.0, 0.0).astype(jnp.float32)


def block_of(blk, d, j):
    return jnp.maximum(blk[d, j], 0)


def with_list(rows, blk, d, lists):
    lane = lax.broadcasted_iota(jnp.int32, (rows.shape[0], TAB), 1)
    lists[:, : NB * BS] = rows
    lists[:, NB * BS :] = jnp.where(lane == 0, blk[d, 0], blk[d, 1]).astype(jnp.float32)


def w_pair_kernel(blk, mine, theirs, out, message):
    first = lax.axis_index("zh") == 0
    low = jnp.where(first, mine[...], theirs[...])
    high = jnp.where(first, theirs[...], mine[...])
    with_list(jnp.concatenate([low, high], axis=0), blk, 0, message)
    for q in range(NP):
        out[q] = message[...]


def read_list(table, q, listed):
    for j in range(CAP):
        table[q * CAP + j] = jnp.maximum(listed[:, j : j + 1].astype(jnp.int32)[0, 0], 0)


def h1_terms_kernel(blk, w0, h, values, w_slots, w_own, out, rows):
    out[:, :96, :] = jnp.zeros((NH, 96, COLS), jnp.float32)
    for j in range(CAP):
        at = pl.multiple_of(block_of(blk, 0, j) * BS, BS)
        for q in range(NP):
            w_slots[j, 4 * q : 4 * q + 4, :] = w0[q, :, pl.ds(at, BS)]
        upper, gram = grams(w_slots[j], both_of(values, j), live_of(blk, j))
        gram = jnp.concatenate([gram[:32], gram[32:]], axis=1)
        for side in range(2):
            q = 2 * block_of(blk, 1, j) + side
            out[q, :64, :] = out[q, :64, :] + upper[:, COLS * side : COLS * (side + 1)]
            out[q, 64:96, :] = out[q, 64:96, :] + gram
    lane = lax.broadcasted_iota(jnp.int32, (4, COLS), 1)
    listed = jnp.where(lane == 0, blk[1, 0], blk[1, 1]).astype(jnp.float32)
    for q in range(NH):
        out[q, 96:100, :] = h[:, COLS * q : COLS * (q + 1)]
        out[q, 100:104, :] = listed
    plane = lax.axis_index(PLANE)
    for b in range(NB):
        w_own[b] = w0[plane, :, b * BS : (b + 1) * BS]
    for q in range(NP):
        read_list(rows, q, w0[q, 0:1, NB * BS :])


def h1_collect_kernel(got, out, cols):
    total = got[0, :96, :]
    for q in range(1, NH):
        total = total + got[q, :96, :]
    out[:96, :] = total
    for q in range(NH):
        out[96 + 4 * q : 100 + 4 * q, :] = got[q, 96:100, :]
        read_list(cols, q, got[q, 100:101, :])


def h1_update_kernel(mine, theirs, out):
    total = mine[:96, :] + theirs[:96, :]
    gram = jnp.concatenate([total[64:, :64], total[64:, 64:]], axis=0)
    first = lax.axis_index("z4") == 0
    low = jnp.where(first, mine[96:, :], theirs[96:, :])
    high = jnp.where(first, theirs[96:, :], mine[96:, :])
    pairs = []
    for k in range(16):
        pairs += [low[2 * k : 2 * k + 2], high[2 * k : 2 * k + 2]]
    old = jnp.concatenate(pairs, axis=0)
    new = old * total[:64] / product(halves(gram), halves(old))
    for q in range(NQ):
        out[q] = new


def whole_block(h_all, b):
    return jnp.concatenate([h_all[0, b], h_all[1, b]], axis=1)


def send_w(out, j, upper, lower):
    for q in range(NP):
        out[q, 8 * j : 8 * j + 4, :] = upper[4 * q : 4 * q + 4, :]
        out[q, 8 * j + 4 : 8 * j + 8, :] = lower[4 * q : 4 * q + 4, :]


def w1_terms_kernel(blk, h_all, w_slots, values, out):
    for j in range(CAP):
        h_slot = whole_block(h_all, block_of(blk, 1, j))
        send_w(out, j, *sums(h_slot, w_slots[j], both_of(values, j), live_of(blk, j)))


def w2_terms_kernel(blk, h_got, w_slots, values, out):
    for j in range(CAP):
        h_slot = h_got[:, 8 * j : 8 * j + 8, :].reshape(RANK, BS)
        send_w(out, j, *sums(h_slot, w_slots[j], both_of(values, j), live_of(blk, j)))


def w_slot(got, j):
    return jnp.concatenate([got[q, 4 * j : 4 * j + 4, :] for q in range(NP)], axis=0)


def h2_terms_kernel(blk, w_got, values, w_slots, out):
    both = []
    for j in range(CAP):
        w_slots[j] = w_slot(w_got, j)
        upper, gram = grams(w_slots[j], both_of(values, j), live_of(blk, j))
        both.append(gram)
        for q in range(NH):
            out[q, :, BS * j : BS * (j + 1)] = upper[8 * q : 8 * q + 8, :]
    both = jnp.concatenate(both, axis=1)
    for q in range(NH):
        out[q, :, CAP * BS :] = both[8 * q : 8 * q + 8, :]


def h2_collect_kernel(table, got, out):
    out[...] = jnp.zeros(out.shape, out.dtype)
    lane = lax.broadcasted_iota(jnp.int32, (8, CAP * RANK), 1)
    for q in range(NH):
        gram = got[q, :, CAP * BS :]
        for j in range(CAP):
            b = table[q * CAP + j]
            out[b, :, :BS] = out[b, :, :BS] + got[q, :, BS * j : BS * (j + 1)]
            out[b, :, BS:] = out[b, :, BS:] + jnp.where(lane // RANK == j, gram, 0.0)


def h2_update_kernel(table, h_all, mine, theirs, final, out, new):
    half = lax.axis_index(HALF)
    first = lax.axis_index("z4") == 0
    for b in range(NB):
        total = mine[b] + theirs[b]
        gram = total[:, BS:]
        high = gram.astype(jnp.bfloat16).astype(jnp.float32)
        gram = jnp.concatenate([high, gram - high], axis=0).astype(jnp.bfloat16)
        block = whole_block(h_all, b)
        block = halves(jnp.concatenate([block, block], axis=0))
        most = lax.dot_general(gram, block[0], NN, preferred_element_type=jnp.float32)
        rest = lax.dot_general(gram, block[1], NN, preferred_element_type=jnp.float32)
        lower = most[:8] + (most[8:] + rest[:8])
        at = pl.multiple_of(8 * half, 8)
        own = jnp.concatenate([h_all[0, b, pl.ds(at, 8), :], h_all[1, b, pl.ds(at, 8), :]], axis=1)
        rows = own * total[:, :BS] / lower
        new[b] = rows
        for high in range(2):
            pair = rows[4 * high : 4 * high + 4]
            final[2 * high : 2 * high + 2, b * BS : (b + 1) * BS] = jnp.where(first, pair[0:2], pair[2:4])
    for q in range(NH):
        for j in range(CAP):
            out[q, 8 * j : 8 * (j + 1), :] = new[table[q * CAP + j]]


def collect_kernel(table, got, out):
    rows = out.shape[1]
    out[...] = jnp.zeros(out.shape, out.dtype)
    for q in range(got.shape[0]):
        for j in range(CAP):
            b = table[q * CAP + j]
            out[b] = out[b] + got[q, rows * j : rows * (j + 1), :]


def updated(own, mine, theirs):
    rows = own.shape[1]
    upper = mine[:, :rows, :] + theirs[:, :rows, :]
    lower = mine[:, rows:, :] + theirs[:, rows:, :]
    return own[...] * upper / lower


def update_kernel(table, own, mine, theirs, new, out):
    rows = own.shape[1]
    new[...] = updated(own, mine, theirs)
    for q in range(out.shape[0]):
        for j in range(CAP):
            out[q, rows * j : rows * (j + 1), :] = new[table[q * CAP + j]]


def last_w_kernel(own, mine, theirs, final, new):
    new[...] = updated(own, mine, theirs)
    first = lax.axis_index("zh") == 0
    for b in range(NB):
        final[:, b * BS : (b + 1) * BS] = jnp.where(first, new[b, 0:2, :], new[b, 2:4, :])


def call(body, scalars, arrays, outs, tables=(), scratch=(), last=False, dtypes=None):
    smem = pl.BlockSpec(memory_space=pltpu.SMEM)
    vmem = pl.BlockSpec(memory_space=pltpu.VMEM)
    kind = jax.ShapeDtypeStruct if last else pltpu.VMEM
    return pl.pallas_call(
        body,
        in_specs=[smem] * len(scalars) + [vmem] * len(arrays),
        out_specs=[vmem] * len(outs) + [smem] * len(tables),
        out_shape=[kind(*s) for s in zip(outs, dtypes or [jnp.float32] * len(outs))] + [pltpu.SMEM(s, jnp.int32) for s in tables],
        scratch_shapes=[pltpu.VMEM(s, jnp.float32) for s in scratch],
    )(
        *(pltpu.with_memory_space_constraint(a, pltpu.SMEM) for a in scalars),
        *(pltpu.with_memory_space_constraint(a, pltpu.VMEM) for a in arrays),
    )


def per_device(blocks, observed, w_factor, h_factor):
    blk = blocks[0, 0]
    wide = NB * BS + TAB

    w_other = swap(w_factor, "zh")
    values, turned, w_mine = call(
        prepare_kernel,
        (),
        (observed[0, 0], w_factor),
        [(CAP, 2, BS, BS), (CAP, 2, BS, BS), w_factor.shape],
        dtypes=[jnp.bfloat16, jnp.bfloat16, jnp.float32],
    )
    (w_pair,) = call(w_pair_kernel, (blk,), (w_mine, w_other), [(NP, 4, wide)], scratch=[(4, wide)])
    w_got = exchange(w_pair, PLANE)

    w_slots, w_own, sent, rows = call(
        h1_terms_kernel,
        (blk,),
        (w_got, h_factor, values),
        [(CAP, RANK, BS), (NB, 4, BS), (NH, 104, COLS)],
        tables=[(NP * CAP,)],
    )
    got = exchange(sent, HALF)
    mine, cols = call(h1_collect_kernel, (), (got,), [(128, COLS)], tables=[(NH * CAP,)])
    theirs = swap(mine, "z4")
    (out,) = call(h1_update_kernel, (), (mine, theirs), [(NQ, RANK, COLS)])
    h_all = lax.all_gather(exchange(out, QUAD), "core", axis=0)

    (sent,) = call(w1_terms_kernel, (blk,), (h_all, w_slots, turned), [(NP, 16, BS)])
    got = exchange(sent, PLANE)
    (mine,) = call(collect_kernel, (rows,), (got,), [(NB, 8, BS)])
    theirs = swap(mine, "zh")
    w_own, out = call(update_kernel, (rows,), (w_own, mine, theirs), [(NB, 4, BS), (NP, 8, BS)])
    w_got = exchange(out, PLANE)

    w_slots, sent = call(h2_terms_kernel, (blk,), (w_got, values), [(CAP, RANK, BS), (NH, 8, CAP * (BS + RANK))])
    got = exchange(sent, HALF)
    (mine,) = call(h2_collect_kernel, (cols,), (got,), [(NB, 8, BS + CAP * RANK)])
    theirs = swap(mine, "z4")
    h_final, out = call(
        h2_update_kernel, (cols,), (h_all, mine, theirs), [(4, NB * BS), (NH, 16, BS)], scratch=[(NB, 8, BS)]
    )
    h_got = exchange(out, HALF)

    (sent,) = call(w2_terms_kernel, (blk,), (h_got, w_slots, turned), [(NP, 16, BS)])
    got = exchange(sent, PLANE)
    (mine,) = call(collect_kernel, (rows,), (got,), [(NB, 8, BS)])
    theirs = swap(mine, "zh")
    (w_final,) = call(last_w_kernel, (), (w_own, mine, theirs), [(2, NB * BS)], scratch=[(NB, 4, BS)], last=True)
    return w_final, h_final


def solution(mesh):
    fine = Mesh(mesh.devices.reshape(2, 2, 2, 2, 2, 4, 4), FINE)
    tex = ("z4",) + HALF
    smp = ("zh",) + PLANE
    in_specs = (P(tex, smp, None, None), P(tex, smp, None, None), P(smp, tex), P(tex, smp))
    out_specs = (P(smp, tex), P(tex, smp))
    return jax.shard_map(per_device, mesh=fine, in_specs=in_specs, out_specs=out_specs, check_vma=False)
```

```python
import jax
import jax.numpy as jnp
from jax import lax
from jax.experimental import pallas as pl
from jax.experimental.pallas import tpu as pltpu
from jax.sharding import Mesh, PartitionSpec as P


RANK = 64
BS = 256
CAP = 2
NB = 4
TAB = 128

FINE = ("z4", "z2", "z1", "core", "zh", "y", "x")
HALF = ("z2", "z1", "core")
QUAD = ("z2", "z1")
PLANE = ("y", "x")
NH = 8
NQ = 4
COLS = NB * BS // NH
NP = 16

NN = (((1,), (0,)), ((), ()))
NT = (((1,), (1,)), ((), ()))


def exchange(x, axes):
    return lax.all_to_all(x, axes, split_axis=0, concat_axis=0, tiled=True)


def swap(x, axis):
    return lax.ppermute(x, axis, [(0, 1), (1, 0)])


def halves(x):
    hi = x.astype(jnp.bfloat16)
    lo = (x - hi.astype(jnp.float32)).astype(jnp.bfloat16)
    return hi, lo


def product(a, b, dims=NN):
    dot = lambda x, y: lax.dot_general(x, y, dims, preferred_element_type=jnp.float32)
    return dot(a[0], b[0]) + (dot(a[0], b[1]) + dot(a[1], b[0]))


def grams(left, values, live):
    whole = halves(left)
    left = halves(left * live)
    return product(left, values), product(left, whole, NT)


def sums(left, right, values, live):
    upper, gram = grams(left, values, live)
    return upper, product(halves(gram), halves(right))


def prepare_kernel(blk, values, w, parts, turned, w_mine, listed):
    for d in range(2):
        for j in range(CAP):
            listed[CAP * d + j] = blk[d, j]
    w_mine[...] = w[...]
    for j in range(CAP):
        block = values[j * BS : (j + 1) * BS, :]
        parts[j, 0], parts[j, 1] = halves(block)
        turned[j, 0], turned[j, 1] = halves(block.T)


def both_of(parts, j):
    return parts[j, 0], parts[j, 1]


def live_of(blk, j):
    return jnp.where(blk[j] >= 0, 1.0, 0.0).astype(jnp.float32)


def block_of(blk, d, j):
    return jnp.maximum(blk[CAP * d + j], 0)


def with_list(rows, blk, d, lists):
    lane = lax.broadcasted_iota(jnp.int32, (rows.shape[0], TAB), 1)
    lists[:, : NB * BS] = rows
    lists[:, NB * BS :] = jnp.where(lane == 0, blk[CAP * d], blk[CAP * d + 1]).astype(jnp.float32)


def w_pair_kernel(blk, mine, theirs, out, message):
    first = lax.axis_index("zh") == 0
    low = jnp.where(first, mine[...], theirs[...])
    high = jnp.where(first, theirs[...], mine[...])
    with_list(jnp.concatenate([low, high], axis=0), blk, 0, message)
    for q in range(NP):
        out[q] = message[...]


def read_list(table, q, listed):
    for j in range(CAP):
        table[q * CAP + j] = jnp.maximum(listed[:, j : j + 1].astype(jnp.int32)[0, 0], 0)


def h1_terms_kernel(blk, w0, h, values, w_slots, w_own, out, rows):
    out[:, :96, :] = jnp.zeros((NH, 96, COLS), jnp.float32)
    for j in range(CAP):
        at = pl.multiple_of(block_of(blk, 0, j) * BS, BS)
        for q in range(NP):
            w_slots[j, 4 * q : 4 * q + 4, :] = w0[q, :, pl.ds(at, BS)]
        upper, gram = grams(w_slots[j], both_of(values, j), live_of(blk, j))
        gram = jnp.concatenate([gram[:32], gram[32:]], axis=1)
        for side in range(2):
            q = 2 * block_of(blk, 1, j) + side
            out[q, :64, :] = out[q, :64, :] + upper[:, COLS * side : COLS * (side + 1)]
            out[q, 64:96, :] = out[q, 64:96, :] + gram
    lane = lax.broadcasted_iota(jnp.int32, (4, COLS), 1)
    listed = jnp.where(lane == 0, blk[CAP], blk[CAP + 1]).astype(jnp.float32)
    for q in range(NH):
        out[q, 96:100, :] = h[:, COLS * q : COLS * (q + 1)]
        out[q, 100:104, :] = listed
    plane = lax.axis_index(PLANE)
    for b in range(NB):
        w_own[b] = w0[plane, :, b * BS : (b + 1) * BS]
    for q in range(NP):
        read_list(rows, q, w0[q, 0:1, NB * BS :])


def h1_collect_kernel(got, out, cols):
    total = got[0, :96, :]
    for q in range(1, NH):
        total = total + got[q, :96, :]
    out[:96, :] = total
    for q in range(NH):
        out[96 + 4 * q : 100 + 4 * q, :] = got[q, 96:100, :]
        read_list(cols, q, got[q, 100:101, :])


def h1_update_kernel(mine, theirs, out):
    total = mine[:96, :] + theirs[:96, :]
    gram = jnp.concatenate([total[64:, :64], total[64:, 64:]], axis=0)
    first = lax.axis_index("z4") == 0
    low = jnp.where(first, mine[96:, :], theirs[96:, :])
    high = jnp.where(first, theirs[96:, :], mine[96:, :])
    pairs = []
    for k in range(16):
        pairs += [low[2 * k : 2 * k + 2], high[2 * k : 2 * k + 2]]
    old = jnp.concatenate(pairs, axis=0)
    new = old * total[:64] / product(halves(gram), halves(old))
    for q in range(NQ):
        out[q] = new


def whole_block(h_all, b):
    return jnp.concatenate([h_all[0, b], h_all[1, b]], axis=1)


def send_w(out, j, upper, lower):
    for q in range(NP):
        out[q, 8 * j : 8 * j + 4, :] = upper[4 * q : 4 * q + 4, :]
        out[q, 8 * j + 4 : 8 * j + 8, :] = lower[4 * q : 4 * q + 4, :]


def w1_terms_kernel(blk, h_all, w_slots, values, out):
    for j in range(CAP):
        h_slot = whole_block(h_all, block_of(blk, 1, j))
        send_w(out, j, *sums(h_slot, w_slots[j], both_of(values, j), live_of(blk, j)))


def w2_terms_kernel(blk, h_got, w_slots, values, out):
    for j in range(CAP):
        h_slot = h_got[:, 8 * j : 8 * j + 8, :].reshape(RANK, BS)
        send_w(out, j, *sums(h_slot, w_slots[j], both_of(values, j), live_of(blk, j)))


def w_slot(got, j):
    return jnp.concatenate([got[q, 4 * j : 4 * j + 4, :] for q in range(NP)], axis=0)


def h2_terms_kernel(blk, w_got, values, w_slots, out):
    both = []
    for j in range(CAP):
        w_slots[j] = w_slot(w_got, j)
        upper, gram = grams(w_slots[j], both_of(values, j), live_of(blk, j))
        both.append(gram)
        for q in range(NH):
            out[q, :, BS * j : BS * (j + 1)] = upper[8 * q : 8 * q + 8, :]
    both = jnp.concatenate(both, axis=1)
    for q in range(NH):
        out[q, :, CAP * BS :] = both[8 * q : 8 * q + 8, :]


def h2_collect_kernel(table, got, out):
    out[...] = jnp.zeros(out.shape, out.dtype)
    lane = lax.broadcasted_iota(jnp.int32, (8, CAP * RANK), 1)
    for q in range(NH):
        gram = got[q, :, CAP * BS :]
        for j in range(CAP):
            b = table[q * CAP + j]
            out[b, :, :BS] = out[b, :, :BS] + got[q, :, BS * j : BS * (j + 1)]
            out[b, :, BS:] = out[b, :, BS:] + jnp.where(lane // RANK == j, gram, 0.0)


def h2_update_kernel(table, h_all, mine, theirs, final, out, new):
    half = lax.axis_index(HALF)
    first = lax.axis_index("z4") == 0
    for b in range(NB):
        total = mine[b] + theirs[b]
        gram = total[:, BS:]
        high = gram.astype(jnp.bfloat16).astype(jnp.float32)
        gram = jnp.concatenate([high, gram - high], axis=0).astype(jnp.bfloat16)
        block = whole_block(h_all, b)
        block = halves(jnp.concatenate([block, block], axis=0))
        most = lax.dot_general(gram, block[0], NN, preferred_element_type=jnp.float32)
        rest = lax.dot_general(gram, block[1], NN, preferred_element_type=jnp.float32)
        lower = most[:8] + (most[8:] + rest[:8])
        at = pl.multiple_of(8 * half, 8)
        own = jnp.concatenate([h_all[0, b, pl.ds(at, 8), :], h_all[1, b, pl.ds(at, 8), :]], axis=1)
        rows = own * total[:, :BS] / lower
        new[b] = rows
        for high in range(2):
            pair = rows[4 * high : 4 * high + 4]
            final[2 * high : 2 * high + 2, b * BS : (b + 1) * BS] = jnp.where(first, pair[0:2], pair[2:4])
    for q in range(NH):
        for j in range(CAP):
            out[q, 8 * j : 8 * (j + 1), :] = new[table[q * CAP + j]]


def collect_kernel(table, got, out):
    rows = out.shape[1]
    out[...] = jnp.zeros(out.shape, out.dtype)
    for q in range(got.shape[0]):
        for j in range(CAP):
            b = table[q * CAP + j]
            out[b] = out[b] + got[q, rows * j : rows * (j + 1), :]


def updated(own, mine, theirs):
    rows = own.shape[1]
    upper = mine[:, :rows, :] + theirs[:, :rows, :]
    lower = mine[:, rows:, :] + theirs[:, rows:, :]
    return own[...] * upper / lower


def update_kernel(table, own, mine, theirs, new, out):
    rows = own.shape[1]
    new[...] = updated(own, mine, theirs)
    for q in range(out.shape[0]):
        for j in range(CAP):
            out[q, rows * j : rows * (j + 1), :] = new[table[q * CAP + j]]


def last_w_kernel(own, mine, theirs, final, new):
    new[...] = updated(own, mine, theirs)
    first = lax.axis_index("zh") == 0
    for b in range(NB):
        final[:, b * BS : (b + 1) * BS] = jnp.where(first, new[b, 0:2, :], new[b, 2:4, :])


def call(body, scalars, arrays, outs, tables=(), scratch=(), last=False, dtypes=None):
    smem = pl.BlockSpec(memory_space=pltpu.SMEM)
    vmem = pl.BlockSpec(memory_space=pltpu.VMEM)
    kind = jax.ShapeDtypeStruct if last else pltpu.VMEM
    return pl.pallas_call(
        body,
        in_specs=[smem] * len(scalars) + [vmem] * len(arrays),
        out_specs=[vmem] * len(outs) + [smem] * len(tables),
        out_shape=[kind(*s) for s in zip(outs, dtypes or [jnp.float32] * len(outs))] + [pltpu.SMEM(s, jnp.int32) for s in tables],
        scratch_shapes=[pltpu.VMEM(s, jnp.float32) for s in scratch],
    )(
        *(pltpu.with_memory_space_constraint(a, pltpu.SMEM) for a in scalars),
        *(pltpu.with_memory_space_constraint(a, pltpu.VMEM) for a in arrays),
    )


def per_device(blocks, observed, w_factor, h_factor):
    wide = NB * BS + TAB

    w_other = swap(w_factor, "zh")
    values, turned, w_mine, blk = call(
        prepare_kernel,
        (blocks[0, 0],),
        (observed[0, 0], w_factor),
        [(CAP, 2, BS, BS), (CAP, 2, BS, BS), w_factor.shape],
        dtypes=[jnp.bfloat16, jnp.bfloat16, jnp.float32],
        tables=[(2 * CAP,)],
    )
    (w_pair,) = call(w_pair_kernel, (blk,), (w_mine, w_other), [(NP, 4, wide)], scratch=[(4, wide)])
    w_got = exchange(w_pair, PLANE)

    w_slots, w_own, sent, rows = call(
        h1_terms_kernel,
        (blk,),
        (w_got, h_factor, values),
        [(CAP, RANK, BS), (NB, 4, BS), (NH, 104, COLS)],
        tables=[(NP * CAP,)],
    )
    got = exchange(sent, HALF)
    mine, cols = call(h1_collect_kernel, (), (got,), [(128, COLS)], tables=[(NH * CAP,)])
    theirs = swap(mine, "z4")
    (out,) = call(h1_update_kernel, (), (mine, theirs), [(NQ, RANK, COLS)])
    h_all = lax.all_gather(exchange(out, QUAD), "core", axis=0)

    (sent,) = call(w1_terms_kernel, (blk,), (h_all, w_slots, turned), [(NP, 16, BS)])
    got = exchange(sent, PLANE)
    (mine,) = call(collect_kernel, (rows,), (got,), [(NB, 8, BS)])
    theirs = swap(mine, "zh")
    w_own, out = call(update_kernel, (rows,), (w_own, mine, theirs), [(NB, 4, BS), (NP, 8, BS)])
    w_got = exchange(out, PLANE)

    w_slots, sent = call(h2_terms_kernel, (blk,), (w_got, values), [(CAP, RANK, BS), (NH, 8, CAP * (BS + RANK))])
    got = exchange(sent, HALF)
    (mine,) = call(h2_collect_kernel, (cols,), (got,), [(NB, 8, BS + CAP * RANK)])
    theirs = swap(mine, "z4")
    h_final, out = call(
        h2_update_kernel, (cols,), (h_all, mine, theirs), [(4, NB * BS), (NH, 16, BS)], scratch=[(NB, 8, BS)]
    )
    h_got = exchange(out, HALF)

    (sent,) = call(w2_terms_kernel, (blk,), (h_got, w_slots, turned), [(NP, 16, BS)])
    got = exchange(sent, PLANE)
    (mine,) = call(collect_kernel, (rows,), (got,), [(NB, 8, BS)])
    theirs = swap(mine, "zh")
    (w_final,) = call(last_w_kernel, (), (w_own, mine, theirs), [(2, NB * BS)], scratch=[(NB, 4, BS)], last=True)
    return w_final, h_final


def solution(mesh):
    fine = Mesh(mesh.devices.reshape(2, 2, 2, 2, 2, 4, 4), FINE)
    tex = ("z4",) + HALF
    smp = ("zh",) + PLANE
    in_specs = (P(tex, smp, None, None), P(tex, smp, None, None), P(smp, tex), P(tex, smp))
    out_specs = (P(smp, tex), P(tex, smp))
    return jax.shard_map(per_device, mesh=fine, in_specs=in_specs, out_specs=out_specs, check_vma=False)
```

```python
import jax
import jax.numpy as jnp
from jax import lax
from jax.experimental import pallas as pl
from jax.experimental.pallas import tpu as pltpu
from jax.sharding import Mesh, PartitionSpec as P


RANK = 64
BS = 256
CAP = 2
NB = 4
TAB = 128

FINE = ("z4", "z2", "z1", "core", "zh", "y", "x")
HALF = ("z2", "z1", "core")
QUAD = ("z2", "z1")
PLANE = ("y", "x")
NH = 8
NQ = 4
COLS = NB * BS // NH
NP = 16

NN = (((1,), (0,)), ((), ()))
NT = (((1,), (1,)), ((), ()))


def exchange(x, axes):
    return lax.all_to_all(x, axes, split_axis=0, concat_axis=0, tiled=True)


def swap(x, axis):
    return lax.ppermute(x, axis, [(0, 1), (1, 0)])


def halves(x):
    hi = x.astype(jnp.bfloat16)
    lo = (x - hi.astype(jnp.float32)).astype(jnp.bfloat16)
    return hi, lo


def product(a, b, dims=NN):
    dot = lambda x, y: lax.dot_general(x, y, dims, preferred_element_type=jnp.float32)
    return dot(a[0], b[0]) + (dot(a[0], b[1]) + dot(a[1], b[0]))


def grams(left, values, live):
    whole = halves(left)
    left = halves(left * live)
    return product(left, values), product(left, whole, NT)


def sums(left, right, values, live):
    upper, gram = grams(left, values, live)
    return upper, product(halves(gram), halves(right))


def prepare_kernel(blk, values, w, parts, turned, w_mine, listed):
    for d in range(2):
        for j in range(CAP):
            listed[CAP * d + j] = blk[d, j]
    w_mine[...] = w[...]
    for j in range(CAP):
        block = values[j * BS : (j + 1) * BS, :]
        parts[j, 0], parts[j, 1] = halves(block)
        turned[j, 0], turned[j, 1] = halves(block.T)


def both_of(parts, j):
    return parts[j, 0], parts[j, 1]


def live_of(blk, j):
    return jnp.where(blk[j] >= 0, 1.0, 0.0).astype(jnp.float32)


def block_of(blk, d, j):
    return jnp.maximum(blk[CAP * d + j], 0)


def with_list(rows, blk, d, lists):
    lane = lax.broadcasted_iota(jnp.int32, (rows.shape[0], TAB), 1)
    lists[:, : NB * BS] = rows
    lists[:, NB * BS :] = jnp.where(lane == 0, blk[CAP * d], blk[CAP * d + 1]).astype(jnp.float32)


def w_pair_kernel(blk, mine, theirs, out, message):
    first = lax.axis_index("zh") == 0
    low = jnp.where(first, mine[...], theirs[...])
    high = jnp.where(first, theirs[...], mine[...])
    with_list(jnp.concatenate([low, high], axis=0), blk, 0, message)
    for q in range(NP):
        out[q] = message[...]


def read_list(table, q, listed):
    for j in range(CAP):
        table[q * CAP + j] = jnp.maximum(listed[:, j : j + 1].astype(jnp.int32)[0, 0], 0)


def h1_terms_kernel(blk, w0, h, values, w_own, out, rows, w_slots):
    out[:, :96, :] = jnp.zeros((NH, 96, COLS), jnp.float32)
    for j in range(CAP):
        at = pl.multiple_of(block_of(blk, 0, j) * BS, BS)
        for q in range(NP):
            w_slots[j, 4 * q : 4 * q + 4, :] = w0[q, :, pl.ds(at, BS)]
        upper, gram = grams(w_slots[j], both_of(values, j), live_of(blk, j))
        gram = jnp.concatenate([gram[:32], gram[32:]], axis=1)
        for side in range(2):
            q = 2 * block_of(blk, 1, j) + side
            out[q, :64, :] = out[q, :64, :] + upper[:, COLS * side : COLS * (side + 1)]
            out[q, 64:96, :] = out[q, 64:96, :] + gram
    lane = lax.broadcasted_iota(jnp.int32, (4, COLS), 1)
    listed = jnp.where(lane == 0, blk[CAP], blk[CAP + 1]).astype(jnp.float32)
    for q in range(NH):
        out[q, 96:100, :] = h[:, COLS * q : COLS * (q + 1)]
        out[q, 100:104, :] = listed
    plane = lax.axis_index(PLANE)
    for b in range(NB):
        w_own[b] = w0[plane, :, b * BS : (b + 1) * BS]
    for q in range(NP):
        read_list(rows, q, w0[q, 0:1, NB * BS :])


def h1_collect_kernel(got, out, cols):
    total = got[0, :96, :]
    for q in range(1, NH):
        total = total + got[q, :96, :]
    out[:96, :] = total
    for q in range(NH):
        out[96 + 4 * q : 100 + 4 * q, :] = got[q, 96:100, :]
        read_list(cols, q, got[q, 100:101, :])


def h1_update_kernel(mine, theirs, out):
    total = mine[:96, :] + theirs[:96, :]
    gram = jnp.concatenate([total[64:, :64], total[64:, 64:]], axis=0)
    first = lax.axis_index("z4") == 0
    low = jnp.where(first, mine[96:, :], theirs[96:, :])
    high = jnp.where(first, theirs[96:, :], mine[96:, :])
    pairs = []
    for k in range(16):
        pairs += [low[2 * k : 2 * k + 2], high[2 * k : 2 * k + 2]]
    old = jnp.concatenate(pairs, axis=0)
    new = old * total[:64] / product(halves(gram), halves(old))
    for q in range(NQ):
        out[q] = new


def whole_block(h_all, b):
    return jnp.concatenate([h_all[0, b], h_all[1, b]], axis=1)


def send_w(out, j, upper, lower):
    for q in range(NP):
        out[q, 8 * j : 8 * j + 4, :] = upper[4 * q : 4 * q + 4, :]
        out[q, 8 * j + 4 : 8 * j + 8, :] = lower[4 * q : 4 * q + 4, :]


def send_grams(out, terms):
    rows = out.shape[1]
    both = jnp.concatenate([gram for _, gram in terms], axis=1)
    for q in range(out.shape[0]):
        for j in range(CAP):
            out[q, :, BS * j : BS * (j + 1)] = terms[j][0][rows * q : rows * (q + 1), :]
        out[q, :, CAP * BS :] = both[rows * q : rows * (q + 1), :]


def w1_terms_kernel(blk, h_all, values, out):
    terms = []
    for j in range(CAP):
        h_slot = whole_block(h_all, block_of(blk, 1, j))
        terms.append(grams(h_slot, both_of(values, j), live_of(blk, j)))
    send_grams(out, terms)


def w2_terms_kernel(blk, h_got, w_slots, values, out):
    for j in range(CAP):
        h_slot = h_got[:, 8 * j : 8 * j + 8, :].reshape(RANK, BS)
        send_w(out, j, *sums(h_slot, w_slots[j], both_of(values, j), live_of(blk, j)))


def w_slot(got, j):
    return jnp.concatenate([got[q, 4 * j : 4 * j + 4, :] for q in range(NP)], axis=0)


def h2_terms_kernel(blk, w_got, values, w_slots, out):
    terms = []
    for j in range(CAP):
        w_slots[j] = w_slot(w_got, j)
        terms.append(grams(w_slots[j], both_of(values, j), live_of(blk, j)))
    send_grams(out, terms)


def gram_collect_kernel(table, got, out):
    rows = out.shape[1]
    out[...] = jnp.zeros(out.shape, out.dtype)
    half = lax.broadcasted_iota(jnp.int32, (rows, CAP * RANK), 1) // RANK
    for q in range(got.shape[0]):
        grams = got[q, :, CAP * BS :]
        turned = jnp.concatenate([grams[:, RANK:], grams[:, :RANK]], axis=1)
        for j in range(CAP):
            b = table[q * CAP + j]
            out[b] = out[b] + got[q, :, BS * j : BS * (j + 1)]
            side = b % 2
            at = pl.ds(pl.multiple_of(b // 2 * CAP * RANK, CAP * RANK), CAP * RANK)
            mine = jnp.where(side == j, grams, turned)
            out[NB, :, at] = out[NB, :, at] + jnp.where(half == side, mine, 0.0)


def owned(own, whole, mine, theirs, b):
    rows = own.shape[0]
    gram = mine[NB, :, RANK * b : RANK * (b + 1)] + theirs[NB, :, RANK * b : RANK * (b + 1)]
    high = gram.astype(jnp.bfloat16).astype(jnp.float32)
    gram = jnp.concatenate([high, gram - high], axis=0).astype(jnp.bfloat16)
    whole = halves(whole)
    most = lax.dot_general(gram, whole[0], NN, preferred_element_type=jnp.float32)
    rest = lax.dot_general(gram, whole[1], NN, preferred_element_type=jnp.float32)
    return own * (mine[b] + theirs[b]) / (most[:rows] + (most[rows:] + rest[:rows]))


def w_arrange_kernel(w0, w_all):
    for b in range(NB):
        for q in range(NP):
            w_all[b, 4 * q : 4 * q + 4, :] = w0[q, :, b * BS : (b + 1) * BS]


def w1_update_kernel(table, own, w_all, mine, theirs, new, out):
    for b in range(NB):
        new[b] = owned(own[b], w_all[b], mine, theirs, b)
    for q in range(NP):
        for j in range(CAP):
            out[q, 4 * j : 4 * (j + 1), :] = new[table[q * CAP + j]]


def h2_update_kernel(table, h_all, mine, theirs, final, out, new):
    first = lax.axis_index("z4") == 0
    at = pl.ds(pl.multiple_of(8 * lax.axis_index(HALF), 8), 8)
    for b in range(NB):
        own = jnp.concatenate([h_all[0, b, at, :], h_all[1, b, at, :]], axis=1)
        rows = owned(own, whole_block(h_all, b), mine, theirs, b)
        new[b] = rows
        for high in range(2):
            pair = rows[4 * high : 4 * high + 4]
            final[2 * high : 2 * high + 2, b * BS : (b + 1) * BS] = jnp.where(first, pair[0:2], pair[2:4])
    for q in range(NH):
        for j in range(CAP):
            out[q, 8 * j : 8 * (j + 1), :] = new[table[q * CAP + j]]


def w2_collect_kernel(table, got, mine, out, total):
    total[...] = jnp.zeros(total.shape, total.dtype)
    for q in range(NP):
        for j in range(CAP):
            b = table[q * CAP + j]
            total[b] = total[b] + got[q, 8 * j : 8 * (j + 1), :]
    first = lax.axis_index("zh") == 0
    for b in range(NB):
        low = jnp.concatenate([total[b, 0:2, :], total[b, 4:6, :]], axis=0)
        high = jnp.concatenate([total[b, 2:4, :], total[b, 6:8, :]], axis=0)
        mine[b] = jnp.where(first, low, high)
        out[b] = jnp.where(first, high, low)


def last_w_kernel(own, mine, theirs, final):
    first = lax.axis_index("zh") == 0
    for b in range(NB):
        total = mine[b] + theirs[b]
        rows = jnp.where(first, own[b, 0:2, :], own[b, 2:4, :])
        final[:, b * BS : (b + 1) * BS] = rows * total[0:2] / total[2:4]


def call(body, scalars, arrays, outs, tables=(), scratch=(), last=False, dtypes=None):
    smem = pl.BlockSpec(memory_space=pltpu.SMEM)
    vmem = pl.BlockSpec(memory_space=pltpu.VMEM)
    kind = jax.ShapeDtypeStruct if last else pltpu.VMEM
    return pl.pallas_call(
        body,
        in_specs=[smem] * len(scalars) + [vmem] * len(arrays),
        out_specs=[vmem] * len(outs) + [smem] * len(tables),
        out_shape=[kind(*s) for s in zip(outs, dtypes or [jnp.float32] * len(outs))] + [pltpu.SMEM(s, jnp.int32) for s in tables],
        scratch_shapes=[pltpu.VMEM(s, jnp.float32) for s in scratch],
    )(
        *(pltpu.with_memory_space_constraint(a, pltpu.SMEM) for a in scalars),
        *(pltpu.with_memory_space_constraint(a, pltpu.VMEM) for a in arrays),
    )


def per_device(blocks, observed, w_factor, h_factor):
    wide = NB * BS + TAB

    w_other = swap(w_factor, "zh")
    values, turned, w_mine, blk = call(
        prepare_kernel,
        (blocks[0, 0],),
        (observed[0, 0], w_factor),
        [(CAP, 2, BS, BS), (CAP, 2, BS, BS), w_factor.shape],
        dtypes=[jnp.bfloat16, jnp.bfloat16, jnp.float32],
        tables=[(2 * CAP,)],
    )
    (w_pair,) = call(w_pair_kernel, (blk,), (w_mine, w_other), [(NP, 4, wide)], scratch=[(4, wide)])
    w_got = exchange(w_pair, PLANE)

    w_own, sent, rows = call(
        h1_terms_kernel,
        (blk,),
        (w_got, h_factor, values),
        [(NB, 4, BS), (NH, 104, COLS)],
        tables=[(NP * CAP,)],
        scratch=[(CAP, RANK, BS)],
    )
    got = exchange(sent, HALF)
    mine, cols = call(h1_collect_kernel, (), (got,), [(128, COLS)], tables=[(NH * CAP,)])
    theirs = swap(mine, "z4")
    (w_all,) = call(w_arrange_kernel, (), (w_got,), [(NB, RANK, BS)])
    (out,) = call(h1_update_kernel, (), (mine, theirs), [(NQ, RANK, COLS)])
    h_all = lax.all_gather(exchange(out, QUAD), "core", axis=0)

    wide = CAP * (BS + RANK)
    (sent,) = call(w1_terms_kernel, (blk,), (h_all, turned), [(NP, 4, wide)])
    got = exchange(sent, PLANE)
    (mine,) = call(gram_collect_kernel, (rows,), (got,), [(NB + 1, 4, BS)])
    theirs = swap(mine, "zh")
    w_own, out = call(w1_update_kernel, (rows,), (w_own, w_all, mine, theirs), [(NB, 4, BS), (NP, 8, BS)])
    w_got = exchange(out, PLANE)

    w_slots, sent = call(h2_terms_kernel, (blk,), (w_got, values), [(CAP, RANK, BS), (NH, 8, wide)])
    got = exchange(sent, HALF)
    (mine,) = call(gram_collect_kernel, (cols,), (got,), [(NB + 1, 8, BS)])
    theirs = swap(mine, "z4")
    h_final, out = call(
        h2_update_kernel, (cols,), (h_all, mine, theirs), [(4, NB * BS), (NH, 16, BS)], scratch=[(NB, 8, BS)]
    )
    h_got = exchange(out, HALF)

    (sent,) = call(w2_terms_kernel, (blk,), (h_got, w_slots, turned), [(NP, 16, BS)])
    got = exchange(sent, PLANE)
    mine, out = call(w2_collect_kernel, (rows,), (got,), [(NB, 4, BS), (NB, 4, BS)], scratch=[(NB, 8, BS)])
    theirs = swap(out, "zh")
    (w_final,) = call(last_w_kernel, (), (w_own, mine, theirs), [(2, NB * BS)], last=True)
    return w_final, h_final


def solution(mesh):
    fine = Mesh(mesh.devices.reshape(2, 2, 2, 2, 2, 4, 4), FINE)
    tex = ("z4",) + HALF
    smp = ("zh",) + PLANE
    in_specs = (P(tex, smp, None, None), P(tex, smp, None, None), P(smp, tex), P(tex, smp))
    out_specs = (P(smp, tex), P(tex, smp))
    return jax.shard_map(per_device, mesh=fine, in_specs=in_specs, out_specs=out_specs, check_vma=False)
```

```python
import jax
import jax.numpy as jnp
from jax import lax
from jax.experimental import pallas as pl
from jax.experimental.pallas import tpu as pltpu
from jax.sharding import Mesh, PartitionSpec as P


RANK = 64
BS = 256
CAP = 2
NB = 4
TAB = 128

FINE = ("z4", "z2", "z1", "core", "zh", "y", "x")
HALF = ("z2", "z1", "core")
QUAD = ("z2", "z1")
PLANE = ("y", "x")
NH = 8
NQ = 4
COLS = NB * BS // NH
NP = 16

NN = (((1,), (0,)), ((), ()))
NT = (((1,), (1,)), ((), ()))


def exchange(x, axes):
    return lax.all_to_all(x, axes, split_axis=0, concat_axis=0, tiled=True)


def swap(x, axis):
    return lax.ppermute(x, axis, [(0, 1), (1, 0)])


def halves(x):
    hi = x.astype(jnp.bfloat16)
    lo = (x - hi.astype(jnp.float32)).astype(jnp.bfloat16)
    return hi, lo


def product(a, b, dims=NN):
    dot = lambda x, y: lax.dot_general(x, y, dims, preferred_element_type=jnp.float32)
    return dot(a[0], b[0]) + (dot(a[0], b[1]) + dot(a[1], b[0]))


def grams(left, values, live):
    whole = halves(left)
    left = halves(left * live)
    return product(left, values), product(left, whole, NT)


def prepare_kernel(blk, values, w, parts, turned, w_mine, listed):
    for d in range(2):
        for j in range(CAP):
            listed[CAP * d + j] = blk[d, j]
    w_mine[...] = w[...]
    for j in range(CAP):
        block = values[j * BS : (j + 1) * BS, :]
        parts[j, 0], parts[j, 1] = halves(block)
        turned[j, 0], turned[j, 1] = halves(block.T)


def both_of(parts, j):
    return parts[j, 0], parts[j, 1]


def live_of(blk, j):
    return jnp.where(blk[j] >= 0, 1.0, 0.0).astype(jnp.float32)


def block_of(blk, d, j):
    return jnp.maximum(blk[CAP * d + j], 0)


def with_list(rows, blk, d, lists):
    lane = lax.broadcasted_iota(jnp.int32, (rows.shape[0], TAB), 1)
    lists[:, : NB * BS] = rows
    lists[:, NB * BS :] = jnp.where(lane == 0, blk[CAP * d], blk[CAP * d + 1]).astype(jnp.float32)


def w_pair_kernel(blk, mine, theirs, out, message):
    first = lax.axis_index("zh") == 0
    low = jnp.where(first, mine[...], theirs[...])
    high = jnp.where(first, theirs[...], mine[...])
    with_list(jnp.concatenate([low, high], axis=0), blk, 0, message)
    for q in range(NP):
        out[q] = message[...]


def read_list(table, q, listed):
    for j in range(CAP):
        table[q * CAP + j] = jnp.maximum(listed[:, j : j + 1].astype(jnp.int32)[0, 0], 0)


def w_slot(w_got, j, blk, w_slots):
    at = pl.multiple_of(block_of(blk, 0, j) * BS, BS)
    for q in range(NP):
        w_slots[j, 4 * q : 4 * q + 4, :] = w_got[q, :, pl.ds(at, BS)]
    return w_slots[j]


def h1_terms_kernel(blk, w0, h, values, w_own, out, rows, w_slots):
    for j in range(CAP):
        upper, gram = grams(w_slot(w0, j, blk, w_slots), both_of(values, j), live_of(blk, j))
        for side in range(2):
            at = 128 * j + RANK * side
            out[at : at + RANK, :] = upper[:, COLS * side : COLS * (side + 1)]
        out[256 + 32 * j : 288 + 32 * j, :] = jnp.concatenate([gram[:32], gram[32:]], axis=1)
    for q in range(NH):
        at = 320 + 16 * (q % 2) + 4 * (q // 2)
        out[at : at + 4, :] = h[:, COLS * q : COLS * (q + 1)]
    lane = lax.broadcasted_iota(jnp.int32, (8, COLS), 1)
    out[352:360, :] = jnp.where(lane == 0, blk[CAP], blk[CAP + 1]).astype(jnp.float32)
    plane = lax.axis_index(PLANE)
    for b in range(NB):
        w_own[b] = w0[plane, :, b * BS : (b + 1) * BS]
    for q in range(NP):
        read_list(rows, q, w0[q, 0:1, NB * BS :])


def h1_build_kernel(pair, out, lists):
    core = lax.axis_index("core")
    out[:, :96, :] = jnp.zeros((NQ, 96, COLS), jnp.float32)
    for i in range(2):
        read_list(lists, i, pair[i, 352:353, :])
        for j in range(CAP):
            q = lists[CAP * i + j]
            at = pl.multiple_of(128 * j + RANK * core, 8)
            out[q, :64, :] = out[q, :64, :] + pair[i, pl.ds(at, RANK), :]
            out[q, 64:96, :] = out[q, 64:96, :] + pair[i, 256 + 32 * j : 288 + 32 * j, :]
        side = pair[i, pl.ds(pl.multiple_of(320 + 16 * core, 8), 16), :]
        for q in range(NQ):
            out[q, 96 + 4 * i : 100 + 4 * i, :] = side[4 * q : 4 * q + 4]
            out[q, 104 + 4 * i : 108 + 4 * i, :] = pair[i, 352:356, :]


def h1_collect_kernel(got, out, cols):
    total = got[0, :96, :]
    for q in range(1, NQ):
        total = total + got[q, :96, :]
    out[:96, :] = total
    for q in range(NQ):
        out[96 + 8 * q : 104 + 8 * q, :] = got[q, 96:104, :]
        for i in range(2):
            read_list(cols, 2 * q + i, got[q, 104 + 4 * i : 105 + 4 * i, :])


def h1_update_kernel(mine, theirs, out):
    total = mine[:96, :] + theirs[:96, :]
    gram = jnp.concatenate([total[64:, :64], total[64:, 64:]], axis=0)
    first = lax.axis_index("z4") == 0
    low = jnp.where(first, mine[96:, :], theirs[96:, :])
    high = jnp.where(first, theirs[96:, :], mine[96:, :])
    pairs = []
    for k in range(16):
        pairs += [low[2 * k : 2 * k + 2], high[2 * k : 2 * k + 2]]
    old = jnp.concatenate(pairs, axis=0)
    new = old * total[:64] / product(halves(gram), halves(old))
    for q in range(NQ):
        out[q] = new


def whole_block(h_all, b):
    return jnp.concatenate([h_all[0, b], h_all[1, b]], axis=1)


def send_grams(out, terms):
    rows = out.shape[1]
    both = jnp.concatenate([gram for _, gram in terms], axis=1)
    for q in range(out.shape[0]):
        for j in range(CAP):
            out[q, :, BS * j : BS * (j + 1)] = terms[j][0][rows * q : rows * (q + 1), :]
        out[q, :, CAP * BS :] = both[rows * q : rows * (q + 1), :]


def w1_terms_kernel(blk, h_all, values, out):
    terms = []
    for j in range(CAP):
        h_slot = whole_block(h_all, block_of(blk, 1, j))
        terms.append(grams(h_slot, both_of(values, j), live_of(blk, j)))
    send_grams(out, terms)


def w2_terms_kernel(blk, h_got, values, out):
    terms = []
    for j in range(CAP):
        h_slot = h_got[:, 8 * j : 8 * j + 8, :].reshape(RANK, BS)
        terms.append(grams(h_slot, both_of(values, j), live_of(blk, j)))
    send_grams(out, terms)


def h2_terms_kernel(blk, w_got, values, out, w_slots):
    terms = []
    for j in range(CAP):
        terms.append(grams(w_slot(w_got, j, blk, w_slots), both_of(values, j), live_of(blk, j)))
    send_grams(out, terms)


def gram_collect_kernel(table, got, out):
    rows = out.shape[1]
    out[...] = jnp.zeros(out.shape, out.dtype)
    half = lax.broadcasted_iota(jnp.int32, (rows, CAP * RANK), 1) // RANK
    for q in range(got.shape[0]):
        grams = got[q, :, CAP * BS :]
        turned = jnp.concatenate([grams[:, RANK:], grams[:, :RANK]], axis=1)
        for j in range(CAP):
            b = table[q * CAP + j]
            out[b] = out[b] + got[q, :, BS * j : BS * (j + 1)]
            side = b % 2
            at = pl.ds(pl.multiple_of(b // 2 * CAP * RANK, CAP * RANK), CAP * RANK)
            mine = jnp.where(side == j, grams, turned)
            out[NB, :, at] = out[NB, :, at] + jnp.where(half == side, mine, 0.0)


def owned(own, whole, mine, theirs, b):
    rows = own.shape[0]
    gram = mine[NB, :, RANK * b : RANK * (b + 1)] + theirs[NB, :, RANK * b : RANK * (b + 1)]
    high = gram.astype(jnp.bfloat16).astype(jnp.float32)
    gram = jnp.concatenate([high, gram - high], axis=0).astype(jnp.bfloat16)
    whole = halves(whole)
    most = lax.dot_general(gram, whole[0], NN, preferred_element_type=jnp.float32)
    rest = lax.dot_general(gram, whole[1], NN, preferred_element_type=jnp.float32)
    return own * (mine[b] + theirs[b]) / (most[:rows] + (most[rows:] + rest[:rows]))


def w_arrange_kernel(w0, w_all):
    for b in range(NB):
        for q in range(NP):
            w_all[b, 4 * q : 4 * q + 4, :] = w0[q, :, b * BS : (b + 1) * BS]


def w1_update_kernel(own, w_all, mine, theirs, new, out):
    for b in range(NB):
        rows = owned(own[b], w_all[b], mine, theirs, b)
        new[b] = rows
        for q in range(NP):
            out[q, :, b * BS : (b + 1) * BS] = rows


def h2_update_kernel(table, h_all, mine, theirs, final, out, new):
    first = lax.axis_index("z4") == 0
    at = pl.ds(pl.multiple_of(8 * lax.axis_index(HALF), 8), 8)
    for b in range(NB):
        own = jnp.concatenate([h_all[0, b, at, :], h_all[1, b, at, :]], axis=1)
        rows = owned(own, whole_block(h_all, b), mine, theirs, b)
        new[b] = rows
        for high in range(2):
            pair = rows[4 * high : 4 * high + 4]
            final[2 * high : 2 * high + 2, b * BS : (b + 1) * BS] = jnp.where(first, pair[0:2], pair[2:4])
    for q in range(NH):
        for j in range(CAP):
            out[q, 8 * j : 8 * (j + 1), :] = new[table[q * CAP + j]]


def w2_collect_kernel(table, got, mine, out, total):
    gram_collect_kernel(table, got, total)
    first = lax.axis_index("zh") == 0
    low, high = total[:, 0:2, :], total[:, 2:4, :]
    mine[...] = jnp.where(first, low, high)
    out[...] = jnp.where(first, high, low)


def last_w_kernel(own, w_all, mine, theirs, final):
    first = lax.axis_index("zh") == 0
    for b in range(NB):
        rows = jnp.where(first, own[b, 0:2, :], own[b, 2:4, :])
        final[:, b * BS : (b + 1) * BS] = owned(rows, w_all[b], mine, theirs, b)


def call(body, scalars, arrays, outs, tables=(), scratch=(), counts=(), last=False, dtypes=None):
    smem = pl.BlockSpec(memory_space=pltpu.SMEM)
    vmem = pl.BlockSpec(memory_space=pltpu.VMEM)
    kind = jax.ShapeDtypeStruct if last else pltpu.VMEM
    return pl.pallas_call(
        body,
        in_specs=[smem] * len(scalars) + [vmem] * len(arrays),
        out_specs=[vmem] * len(outs) + [smem] * len(tables),
        out_shape=[kind(*s) for s in zip(outs, dtypes or [jnp.float32] * len(outs))] + [pltpu.SMEM(s, jnp.int32) for s in tables],
        scratch_shapes=[pltpu.VMEM(s, jnp.float32) for s in scratch] + [pltpu.SMEM((n,), jnp.int32) for n in counts],
    )(
        *(pltpu.with_memory_space_constraint(a, pltpu.SMEM) for a in scalars),
        *(pltpu.with_memory_space_constraint(a, pltpu.VMEM) for a in arrays),
    )


def per_device(blocks, observed, w_factor, h_factor):
    wide = NB * BS + TAB

    w_other = swap(w_factor, "zh")
    values, turned, w_mine, blk = call(
        prepare_kernel,
        (blocks[0, 0],),
        (observed[0, 0], w_factor),
        [(CAP, 2, BS, BS), (CAP, 2, BS, BS), w_factor.shape],
        dtypes=[jnp.bfloat16, jnp.bfloat16, jnp.float32],
        tables=[(2 * CAP,)],
    )
    (w_pair,) = call(w_pair_kernel, (blk,), (w_mine, w_other), [(NP, 4, wide)], scratch=[(4, wide)])
    w_got = exchange(w_pair, PLANE)

    w_own, sent, rows = call(
        h1_terms_kernel,
        (blk,),
        (w_got, h_factor, values),
        [(NB, 4, BS), (360, COLS)],
        tables=[(NP * CAP,)],
        scratch=[(CAP, RANK, BS)],
    )
    pair = lax.all_gather(sent, "core", axis=0)
    (sent,) = call(h1_build_kernel, (), (pair,), [(NQ, 112, COLS)], counts=(2 * CAP,))
    got = exchange(sent, QUAD)
    mine, cols = call(h1_collect_kernel, (), (got,), [(128, COLS)], tables=[(NH * CAP,)])
    theirs = swap(mine, "z4")
    (w_all,) = call(w_arrange_kernel, (), (w_got,), [(NB, RANK, BS)])
    (out,) = call(h1_update_kernel, (), (mine, theirs), [(NQ, RANK, COLS)])
    h_all = lax.all_gather(exchange(out, QUAD), "core", axis=0)

    wide = CAP * (BS + RANK)
    (sent,) = call(w1_terms_kernel, (blk,), (h_all, turned), [(NP, 4, wide)])
    got = exchange(sent, PLANE)
    (mine,) = call(gram_collect_kernel, (rows,), (got,), [(NB + 1, 4, BS)])
    theirs = swap(mine, "zh")
    w_own, out = call(w1_update_kernel, (), (w_own, w_all, mine, theirs), [(NB, 4, BS), (NP, 4, NB * BS)])
    w_got = exchange(out, PLANE)

    (sent,) = call(h2_terms_kernel, (blk,), (w_got, values), [(NH, 8, wide)], scratch=[(CAP, RANK, BS)])
    got = exchange(sent, HALF)
    (mine,) = call(gram_collect_kernel, (cols,), (got,), [(NB + 1, 8, BS)])
    theirs = swap(mine, "z4")
    (w_all,) = call(w_arrange_kernel, (), (w_got,), [(NB, RANK, BS)])
    h_final, out = call(
        h2_update_kernel, (cols,), (h_all, mine, theirs), [(4, NB * BS), (NH, 16, BS)], scratch=[(NB, 8, BS)]
    )
    h_got = exchange(out, HALF)

    (sent,) = call(w2_terms_kernel, (blk,), (h_got, turned), [(NP, 4, wide)])
    got = exchange(sent, PLANE)
    mine, out = call(w2_collect_kernel, (rows,), (got,), [(NB + 1, 2, BS), (NB + 1, 2, BS)], scratch=[(NB + 1, 4, BS)])
    theirs = swap(out, "zh")
    (w_final,) = call(last_w_kernel, (), (w_own, w_all, mine, theirs), [(2, NB * BS)], last=True)
    return w_final, h_final


def solution(mesh):
    fine = Mesh(mesh.devices.reshape(2, 2, 2, 2, 2, 4, 4), FINE)
    tex = ("z4",) + HALF
    smp = ("zh",) + PLANE
    in_specs = (P(tex, smp, None, None), P(tex, smp, None, None), P(smp, tex), P(tex, smp))
    out_specs = (P(smp, tex), P(tex, smp))
    return jax.shard_map(per_device, mesh=fine, in_specs=in_specs, out_specs=out_specs, check_vma=False)
```

```python
import jax
import jax.numpy as jnp
from jax import lax
from jax.experimental import pallas as pl
from jax.experimental.pallas import tpu as pltpu
from jax.sharding import Mesh, PartitionSpec as P


RANK = 64
BS = 256
CAP = 2
NB = 4
TAB = 128

FINE = ("z4", "z2", "z1", "core", "zh", "y", "x")
HALF = ("z2", "z1", "core")
QUAD = ("z2", "z1")
PLANE = ("y", "x")
NH = 8
NQ = 4
COLS = NB * BS // NH
NP = 16

NN = (((1,), (0,)), ((), ()))
NT = (((1,), (1,)), ((), ()))


def exchange(x, axes):
    return lax.all_to_all(x, axes, split_axis=0, concat_axis=0, tiled=True)


def swap(x, axis):
    return lax.ppermute(x, axis, [(0, 1), (1, 0)])


def halves(x):
    hi = x.astype(jnp.bfloat16)
    lo = (x - hi.astype(jnp.float32)).astype(jnp.bfloat16)
    return hi, lo


def product(a, b, dims=NN):
    dot = lambda x, y: lax.dot_general(x, y, dims, preferred_element_type=jnp.float32)
    return dot(a[0], b[0]) + (dot(a[0], b[1]) + dot(a[1], b[0]))


def grams(left, values, live):
    whole = halves(left)
    left = halves(left * live)
    return product(left, values), product(left, whole, NT)


def prepare_kernel(blk, values, w, parts, turned, w_mine, listed):
    for d in range(2):
        for j in range(CAP):
            listed[CAP * d + j] = blk[d, j]
    w_mine[...] = w[...]
    for j in range(CAP):
        block = values[j * BS : (j + 1) * BS, :]
        parts[j, 0], parts[j, 1] = halves(block)
        turned[j, 0], turned[j, 1] = halves(block.T)


def both_of(parts, j):
    return parts[j, 0], parts[j, 1]


def live_of(blk, j):
    return jnp.where(blk[j] >= 0, 1.0, 0.0).astype(jnp.float32)


def block_of(blk, d, j):
    return jnp.maximum(blk[CAP * d + j], 0)


def with_list(rows, blk, d, lists):
    lane = lax.broadcasted_iota(jnp.int32, (rows.shape[0], TAB), 1)
    lists[:, : NB * BS] = rows
    lists[:, NB * BS :] = jnp.where(lane == 0, blk[CAP * d], blk[CAP * d + 1]).astype(jnp.float32)


def w_pair_kernel(blk, mine, theirs, out, message):
    first = lax.axis_index("zh") == 0
    low = jnp.where(first, mine[...], theirs[...])
    high = jnp.where(first, theirs[...], mine[...])
    with_list(jnp.concatenate([low, high], axis=0), blk, 0, message)
    for q in range(NP):
        out[q] = message[...]


def read_list(table, q, listed):
    for j in range(CAP):
        table[q * CAP + j] = jnp.maximum(listed[:, j : j + 1].astype(jnp.int32)[0, 0], 0)


def w_slot(w_got, j, blk, w_slots):
    at = pl.multiple_of(block_of(blk, 0, j) * BS, BS)
    for q in range(NP):
        w_slots[j, 4 * q : 4 * q + 4, :] = w_got[q, :, pl.ds(at, BS)]
    return w_slots[j]


def h1_terms_kernel(blk, w0, h, h_other, values, w_own, out, rows, w_slots):
    for j in range(CAP):
        upper, gram = grams(w_slot(w0, j, blk, w_slots), both_of(values, j), live_of(blk, j))
        for side in range(2):
            at = 128 * j + RANK * side
            out[at : at + RANK, :] = upper[:, COLS * side : COLS * (side + 1)]
        out[256 + 32 * j : 288 + 32 * j, :] = jnp.concatenate([gram[:32], gram[32:]], axis=1)
    first = lax.axis_index("z4") == 0
    low = jnp.where(first, h[...], h_other[...])
    high = jnp.where(first, h_other[...], h[...])
    old = jnp.concatenate([low[0:2], high[0:2], low[2:4], high[2:4]], axis=0)
    for q in range(NH):
        at = 320 + 32 * (q % 2) + 8 * (q // 2)
        out[at : at + 8, :] = old[:, COLS * q : COLS * (q + 1)]
    lane = lax.broadcasted_iota(jnp.int32, (8, COLS), 1)
    out[384:392, :] = jnp.where(lane == 0, blk[CAP], blk[CAP + 1]).astype(jnp.float32)
    plane = lax.axis_index(PLANE)
    for b in range(NB):
        w_own[b] = w0[plane, :, b * BS : (b + 1) * BS]
    for q in range(NP):
        read_list(rows, q, w0[q, 0:1, NB * BS :])


def h1_build_kernel(pair, out, lists):
    core = lax.axis_index("core")
    out[:, :96, :] = jnp.zeros((NQ, 96, COLS), jnp.float32)
    for i in range(2):
        read_list(lists, i, pair[i, 384:385, :])
        for j in range(CAP):
            q = lists[CAP * i + j]
            at = pl.multiple_of(128 * j + RANK * core, 8)
            out[q, :64, :] = out[q, :64, :] + pair[i, pl.ds(at, RANK), :]
            out[q, 64:96, :] = out[q, 64:96, :] + pair[i, 256 + 32 * j : 288 + 32 * j, :]
        side = pair[i, pl.ds(pl.multiple_of(320 + 32 * core, 8), 32), :]
        for q in range(NQ):
            out[q, 96 + 8 * i : 104 + 8 * i, :] = side[8 * q : 8 * q + 8]
            out[q, 112 + 4 * i : 116 + 4 * i, :] = pair[i, 384:388, :]


def h1_collect_kernel(got, out, old, cols):
    total = got[0, :96, :]
    for q in range(1, NQ):
        total = total + got[q, :96, :]
    out[...] = total
    for q in range(NQ):
        old[16 * q : 16 * q + 16, :] = got[q, 96:112, :]
        for i in range(2):
            read_list(cols, 2 * q + i, got[q, 112 + 4 * i : 113 + 4 * i, :])


def h1_update_kernel(mine, theirs, old, out):
    total = mine[...] + theirs[...]
    gram = jnp.concatenate([total[64:, :64], total[64:, 64:]], axis=0)
    new = old[...] * total[:64] / product(halves(gram), halves(old[...]))
    for q in range(NQ):
        out[q] = new


def whole_block(h_all, b):
    return jnp.concatenate([h_all[0, b], h_all[1, b]], axis=1)


def send_grams(out, terms):
    rows = out.shape[1]
    both = jnp.concatenate([gram for _, gram in terms], axis=1)
    for q in range(out.shape[0]):
        for j in range(CAP):
            out[q, :, BS * j : BS * (j + 1)] = terms[j][0][rows * q : rows * (q + 1), :]
        out[q, :, CAP * BS :] = both[rows * q : rows * (q + 1), :]


def w1_terms_kernel(blk, h_all, values, out):
    terms = []
    for j in range(CAP):
        h_slot = whole_block(h_all, block_of(blk, 1, j))
        terms.append(grams(h_slot, both_of(values, j), live_of(blk, j)))
    send_grams(out, terms)


def w2_terms_kernel(blk, h_got, values, out):
    terms = []
    for j in range(CAP):
        h_slot = h_got[:, 8 * j : 8 * j + 8, :].reshape(RANK, BS)
        terms.append(grams(h_slot, both_of(values, j), live_of(blk, j)))
    send_grams(out, terms)


def h2_terms_kernel(blk, w_got, values, out, w_slots):
    terms = []
    for j in range(CAP):
        terms.append(grams(w_slot(w_got, j, blk, w_slots), both_of(values, j), live_of(blk, j)))
    send_grams(out, terms)


def gram_collect_kernel(table, got, out):
    rows = out.shape[1]
    out[...] = jnp.zeros(out.shape, out.dtype)
    half = lax.broadcasted_iota(jnp.int32, (rows, CAP * RANK), 1) // RANK
    for q in range(got.shape[0]):
        grams = got[q, :, CAP * BS :]
        turned = jnp.concatenate([grams[:, RANK:], grams[:, :RANK]], axis=1)
        for j in range(CAP):
            b = table[q * CAP + j]
            out[b] = out[b] + got[q, :, BS * j : BS * (j + 1)]
            side = b % 2
            at = pl.ds(pl.multiple_of(b // 2 * CAP * RANK, CAP * RANK), CAP * RANK)
            mine = jnp.where(side == j, grams, turned)
            out[NB, :, at] = out[NB, :, at] + jnp.where(half == side, mine, 0.0)


def owned(own, whole, mine, theirs, b):
    rows = own.shape[0]
    gram = mine[NB, :, RANK * b : RANK * (b + 1)] + theirs[NB, :, RANK * b : RANK * (b + 1)]
    high = gram.astype(jnp.bfloat16).astype(jnp.float32)
    gram = jnp.concatenate([high, gram - high], axis=0).astype(jnp.bfloat16)
    whole = halves(whole)
    most = lax.dot_general(gram, whole[0], NN, preferred_element_type=jnp.float32)
    rest = lax.dot_general(gram, whole[1], NN, preferred_element_type=jnp.float32)
    return own * (mine[b] + theirs[b]) / (most[:rows] + (most[rows:] + rest[:rows]))


def w_arrange_kernel(w0, w_all):
    for b in range(NB):
        for q in range(NP):
            w_all[b, 4 * q : 4 * q + 4, :] = w0[q, :, b * BS : (b + 1) * BS]


def w1_update_kernel(own, w_all, mine, theirs, new, out):
    for b in range(NB):
        rows = owned(own[b], w_all[b], mine, theirs, b)
        new[b] = rows
        for q in range(NP):
            out[q, :, b * BS : (b + 1) * BS] = rows


def h2_update_kernel(table, h_all, mine, theirs, final, out, new):
    first = lax.axis_index("z4") == 0
    at = pl.ds(pl.multiple_of(8 * lax.axis_index(HALF), 8), 8)
    for b in range(NB):
        own = jnp.concatenate([h_all[0, b, at, :], h_all[1, b, at, :]], axis=1)
        rows = owned(own, whole_block(h_all, b), mine, theirs, b)
        new[b] = rows
        for high in range(2):
            pair = rows[4 * high : 4 * high + 4]
            final[2 * high : 2 * high + 2, b * BS : (b + 1) * BS] = jnp.where(first, pair[0:2], pair[2:4])
    for q in range(NH):
        for j in range(CAP):
            out[q, 8 * j : 8 * (j + 1), :] = new[table[q * CAP + j]]


def w2_collect_kernel(table, got, mine, out, total):
    gram_collect_kernel(table, got, total)
    first = lax.axis_index("zh") == 0
    low, high = total[:, 0:2, :], total[:, 2:4, :]
    mine[...] = jnp.where(first, low, high)
    out[...] = jnp.where(first, high, low)


def last_w_kernel(own, w_all, mine, theirs, final):
    first = lax.axis_index("zh") == 0
    for b in range(NB):
        rows = jnp.where(first, own[b, 0:2, :], own[b, 2:4, :])
        final[:, b * BS : (b + 1) * BS] = owned(rows, w_all[b], mine, theirs, b)


def call(body, scalars, arrays, outs, tables=(), scratch=(), counts=(), last=False, dtypes=None):
    smem = pl.BlockSpec(memory_space=pltpu.SMEM)
    vmem = pl.BlockSpec(memory_space=pltpu.VMEM)
    kind = jax.ShapeDtypeStruct if last else pltpu.VMEM
    return pl.pallas_call(
        body,
        in_specs=[smem] * len(scalars) + [vmem] * len(arrays),
        out_specs=[vmem] * len(outs) + [smem] * len(tables),
        out_shape=[kind(*s) for s in zip(outs, dtypes or [jnp.float32] * len(outs))] + [pltpu.SMEM(s, jnp.int32) for s in tables],
        scratch_shapes=[pltpu.VMEM(s, jnp.float32) for s in scratch] + [pltpu.SMEM((n,), jnp.int32) for n in counts],
    )(
        *(pltpu.with_memory_space_constraint(a, pltpu.SMEM) for a in scalars),
        *(pltpu.with_memory_space_constraint(a, pltpu.VMEM) for a in arrays),
    )


def per_device(blocks, observed, w_factor, h_factor):
    wide = NB * BS + TAB

    w_other = swap(w_factor, "zh")
    h_other = swap(h_factor, "z4")
    values, turned, w_mine, blk = call(
        prepare_kernel,
        (blocks[0, 0],),
        (observed[0, 0], w_factor),
        [(CAP, 2, BS, BS), (CAP, 2, BS, BS), w_factor.shape],
        dtypes=[jnp.bfloat16, jnp.bfloat16, jnp.float32],
        tables=[(2 * CAP,)],
    )
    (w_pair,) = call(w_pair_kernel, (blk,), (w_mine, w_other), [(NP, 4, wide)], scratch=[(4, wide)])
    w_pair, h_other = lax.optimization_barrier((w_pair, h_other))
    w_got = exchange(w_pair, PLANE)

    w_own, sent, rows = call(
        h1_terms_kernel,
        (blk,),
        (w_got, h_factor, h_other, values),
        [(NB, 4, BS), (392, COLS)],
        tables=[(NP * CAP,)],
        scratch=[(CAP, RANK, BS)],
    )
    pair = lax.all_gather(sent, "core", axis=0)
    (sent,) = call(h1_build_kernel, (), (pair,), [(NQ, 120, COLS)], counts=(2 * CAP,))
    got = exchange(sent, QUAD)
    mine, old, cols = call(h1_collect_kernel, (), (got,), [(96, COLS), (RANK, COLS)], tables=[(NH * CAP,)])
    theirs = swap(mine, "z4")
    (w_all,) = call(w_arrange_kernel, (), (w_got,), [(NB, RANK, BS)])
    (out,) = call(h1_update_kernel, (), (mine, theirs, old), [(NQ, RANK, COLS)])
    h_all = lax.all_gather(exchange(out, QUAD), "core", axis=0)

    wide = CAP * (BS + RANK)
    (sent,) = call(w1_terms_kernel, (blk,), (h_all, turned), [(NP, 4, wide)])
    got = exchange(sent, PLANE)
    (mine,) = call(gram_collect_kernel, (rows,), (got,), [(NB + 1, 4, BS)])
    theirs = swap(mine, "zh")
    w_own, out = call(w1_update_kernel, (), (w_own, w_all, mine, theirs), [(NB, 4, BS), (NP, 4, NB * BS)])
    w_got = exchange(out, PLANE)

    (sent,) = call(h2_terms_kernel, (blk,), (w_got, values), [(NH, 8, wide)], scratch=[(CAP, RANK, BS)])
    got = exchange(sent, HALF)
    (mine,) = call(gram_collect_kernel, (cols,), (got,), [(NB + 1, 8, BS)])
    theirs = swap(mine, "z4")
    (w_all,) = call(w_arrange_kernel, (), (w_got,), [(NB, RANK, BS)])
    h_final, out = call(
        h2_update_kernel, (cols,), (h_all, mine, theirs), [(4, NB * BS), (NH, 16, BS)], scratch=[(NB, 8, BS)]
    )
    h_got = exchange(out, HALF)

    (sent,) = call(w2_terms_kernel, (blk,), (h_got, turned), [(NP, 4, wide)])
    got = exchange(sent, PLANE)
    mine, out = call(w2_collect_kernel, (rows,), (got,), [(NB + 1, 2, BS), (NB + 1, 2, BS)], scratch=[(NB + 1, 4, BS)])
    theirs = swap(out, "zh")
    (w_final,) = call(last_w_kernel, (), (w_own, w_all, mine, theirs), [(2, NB * BS)], last=True)
    return w_final, h_final


def solution(mesh):
    fine = Mesh(mesh.devices.reshape(2, 2, 2, 2, 2, 4, 4), FINE)
    tex = ("z4",) + HALF
    smp = ("zh",) + PLANE
    in_specs = (P(tex, smp, None, None), P(tex, smp, None, None), P(smp, tex), P(tex, smp))
    out_specs = (P(smp, tex), P(tex, smp))
    return jax.shard_map(per_device, mesh=fine, in_specs=in_specs, out_specs=out_specs, check_vma=False)
```

```python
import jax
import jax.numpy as jnp
from jax import lax
from jax.experimental import pallas as pl
from jax.experimental.pallas import tpu as pltpu
from jax.sharding import Mesh, PartitionSpec as P


RANK = 64
BS = 256
CAP = 2
NB = 4
TAB = 128

FINE = ("z4", "z2", "z1", "core", "zh", "y", "x")
HALF = ("z2", "z1", "core")
QUAD = ("z2", "z1")
PLANE = ("y", "x")
NH = 8
NQ = 4
COLS = NB * BS // NH
NP = 16

NN = (((1,), (0,)), ((), ()))
NT = (((1,), (1,)), ((), ()))


def exchange(x, axes):
    return lax.all_to_all(x, axes, split_axis=0, concat_axis=0, tiled=True)


def swap(x, axis):
    return lax.ppermute(x, axis, [(0, 1), (1, 0)])


def halves(x):
    hi = x.astype(jnp.bfloat16)
    lo = (x - hi.astype(jnp.float32)).astype(jnp.bfloat16)
    return hi, lo


def product(a, b, dims=NN):
    dot = lambda x, y: lax.dot_general(x, y, dims, preferred_element_type=jnp.float32)
    return dot(a[0], b[0]) + (dot(a[0], b[1]) + dot(a[1], b[0]))


def grams(left, values, live):
    whole = halves(left)
    left = halves(left * live)
    return product(left, values), product(left, whole, NT)


def prepare_kernel(blk, values, w, parts, turned, w_mine, listed):
    for d in range(2):
        for j in range(CAP):
            listed[CAP * d + j] = blk[d, j]
    w_mine[...] = w[...]
    for j in range(CAP):
        block = values[j * BS : (j + 1) * BS, :]
        parts[j, 0], parts[j, 1] = halves(block)
        turned[j, 0], turned[j, 1] = halves(block.T)


def both_of(parts, j):
    return parts[j, 0], parts[j, 1]


def live_of(blk, j):
    return jnp.where(blk[j] >= 0, 1.0, 0.0).astype(jnp.float32)


def block_of(blk, d, j):
    return jnp.maximum(blk[CAP * d + j], 0)


def w_pair_kernel(mine, theirs, out):
    first = lax.axis_index("zh") == 0
    low = jnp.where(first, mine[...], theirs[...])
    high = jnp.where(first, theirs[...], mine[...])
    both = jnp.concatenate([low, high], axis=0)
    for q in range(NP):
        out[q] = both


def read_list(table, q, listed):
    for j in range(CAP):
        table[q * CAP + j] = jnp.maximum(listed[:, j : j + 1].astype(jnp.int32)[0, 0], 0)


def w_slot(w_got, j, blk, w_slots):
    at = pl.multiple_of(block_of(blk, 0, j) * BS, BS)
    for q in range(NP):
        w_slots[j, 4 * q : 4 * q + 4, :] = w_got[q, :, pl.ds(at, BS)]
    return w_slots[j]


def h1_terms_kernel(blk, w0, h, values, w_own, out, w_slots):
    for j in range(CAP):
        upper, gram = grams(w_slot(w0, j, blk, w_slots), both_of(values, j), live_of(blk, j))
        for side in range(2):
            at = 128 * j + RANK * side
            out[at : at + RANK, :] = upper[:, COLS * side : COLS * (side + 1)]
        out[256 + 32 * j : 288 + 32 * j, :] = jnp.concatenate([gram[:32], gram[32:]], axis=1)
    for q in range(NH):
        at = 320 + 16 * (q % 2) + 4 * (q // 2)
        out[at : at + 4, :] = h[:, COLS * q : COLS * (q + 1)]
    lane = lax.broadcasted_iota(jnp.int32, (8, COLS), 1)
    out[352:360, :] = jnp.where(lane == 0, blk[CAP], blk[CAP + 1]).astype(jnp.float32)
    plane = lax.axis_index(PLANE)
    for b in range(NB):
        w_own[b] = w0[plane, :, b * BS : (b + 1) * BS]


def h1_build_kernel(pair, out, lists):
    core = lax.axis_index("core")
    out[:, :96, :] = jnp.zeros((NQ, 96, COLS), jnp.float32)
    for i in range(2):
        read_list(lists, i, pair[i, 352:353, :])
        for j in range(CAP):
            q = lists[CAP * i + j]
            at = pl.multiple_of(128 * j + RANK * core, 8)
            out[q, :64, :] = out[q, :64, :] + pair[i, pl.ds(at, RANK), :]
            out[q, 64:96, :] = out[q, 64:96, :] + pair[i, 256 + 32 * j : 288 + 32 * j, :]
        side = pair[i, pl.ds(pl.multiple_of(320 + 16 * core, 8), 16), :]
        for q in range(NQ):
            out[q, 96 + 4 * i : 100 + 4 * i, :] = side[4 * q : 4 * q + 4]
            out[q, 104 + 4 * i : 108 + 4 * i, :] = pair[i, 352:356, :]


def h1_collect_kernel(got, out, cols):
    total = got[0, :96, :]
    for q in range(1, NQ):
        total = total + got[q, :96, :]
    out[:96, :] = total
    for q in range(NQ):
        out[96 + 8 * q : 104 + 8 * q, :] = got[q, 96:104, :]
        for i in range(2):
            read_list(cols, 2 * q + i, got[q, 104 + 4 * i : 105 + 4 * i, :])


def h1_update_kernel(mine, theirs, out):
    total = mine[:96, :] + theirs[:96, :]
    gram = jnp.concatenate([total[64:, :64], total[64:, 64:]], axis=0)
    first = lax.axis_index("z4") == 0
    low = jnp.where(first, mine[96:, :], theirs[96:, :])
    high = jnp.where(first, theirs[96:, :], mine[96:, :])
    pairs = []
    for k in range(16):
        pairs += [low[2 * k : 2 * k + 2], high[2 * k : 2 * k + 2]]
    old = jnp.concatenate(pairs, axis=0)
    new = old * total[:64] / product(halves(gram), halves(old))
    for q in range(NQ):
        out[q] = new


def whole_block(h_all, b):
    return jnp.concatenate([h_all[0, b], h_all[1, b]], axis=1)


def send_grams(out, terms):
    rows = out.shape[1]
    both = jnp.concatenate([gram for _, gram in terms], axis=1)
    for q in range(out.shape[0]):
        for j in range(CAP):
            out[q, :, BS * j : BS * (j + 1)] = terms[j][0][rows * q : rows * (q + 1), :]
        out[q, :, CAP * BS : CAP * (BS + RANK)] = both[rows * q : rows * (q + 1), :]


def w1_terms_kernel(blk, h_all, values, out):
    terms = []
    for j in range(CAP):
        h_slot = whole_block(h_all, block_of(blk, 1, j))
        terms.append(grams(h_slot, both_of(values, j), live_of(blk, j)))
    send_grams(out, terms)
    lane = lax.broadcasted_iota(jnp.int32, (4, TAB), 1)
    listed = jnp.where(lane == 0, blk[0], blk[1]).astype(jnp.float32)
    for q in range(NP):
        out[q, :, CAP * (BS + RANK) :] = listed


def w2_terms_kernel(blk, h_got, values, out):
    terms = []
    for j in range(CAP):
        h_slot = h_got[:, 8 * j : 8 * j + 8, :].reshape(RANK, BS)
        terms.append(grams(h_slot, both_of(values, j), live_of(blk, j)))
    send_grams(out, terms)


def h2_terms_kernel(blk, w_got, values, out, w_slots):
    terms = []
    for j in range(CAP):
        terms.append(grams(w_slot(w_got, j, blk, w_slots), both_of(values, j), live_of(blk, j)))
    send_grams(out, terms)


def gram_collect_kernel(table, got, out):
    rows = out.shape[1]
    out[...] = jnp.zeros(out.shape, out.dtype)
    half = lax.broadcasted_iota(jnp.int32, (rows, CAP * RANK), 1) // RANK
    for q in range(got.shape[0]):
        grams = got[q, :, CAP * BS : CAP * (BS + RANK)]
        turned = jnp.concatenate([grams[:, RANK:], grams[:, :RANK]], axis=1)
        for j in range(CAP):
            b = table[q * CAP + j]
            out[b] = out[b] + got[q, :, BS * j : BS * (j + 1)]
            side = b % 2
            at = pl.ds(pl.multiple_of(b // 2 * CAP * RANK, CAP * RANK), CAP * RANK)
            mine = jnp.where(side == j, grams, turned)
            out[NB, :, at] = out[NB, :, at] + jnp.where(half == side, mine, 0.0)


def w1_collect_kernel(got, out, rows):
    for q in range(NP):
        read_list(rows, q, got[q, 0:1, CAP * (BS + RANK) :])
    gram_collect_kernel(rows, got, out)


def owned(own, whole, mine, theirs, b):
    rows = own.shape[0]
    gram = mine[NB, :, RANK * b : RANK * (b + 1)] + theirs[NB, :, RANK * b : RANK * (b + 1)]
    high = gram.astype(jnp.bfloat16).astype(jnp.float32)
    gram = jnp.concatenate([high, gram - high], axis=0).astype(jnp.bfloat16)
    whole = halves(whole)
    most = lax.dot_general(gram, whole[0], NN, preferred_element_type=jnp.float32)
    rest = lax.dot_general(gram, whole[1], NN, preferred_element_type=jnp.float32)
    return own * (mine[b] + theirs[b]) / (most[:rows] + (most[rows:] + rest[:rows]))


def w_arrange_kernel(w0, w_all):
    for b in range(NB):
        for q in range(NP):
            w_all[b, 4 * q : 4 * q + 4, :] = w0[q, :, b * BS : (b + 1) * BS]


def w1_update_kernel(own, w_all, mine, theirs, new, out):
    for b in range(NB):
        rows = owned(own[b], w_all[b], mine, theirs, b)
        new[b] = rows
        for q in range(NP):
            out[q, :, b * BS : (b + 1) * BS] = rows


def h2_update_kernel(table, h_all, mine, theirs, final, out, new):
    first = lax.axis_index("z4") == 0
    at = pl.ds(pl.multiple_of(8 * lax.axis_index(HALF), 8), 8)
    for b in range(NB):
        own = jnp.concatenate([h_all[0, b, at, :], h_all[1, b, at, :]], axis=1)
        rows = owned(own, whole_block(h_all, b), mine, theirs, b)
        new[b] = rows
        for high in range(2):
            pair = rows[4 * high : 4 * high + 4]
            final[2 * high : 2 * high + 2, b * BS : (b + 1) * BS] = jnp.where(first, pair[0:2], pair[2:4])
    for q in range(NH):
        for j in range(CAP):
            out[q, 8 * j : 8 * (j + 1), :] = new[table[q * CAP + j]]


def w2_collect_kernel(table, got, mine, out, total):
    gram_collect_kernel(table, got, total)
    first = lax.axis_index("zh") == 0
    low, high = total[:, 0:2, :], total[:, 2:4, :]
    mine[...] = jnp.where(first, low, high)
    out[...] = jnp.where(first, high, low)


def last_w_kernel(own, w_all, mine, theirs, final):
    first = lax.axis_index("zh") == 0
    for b in range(NB):
        rows = jnp.where(first, own[b, 0:2, :], own[b, 2:4, :])
        final[:, b * BS : (b + 1) * BS] = owned(rows, w_all[b], mine, theirs, b)


def call(body, scalars, arrays, outs, tables=(), scratch=(), counts=(), last=False, dtypes=None):
    smem = pl.BlockSpec(memory_space=pltpu.SMEM)
    vmem = pl.BlockSpec(memory_space=pltpu.VMEM)
    kind = jax.ShapeDtypeStruct if last else pltpu.VMEM
    return pl.pallas_call(
        body,
        in_specs=[smem] * len(scalars) + [vmem] * len(arrays),
        out_specs=[vmem] * len(outs) + [smem] * len(tables),
        out_shape=[kind(*s) for s in zip(outs, dtypes or [jnp.float32] * len(outs))] + [pltpu.SMEM(s, jnp.int32) for s in tables],
        scratch_shapes=[pltpu.VMEM(s, jnp.float32) for s in scratch] + [pltpu.SMEM((n,), jnp.int32) for n in counts],
    )(
        *(pltpu.with_memory_space_constraint(a, pltpu.SMEM) for a in scalars),
        *(pltpu.with_memory_space_constraint(a, pltpu.VMEM) for a in arrays),
    )


def per_device(blocks, observed, w_factor, h_factor):
    w_other = swap(w_factor, "zh")
    values, turned, w_mine, blk = call(
        prepare_kernel,
        (blocks[0, 0],),
        (observed[0, 0], w_factor),
        [(CAP, 2, BS, BS), (CAP, 2, BS, BS), w_factor.shape],
        dtypes=[jnp.bfloat16, jnp.bfloat16, jnp.float32],
        tables=[(2 * CAP,)],
    )
    (w_pair,) = call(w_pair_kernel, (), (w_mine, w_other), [(NP, 4, NB * BS)])
    w_got = exchange(w_pair, PLANE)

    w_own, sent = call(
        h1_terms_kernel, (blk,), (w_got, h_factor, values), [(NB, 4, BS), (360, COLS)], scratch=[(CAP, RANK, BS)]
    )
    pair = lax.all_gather(sent, "core", axis=0)
    (sent,) = call(h1_build_kernel, (), (pair,), [(NQ, 112, COLS)], counts=(2 * CAP,))
    got = exchange(sent, QUAD)
    mine, cols = call(h1_collect_kernel, (), (got,), [(128, COLS)], tables=[(NH * CAP,)])
    theirs = swap(mine, "z4")
    (w_all,) = call(w_arrange_kernel, (), (w_got,), [(NB, RANK, BS)])
    (out,) = call(h1_update_kernel, (), (mine, theirs), [(NQ, RANK, COLS)])
    h_all = lax.all_gather(exchange(out, QUAD), "core", axis=0)

    wide = CAP * (BS + RANK)
    (sent,) = call(w1_terms_kernel, (blk,), (h_all, turned), [(NP, 4, wide + TAB)])
    got = exchange(sent, PLANE)
    mine, rows = call(w1_collect_kernel, (), (got,), [(NB + 1, 4, BS)], tables=[(NP * CAP,)])
    theirs = swap(mine, "zh")
    w_own, out = call(w1_update_kernel, (), (w_own, w_all, mine, theirs), [(NB, 4, BS), (NP, 4, NB * BS)])
    w_got = exchange(out, PLANE)

    (sent,) = call(h2_terms_kernel, (blk,), (w_got, values), [(NH, 8, wide)], scratch=[(CAP, RANK, BS)])
    got = exchange(sent, HALF)
    (mine,) = call(gram_collect_kernel, (cols,), (got,), [(NB + 1, 8, BS)])
    theirs = swap(mine, "z4")
    (w_all,) = call(w_arrange_kernel, (), (w_got,), [(NB, RANK, BS)])
    h_final, out = call(
        h2_update_kernel, (cols,), (h_all, mine, theirs), [(4, NB * BS), (NH, 16, BS)], scratch=[(NB, 8, BS)]
    )
    h_got = exchange(out, HALF)

    (sent,) = call(w2_terms_kernel, (blk,), (h_got, turned), [(NP, 4, wide)])
    got = exchange(sent, PLANE)
    mine, out = call(w2_collect_kernel, (rows,), (got,), [(NB + 1, 2, BS), (NB + 1, 2, BS)], scratch=[(NB + 1, 4, BS)])
    theirs = swap(out, "zh")
    (w_final,) = call(last_w_kernel, (), (w_own, w_all, mine, theirs), [(2, NB * BS)], last=True)
    return w_final, h_final


def solution(mesh):
    fine = Mesh(mesh.devices.reshape(2, 2, 2, 2, 2, 4, 4), FINE)
    tex = ("z4",) + HALF
    smp = ("zh",) + PLANE
    in_specs = (P(tex, smp, None, None), P(tex, smp, None, None), P(smp, tex), P(tex, smp))
    out_specs = (P(smp, tex), P(tex, smp))
    return jax.shard_map(per_device, mesh=fine, in_specs=in_specs, out_specs=out_specs, check_vma=False)
```

```python
import jax
import jax.numpy as jnp
from jax import lax
from jax.experimental import pallas as pl
from jax.experimental.pallas import tpu as pltpu
from jax.sharding import Mesh, PartitionSpec as P


RANK = 64
BS = 256
CAP = 2
NB = 4
TAB = 128

FINE = ("z4", "z2", "z1", "core", "zh", "y", "x")
HALF = ("z2", "z1", "core")
QUAD = ("z2", "z1")
PLANE = ("y", "x")
NH = 8
NQ = 4
COLS = NB * BS // NH
NP = 16

NN = (((1,), (0,)), ((), ()))
NT = (((1,), (1,)), ((), ()))


def exchange(x, axes):
    return lax.all_to_all(x, axes, split_axis=0, concat_axis=0, tiled=True)


def swap(x, axis):
    return lax.ppermute(x, axis, [(0, 1), (1, 0)])


def halves(x):
    hi = x.astype(jnp.bfloat16)
    lo = (x - hi.astype(jnp.float32)).astype(jnp.bfloat16)
    return hi, lo


def product(a, b, dims=NN):
    dot = lambda x, y: lax.dot_general(x, y, dims, preferred_element_type=jnp.float32)
    return dot(a[0], b[0]) + (dot(a[0], b[1]) + dot(a[1], b[0]))


def grams(left, values, live):
    whole = halves(left)
    left = halves(left * live)
    return product(left, values), product(left, whole, NT)


def packed(gram):
    parts = gram[:32, :32], gram[:32, 32:], gram[32:, 32:]
    rest = jnp.concatenate([p[24:] for p in parts], axis=0)
    return jnp.concatenate([p[:24] for p in parts] + [rest], axis=1)


def unpacked(rows):
    a, b, c = (
        jnp.concatenate([rows[:, 32 * i : 32 * i + 32], rows[8 * i : 8 * i + 8, 96:]], axis=0) for i in range(3)
    )
    return jnp.concatenate([jnp.concatenate([a, b], axis=1), jnp.concatenate([b.T, c], axis=1)], axis=0)


def prepare_kernel(blk, values, w, parts, turned, w_mine, listed):
    for d in range(2):
        for j in range(CAP):
            listed[CAP * d + j] = blk[d, j]
    w_mine[...] = w[...]
    for j in range(CAP):
        block = values[j * BS : (j + 1) * BS, :]
        parts[j, 0], parts[j, 1] = halves(block)
        turned[j, 0], turned[j, 1] = halves(block.T)


def both_of(parts, j):
    return parts[j, 0], parts[j, 1]


def live_of(blk, j):
    return jnp.where(blk[j] >= 0, 1.0, 0.0).astype(jnp.float32)


def block_of(blk, d, j):
    return jnp.maximum(blk[CAP * d + j], 0)


def w_pair_kernel(mine, theirs, out):
    first = lax.axis_index("zh") == 0
    low = jnp.where(first, mine[...], theirs[...])
    high = jnp.where(first, theirs[...], mine[...])
    both = jnp.concatenate([low, high], axis=0)
    for q in range(NP):
        out[q] = both


def read_list(table, q, listed):
    for j in range(CAP):
        table[q * CAP + j] = jnp.maximum(listed[:, j : j + 1].astype(jnp.int32)[0, 0], 0)


def w_slot(w_got, j, blk, w_slots):
    at = pl.multiple_of(block_of(blk, 0, j) * BS, BS)
    for q in range(NP):
        w_slots[j, 4 * q : 4 * q + 4, :] = w_got[q, :, pl.ds(at, BS)]
    return w_slots[j]


def h1_terms_kernel(blk, w0, h, values, w_own, out, w_slots):
    for j in range(CAP):
        upper, gram = grams(w_slot(w0, j, blk, w_slots), both_of(values, j), live_of(blk, j))
        for side in range(2):
            at = 128 * j + RANK * side
            out[at : at + RANK, :] = upper[:, COLS * side : COLS * (side + 1)]
        out[256 + 24 * j : 280 + 24 * j, :] = packed(gram)
    for q in range(NH):
        at = 304 + 16 * (q % 2) + 4 * (q // 2)
        out[at : at + 4, :] = h[:, COLS * q : COLS * (q + 1)]
    lane = lax.broadcasted_iota(jnp.int32, (8, COLS), 1)
    out[336:344, :] = jnp.where(lane == 0, blk[CAP], blk[CAP + 1]).astype(jnp.float32)
    plane = lax.axis_index(PLANE)
    for b in range(NB):
        w_own[b] = w0[plane, :, b * BS : (b + 1) * BS]


def h1_build_kernel(pair, out, lists):
    core = lax.axis_index("core")
    out[:, :88, :] = jnp.zeros((NQ, 88, COLS), jnp.float32)
    for i in range(2):
        read_list(lists, i, pair[i, 336:337, :])
        for j in range(CAP):
            q = lists[CAP * i + j]
            at = pl.multiple_of(128 * j + RANK * core, 8)
            out[q, :64, :] = out[q, :64, :] + pair[i, pl.ds(at, RANK), :]
            out[q, 64:88, :] = out[q, 64:88, :] + pair[i, 256 + 24 * j : 280 + 24 * j, :]
        side = pair[i, pl.ds(pl.multiple_of(304 + 16 * core, 8), 16), :]
        for q in range(NQ):
            out[q, 88 + 4 * i : 92 + 4 * i, :] = side[4 * q : 4 * q + 4]
            out[q, 96 + 4 * i : 100 + 4 * i, :] = pair[i, 336:340, :]


def h1_collect_kernel(got, out, cols):
    total = got[0, :88, :]
    for q in range(1, NQ):
        total = total + got[q, :88, :]
    out[:88, :] = total
    for q in range(NQ):
        out[88 + 8 * q : 96 + 8 * q, :] = got[q, 88:96, :]
        for i in range(2):
            read_list(cols, 2 * q + i, got[q, 96 + 4 * i : 97 + 4 * i, :])


def h1_update_kernel(mine, theirs, out):
    total = mine[:88, :] + theirs[:88, :]
    gram = unpacked(total[64:])
    first = lax.axis_index("z4") == 0
    low = jnp.where(first, mine[88:, :], theirs[88:, :])
    high = jnp.where(first, theirs[88:, :], mine[88:, :])
    pairs = []
    for k in range(16):
        pairs += [low[2 * k : 2 * k + 2], high[2 * k : 2 * k + 2]]
    old = jnp.concatenate(pairs, axis=0)
    new = old * total[:64] / product(halves(gram), halves(old))
    for q in range(NQ):
        out[q] = new


def whole_block(h_all, b):
    return jnp.concatenate([h_all[0, b], h_all[1, b]], axis=1)


def send_grams(out, terms):
    rows = out.shape[1]
    both = jnp.concatenate([gram for _, gram in terms], axis=1)
    for q in range(out.shape[0]):
        for j in range(CAP):
            out[q, :, BS * j : BS * (j + 1)] = terms[j][0][rows * q : rows * (q + 1), :]
        out[q, :, CAP * BS : CAP * (BS + RANK)] = both[rows * q : rows * (q + 1), :]


def w1_terms_kernel(blk, h_all, values, out):
    terms = []
    for j in range(CAP):
        h_slot = whole_block(h_all, block_of(blk, 1, j))
        terms.append(grams(h_slot, both_of(values, j), live_of(blk, j)))
    send_grams(out, terms)
    lane = lax.broadcasted_iota(jnp.int32, (4, TAB), 1)
    listed = jnp.where(lane == 0, blk[0], blk[1]).astype(jnp.float32)
    for q in range(NP):
        out[q, :, CAP * (BS + RANK) :] = listed


def w2_terms_kernel(blk, h_got, values, out):
    terms = []
    for j in range(CAP):
        h_slot = h_got[:, 8 * j : 8 * j + 8, :].reshape(RANK, BS)
        terms.append(grams(h_slot, both_of(values, j), live_of(blk, j)))
    send_grams(out, terms)


def h2_terms_kernel(blk, w_got, values, out, w_slots):
    terms = []
    for j in range(CAP):
        terms.append(grams(w_slot(w_got, j, blk, w_slots), both_of(values, j), live_of(blk, j)))
    send_grams(out, terms)


def gram_collect_kernel(table, got, out):
    rows = out.shape[1]
    out[...] = jnp.zeros(out.shape, out.dtype)
    half = lax.broadcasted_iota(jnp.int32, (rows, CAP * RANK), 1) // RANK
    for q in range(got.shape[0]):
        grams = got[q, :, CAP * BS : CAP * (BS + RANK)]
        turned = jnp.concatenate([grams[:, RANK:], grams[:, :RANK]], axis=1)
        for j in range(CAP):
            b = table[q * CAP + j]
            out[b] = out[b] + got[q, :, BS * j : BS * (j + 1)]
            side = b % 2
            at = pl.ds(pl.multiple_of(b // 2 * CAP * RANK, CAP * RANK), CAP * RANK)
            mine = jnp.where(side == j, grams, turned)
            out[NB, :, at] = out[NB, :, at] + jnp.where(half == side, mine, 0.0)


def w1_collect_kernel(got, out, rows):
    for q in range(NP):
        read_list(rows, q, got[q, 0:1, CAP * (BS + RANK) :])
    gram_collect_kernel(rows, got, out)


def owned(own, whole, mine, theirs, b):
    rows = own.shape[0]
    gram = mine[NB, :, RANK * b : RANK * (b + 1)] + theirs[NB, :, RANK * b : RANK * (b + 1)]
    high = gram.astype(jnp.bfloat16).astype(jnp.float32)
    gram = jnp.concatenate([high, gram - high], axis=0).astype(jnp.bfloat16)
    whole = halves(whole)
    most = lax.dot_general(gram, whole[0], NN, preferred_element_type=jnp.float32)
    rest = lax.dot_general(gram, whole[1], NN, preferred_element_type=jnp.float32)
    return own * (mine[b] + theirs[b]) / (most[:rows] + (most[rows:] + rest[:rows]))


def w_arrange_kernel(w0, w_all):
    for b in range(NB):
        for q in range(NP):
            w_all[b, 4 * q : 4 * q + 4, :] = w0[q, :, b * BS : (b + 1) * BS]


def w1_update_kernel(own, w_all, mine, theirs, new, out):
    for b in range(NB):
        rows = owned(own[b], w_all[b], mine, theirs, b)
        new[b] = rows
        for q in range(NP):
            out[q, :, b * BS : (b + 1) * BS] = rows


def h2_update_kernel(table, h_all, mine, theirs, final, out, new):
    first = lax.axis_index("z4") == 0
    at = pl.ds(pl.multiple_of(8 * lax.axis_index(HALF), 8), 8)
    for b in range(NB):
        own = jnp.concatenate([h_all[0, b, at, :], h_all[1, b, at, :]], axis=1)
        rows = owned(own, whole_block(h_all, b), mine, theirs, b)
        new[b] = rows
        for high in range(2):
            pair = rows[4 * high : 4 * high + 4]
            final[2 * high : 2 * high + 2, b * BS : (b + 1) * BS] = jnp.where(first, pair[0:2], pair[2:4])
    for q in range(NH):
        for j in range(CAP):
            out[q, 8 * j : 8 * (j + 1), :] = new[table[q * CAP + j]]


def w2_collect_kernel(table, got, mine, out, total):
    gram_collect_kernel(table, got, total)
    first = lax.axis_index("zh") == 0
    low, high = total[:, 0:2, :], total[:, 2:4, :]
    mine[...] = jnp.where(first, low, high)
    out[...] = jnp.where(first, high, low)


def last_w_kernel(own, w_all, mine, theirs, final):
    first = lax.axis_index("zh") == 0
    for b in range(NB):
        rows = jnp.where(first, own[b, 0:2, :], own[b, 2:4, :])
        final[:, b * BS : (b + 1) * BS] = owned(rows, w_all[b], mine, theirs, b)


def call(body, scalars, arrays, outs, tables=(), scratch=(), counts=(), last=False, dtypes=None):
    smem = pl.BlockSpec(memory_space=pltpu.SMEM)
    vmem = pl.BlockSpec(memory_space=pltpu.VMEM)
    kind = jax.ShapeDtypeStruct if last else pltpu.VMEM
    return pl.pallas_call(
        body,
        in_specs=[smem] * len(scalars) + [vmem] * len(arrays),
        out_specs=[vmem] * len(outs) + [smem] * len(tables),
        out_shape=[kind(*s) for s in zip(outs, dtypes or [jnp.float32] * len(outs))] + [pltpu.SMEM(s, jnp.int32) for s in tables],
        scratch_shapes=[pltpu.VMEM(s, jnp.float32) for s in scratch] + [pltpu.SMEM((n,), jnp.int32) for n in counts],
    )(
        *(pltpu.with_memory_space_constraint(a, pltpu.SMEM) for a in scalars),
        *(pltpu.with_memory_space_constraint(a, pltpu.VMEM) for a in arrays),
    )


def per_device(blocks, observed, w_factor, h_factor):
    w_other = swap(w_factor, "zh")
    values, turned, w_mine, blk = call(
        prepare_kernel,
        (blocks[0, 0],),
        (observed[0, 0], w_factor),
        [(CAP, 2, BS, BS), (CAP, 2, BS, BS), w_factor.shape],
        dtypes=[jnp.bfloat16, jnp.bfloat16, jnp.float32],
        tables=[(2 * CAP,)],
    )
    (w_pair,) = call(w_pair_kernel, (), (w_mine, w_other), [(NP, 4, NB * BS)])
    w_got = exchange(w_pair, PLANE)

    w_own, sent = call(
        h1_terms_kernel, (blk,), (w_got, h_factor, values), [(NB, 4, BS), (344, COLS)], scratch=[(CAP, RANK, BS)]
    )
    pair = lax.all_gather(sent, "core", axis=0)
    (sent,) = call(h1_build_kernel, (), (pair,), [(NQ, 104, COLS)], counts=(2 * CAP,))
    got = exchange(sent, QUAD)
    mine, cols = call(h1_collect_kernel, (), (got,), [(120, COLS)], tables=[(NH * CAP,)])
    theirs = swap(mine, "z4")
    (w_all,) = call(w_arrange_kernel, (), (w_got,), [(NB, RANK, BS)])
    (out,) = call(h1_update_kernel, (), (mine, theirs), [(NQ, RANK, COLS)])
    h_all = lax.all_gather(exchange(out, QUAD), "core", axis=0)

    wide = CAP * (BS + RANK)
    (sent,) = call(w1_terms_kernel, (blk,), (h_all, turned), [(NP, 4, wide + TAB)])
    got = exchange(sent, PLANE)
    mine, rows = call(w1_collect_kernel, (), (got,), [(NB + 1, 4, BS)], tables=[(NP * CAP,)])
    theirs = swap(mine, "zh")
    w_own, out = call(w1_update_kernel, (), (w_own, w_all, mine, theirs), [(NB, 4, BS), (NP, 4, NB * BS)])
    w_got = exchange(out, PLANE)

    (sent,) = call(h2_terms_kernel, (blk,), (w_got, values), [(NH, 8, wide)], scratch=[(CAP, RANK, BS)])
    got = exchange(sent, HALF)
    (mine,) = call(gram_collect_kernel, (cols,), (got,), [(NB + 1, 8, BS)])
    theirs = swap(mine, "z4")
    (w_all,) = call(w_arrange_kernel, (), (w_got,), [(NB, RANK, BS)])
    h_final, out = call(
        h2_update_kernel, (cols,), (h_all, mine, theirs), [(4, NB * BS), (NH, 16, BS)], scratch=[(NB, 8, BS)]
    )
    h_got = exchange(out, HALF)

    (sent,) = call(w2_terms_kernel, (blk,), (h_got, turned), [(NP, 4, wide)])
    got = exchange(sent, PLANE)
    mine, out = call(w2_collect_kernel, (rows,), (got,), [(NB + 1, 2, BS), (NB + 1, 2, BS)], scratch=[(NB + 1, 4, BS)])
    theirs = swap(out, "zh")
    (w_final,) = call(last_w_kernel, (), (w_own, w_all, mine, theirs), [(2, NB * BS)], last=True)
    return w_final, h_final


def solution(mesh):
    fine = Mesh(mesh.devices.reshape(2, 2, 2, 2, 2, 4, 4), FINE)
    tex = ("z4",) + HALF
    smp = ("zh",) + PLANE
    in_specs = (P(tex, smp, None, None), P(tex, smp, None, None), P(smp, tex), P(tex, smp))
    out_specs = (P(smp, tex), P(tex, smp))
    return jax.shard_map(per_device, mesh=fine, in_specs=in_specs, out_specs=out_specs, check_vma=False)
```

```python
import jax
import jax.numpy as jnp
from jax import lax
from jax.experimental import pallas as pl
from jax.experimental.pallas import tpu as pltpu
from jax.sharding import Mesh, PartitionSpec as P


RANK = 64
BS = 256
CAP = 2
NB = 4
TAB = 128

FINE = ("z4", "z2", "z1", "core", "zh", "y", "x")
HALF = ("z2", "z1", "core")
QUAD = ("z2", "z1")
PLANE = ("y", "x")
NH = 8
NQ = 4
COLS = NB * BS // NH
NP = 16

NN = (((1,), (0,)), ((), ()))
NT = (((1,), (1,)), ((), ()))


def exchange(x, axes):
    return lax.all_to_all(x, axes, split_axis=0, concat_axis=0, tiled=True)


def swap(x, axis):
    return lax.ppermute(x, axis, [(0, 1), (1, 0)])


def halves(x):
    hi = x.astype(jnp.bfloat16)
    lo = (x - hi.astype(jnp.float32)).astype(jnp.bfloat16)
    return hi, lo


def product(a, b, dims=NN):
    dot = lambda x, y: lax.dot_general(x, y, dims, preferred_element_type=jnp.float32)
    return dot(a[0], b[0]) + (dot(a[0], b[1]) + dot(a[1], b[0]))


def grams(left, values, live):
    whole = halves(left)
    left = halves(left * live)
    return product(left, values), product(left, whole, NT)


def packed(gram):
    parts = gram[:32, :32], gram[:32, 32:], gram[32:, 32:]
    rest = jnp.concatenate([p[24:] for p in parts], axis=0)
    return jnp.concatenate([p[:24] for p in parts] + [rest], axis=1)


def unpacked(rows):
    a, b, c = (
        jnp.concatenate([rows[:, 32 * i : 32 * i + 32], rows[8 * i : 8 * i + 8, 96:]], axis=0) for i in range(3)
    )
    return jnp.concatenate([jnp.concatenate([a, b], axis=1), jnp.concatenate([b.T, c], axis=1)], axis=0)


def prepare_kernel(blk, values, w, parts, turned, w_mine, listed):
    for d in range(2):
        for j in range(CAP):
            listed[CAP * d + j] = blk[d, j]
    w_mine[...] = w[...]
    for j in range(CAP):
        block = values[j * BS : (j + 1) * BS, :]
        parts[j, 0], parts[j, 1] = halves(block)
        turned[j, 0], turned[j, 1] = halves(block.T)


def both_of(parts, j):
    return parts[j, 0], parts[j, 1]


def live_of(blk, j):
    return jnp.where(blk[j] >= 0, 1.0, 0.0).astype(jnp.float32)


def block_of(blk, d, j):
    return jnp.maximum(blk[CAP * d + j], 0)


def w_pair_kernel(mine, theirs, out):
    first = lax.axis_index("zh") == 0
    low = jnp.where(first, mine[...], theirs[...])
    high = jnp.where(first, theirs[...], mine[...])
    both = jnp.concatenate([low, high], axis=0)
    for q in range(NP):
        out[q] = both


def read_list(table, q, listed):
    for j in range(CAP):
        table[q * CAP + j] = jnp.maximum(listed[:, j : j + 1].astype(jnp.int32)[0, 0], 0)


def w_slot(w_got, j, blk, w_slots):
    at = pl.multiple_of(block_of(blk, 0, j) * BS, BS)
    for q in range(NP):
        w_slots[j, 4 * q : 4 * q + 4, :] = w_got[q, :, pl.ds(at, BS)]
    return w_slots[j]


def h1_terms_kernel(blk, w0, h, values, w_own, out, w_slots):
    for j in range(CAP):
        upper, gram = grams(w_slot(w0, j, blk, w_slots), both_of(values, j), live_of(blk, j))
        for side in range(2):
            at = 128 * j + RANK * side
            out[at : at + RANK, :] = upper[:, COLS * side : COLS * (side + 1)]
        out[256 + 24 * j : 280 + 24 * j, :] = packed(gram)
    for q in range(NH):
        at = 304 + 16 * (q % 2) + 4 * (q // 2)
        out[at : at + 4, :] = h[:, COLS * q : COLS * (q + 1)]
    lane = lax.broadcasted_iota(jnp.int32, (8, COLS), 1)
    out[336:344, :] = jnp.where(lane == 0, blk[CAP], blk[CAP + 1]).astype(jnp.float32)
    plane = lax.axis_index(PLANE)
    for b in range(NB):
        w_own[b] = w0[plane, :, b * BS : (b + 1) * BS]


def h1_build_kernel(pair, out, lists):
    core = lax.axis_index("core")
    out[:, :88, :] = jnp.zeros((NQ, 88, COLS), jnp.float32)
    for i in range(2):
        read_list(lists, i, pair[i, 336:337, :])
        for j in range(CAP):
            q = lists[CAP * i + j]
            at = pl.multiple_of(128 * j + RANK * core, 8)
            out[q, :64, :] = out[q, :64, :] + pair[i, pl.ds(at, RANK), :]
            out[q, 64:88, :] = out[q, 64:88, :] + pair[i, 256 + 24 * j : 280 + 24 * j, :]
        side = pair[i, pl.ds(pl.multiple_of(304 + 16 * core, 8), 16), :]
        for q in range(NQ):
            out[q, 88 + 4 * i : 92 + 4 * i, :] = side[4 * q : 4 * q + 4]
            out[q, 96 + 4 * i : 100 + 4 * i, :] = pair[i, 336:340, :]


def h1_collect_kernel(got, out, cols):
    total = got[0, :88, :]
    for q in range(1, NQ):
        total = total + got[q, :88, :]
    out[:88, :] = total
    for q in range(NQ):
        out[88 + 8 * q : 96 + 8 * q, :] = got[q, 88:96, :]
        for i in range(2):
            read_list(cols, 2 * q + i, got[q, 96 + 4 * i : 97 + 4 * i, :])


def h1_update_kernel(mine, theirs, out):
    total = mine[:88, :] + theirs[:88, :]
    gram = unpacked(total[64:])
    first = lax.axis_index("z4") == 0
    low = jnp.where(first, mine[88:, :], theirs[88:, :])
    high = jnp.where(first, theirs[88:, :], mine[88:, :])
    pairs = []
    for k in range(16):
        pairs += [low[2 * k : 2 * k + 2], high[2 * k : 2 * k + 2]]
    old = jnp.concatenate(pairs, axis=0)
    new = old * total[:64] / product(halves(gram), halves(old))
    for q in range(NQ):
        out[q] = new


def whole_block(h_all, b):
    return jnp.concatenate([h_all[0, b], h_all[1, b]], axis=1)


def send_grams(out, terms):
    rows = out.shape[1]
    both = jnp.concatenate([gram for _, gram in terms], axis=1)
    for q in range(out.shape[0]):
        for j in range(CAP):
            out[q, :, BS * j : BS * (j + 1)] = terms[j][0][rows * q : rows * (q + 1), :]
        out[q, :, CAP * BS : CAP * (BS + RANK)] = both[rows * q : rows * (q + 1), :]


def w1_terms_kernel(blk, h_all, values, out):
    terms = []
    for j in range(CAP):
        h_slot = whole_block(h_all, block_of(blk, 1, j))
        terms.append(grams(h_slot, both_of(values, j), live_of(blk, j)))
    send_grams(out, terms)
    lane = lax.broadcasted_iota(jnp.int32, (4, TAB), 1)
    listed = jnp.where(lane == 0, blk[0], blk[1]).astype(jnp.float32)
    for q in range(NP):
        out[q, :, CAP * (BS + RANK) :] = listed


def w2_terms_kernel(blk, h_got, values, out):
    terms = []
    for j in range(CAP):
        h_slot = h_got[:, 8 * j : 8 * j + 8, :].reshape(RANK, BS)
        terms.append(grams(h_slot, both_of(values, j), live_of(blk, j)))
    send_grams(out, terms)


def h2_terms_kernel(blk, w_got, values, out, w_slots):
    terms = []
    for j in range(CAP):
        terms.append(grams(w_slot(w_got, j, blk, w_slots), both_of(values, j), live_of(blk, j)))
    send_grams(out, terms)


def gram_collect_kernel(table, got, out):
    rows = out.shape[1]
    out[...] = jnp.zeros(out.shape, out.dtype)
    half = lax.broadcasted_iota(jnp.int32, (rows, CAP * RANK), 1) // RANK
    for q in range(got.shape[0]):
        grams = got[q, :, CAP * BS : CAP * (BS + RANK)]
        turned = jnp.concatenate([grams[:, RANK:], grams[:, :RANK]], axis=1)
        for j in range(CAP):
            b = table[q * CAP + j]
            out[b] = out[b] + got[q, :, BS * j : BS * (j + 1)]
            side = b % 2
            at = pl.ds(pl.multiple_of(b // 2 * CAP * RANK, CAP * RANK), CAP * RANK)
            mine = jnp.where(side == j, grams, turned)
            out[NB, :, at] = out[NB, :, at] + jnp.where(half == side, mine, 0.0)


def w1_collect_kernel(got, out, rows):
    for q in range(NP):
        read_list(rows, q, got[q, 0:1, CAP * (BS + RANK) :])
    gram_collect_kernel(rows, got, out)


def owned(own, whole, mine, theirs, b):
    rows = own.shape[0]
    gram = mine[NB, :, RANK * b : RANK * (b + 1)] + theirs[NB, :, RANK * b : RANK * (b + 1)]
    high = gram.astype(jnp.bfloat16).astype(jnp.float32)
    gram = jnp.concatenate([high, gram - high], axis=0).astype(jnp.bfloat16)
    most = lax.dot_general(gram, whole[0], NN, preferred_element_type=jnp.float32)
    rest = lax.dot_general(gram, whole[1], NN, preferred_element_type=jnp.float32)
    return own * (mine[b] + theirs[b]) / (most[:rows] + (most[rows:] + rest[:rows]))


def w_arrange_kernel(w0, w_all, block):
    for b in range(NB):
        for q in range(NP):
            block[4 * q : 4 * q + 4, :] = w0[q, :, b * BS : (b + 1) * BS]
        w_all[b, 0], w_all[b, 1] = halves(block[...])


def h_arrange_kernel(h_all, h_parts):
    for b in range(NB):
        h_parts[b, 0], h_parts[b, 1] = halves(whole_block(h_all, b))


def w1_update_kernel(own, w_all, mine, theirs, new, out):
    for b in range(NB):
        rows = owned(own[b], both_of(w_all, b), mine, theirs, b)
        new[b] = rows
        for q in range(NP):
            out[q, :, b * BS : (b + 1) * BS] = rows


def h2_update_kernel(table, h_all, h_parts, mine, theirs, final, out, new):
    first = lax.axis_index("z4") == 0
    at = pl.ds(pl.multiple_of(8 * lax.axis_index(HALF), 8), 8)
    for b in range(NB):
        own = jnp.concatenate([h_all[0, b, at, :], h_all[1, b, at, :]], axis=1)
        rows = owned(own, both_of(h_parts, b), mine, theirs, b)
        new[b] = rows
        for high in range(2):
            pair = rows[4 * high : 4 * high + 4]
            final[2 * high : 2 * high + 2, b * BS : (b + 1) * BS] = jnp.where(first, pair[0:2], pair[2:4])
    for q in range(NH):
        for j in range(CAP):
            out[q, 8 * j : 8 * (j + 1), :] = new[table[q * CAP + j]]


def w2_collect_kernel(table, got, mine, out, total):
    gram_collect_kernel(table, got, total)
    first = lax.axis_index("zh") == 0
    low, high = total[:, 0:2, :], total[:, 2:4, :]
    mine[...] = jnp.where(first, low, high)
    out[...] = jnp.where(first, high, low)


def last_w_kernel(own, w_all, mine, theirs, final):
    first = lax.axis_index("zh") == 0
    for b in range(NB):
        rows = jnp.where(first, own[b, 0:2, :], own[b, 2:4, :])
        final[:, b * BS : (b + 1) * BS] = owned(rows, both_of(w_all, b), mine, theirs, b)


def call(body, scalars, arrays, outs, tables=(), scratch=(), counts=(), last=False, dtypes=None):
    smem = pl.BlockSpec(memory_space=pltpu.SMEM)
    vmem = pl.BlockSpec(memory_space=pltpu.VMEM)
    kind = jax.ShapeDtypeStruct if last else pltpu.VMEM
    return pl.pallas_call(
        body,
        in_specs=[smem] * len(scalars) + [vmem] * len(arrays),
        out_specs=[vmem] * len(outs) + [smem] * len(tables),
        out_shape=[kind(*s) for s in zip(outs, dtypes or [jnp.float32] * len(outs))] + [pltpu.SMEM(s, jnp.int32) for s in tables],
        scratch_shapes=[pltpu.VMEM(s, jnp.float32) for s in scratch] + [pltpu.SMEM((n,), jnp.int32) for n in counts],
    )(
        *(pltpu.with_memory_space_constraint(a, pltpu.SMEM) for a in scalars),
        *(pltpu.with_memory_space_constraint(a, pltpu.VMEM) for a in arrays),
    )


def arranged(body, factor, scratch=()):
    return call(body, (), (factor,), [(NB, 2, RANK, BS)], scratch=scratch, dtypes=[jnp.bfloat16])


def per_device(blocks, observed, w_factor, h_factor):
    w_other = swap(w_factor, "zh")
    values, turned, w_mine, blk = call(
        prepare_kernel,
        (blocks[0, 0],),
        (observed[0, 0], w_factor),
        [(CAP, 2, BS, BS), (CAP, 2, BS, BS), w_factor.shape],
        dtypes=[jnp.bfloat16, jnp.bfloat16, jnp.float32],
        tables=[(2 * CAP,)],
    )
    (w_pair,) = call(w_pair_kernel, (), (w_mine, w_other), [(NP, 4, NB * BS)])
    w_got = exchange(w_pair, PLANE)

    w_own, sent = call(
        h1_terms_kernel, (blk,), (w_got, h_factor, values), [(NB, 4, BS), (344, COLS)], scratch=[(CAP, RANK, BS)]
    )
    pair = lax.all_gather(sent, "core", axis=0)
    (sent,) = call(h1_build_kernel, (), (pair,), [(NQ, 104, COLS)], counts=(2 * CAP,))
    got = exchange(sent, QUAD)
    mine, cols = call(h1_collect_kernel, (), (got,), [(120, COLS)], tables=[(NH * CAP,)])
    theirs = swap(mine, "z4")
    (w_all,) = arranged(w_arrange_kernel, w_got, scratch=[(RANK, BS)])
    (out,) = call(h1_update_kernel, (), (mine, theirs), [(NQ, RANK, COLS)])
    h_all = lax.all_gather(exchange(out, QUAD), "core", axis=0)

    wide = CAP * (BS + RANK)
    (sent,) = call(w1_terms_kernel, (blk,), (h_all, turned), [(NP, 4, wide + TAB)])
    got = exchange(sent, PLANE)
    mine, rows = call(w1_collect_kernel, (), (got,), [(NB + 1, 4, BS)], tables=[(NP * CAP,)])
    theirs = swap(mine, "zh")
    (h_parts,) = arranged(h_arrange_kernel, h_all)
    w_own, out = call(w1_update_kernel, (), (w_own, w_all, mine, theirs), [(NB, 4, BS), (NP, 4, NB * BS)])
    w_got = exchange(out, PLANE)

    (sent,) = call(h2_terms_kernel, (blk,), (w_got, values), [(NH, 8, wide)], scratch=[(CAP, RANK, BS)])
    got = exchange(sent, HALF)
    (mine,) = call(gram_collect_kernel, (cols,), (got,), [(NB + 1, 8, BS)])
    theirs = swap(mine, "z4")
    (w_all,) = arranged(w_arrange_kernel, w_got, scratch=[(RANK, BS)])
    h_final, out = call(
        h2_update_kernel, (cols,), (h_all, h_parts, mine, theirs), [(4, NB * BS), (NH, 16, BS)], scratch=[(NB, 8, BS)]
    )
    h_got = exchange(out, HALF)

    (sent,) = call(w2_terms_kernel, (blk,), (h_got, turned), [(NP, 4, wide)])
    got = exchange(sent, PLANE)
    mine, out = call(w2_collect_kernel, (rows,), (got,), [(NB + 1, 2, BS), (NB + 1, 2, BS)], scratch=[(NB + 1, 4, BS)])
    theirs = swap(out, "zh")
    (w_final,) = call(last_w_kernel, (), (w_own, w_all, mine, theirs), [(2, NB * BS)], last=True)
    return w_final, h_final


def solution(mesh):
    fine = Mesh(mesh.devices.reshape(2, 2, 2, 2, 2, 4, 4), FINE)
    tex = ("z4",) + HALF
    smp = ("zh",) + PLANE
    in_specs = (P(tex, smp, None, None), P(tex, smp, None, None), P(smp, tex), P(tex, smp))
    out_specs = (P(smp, tex), P(tex, smp))
    return jax.shard_map(per_device, mesh=fine, in_specs=in_specs, out_specs=out_specs, check_vma=False)
```

```python
import jax
import jax.numpy as jnp
from jax import lax
from jax.experimental import pallas as pl
from jax.experimental.pallas import tpu as pltpu
from jax.sharding import Mesh, PartitionSpec as P


RANK = 64
BS = 256
CAP = 2
NB = 4
TAB = 128

FINE = ("z4", "z2", "z1", "core", "zh", "y", "x")
HALF = ("z2", "z1", "core")
QUAD = ("z2", "z1")
PLANE = ("y", "x")
NH = 8
NQ = 4
COLS = NB * BS // NH
NP = 16

NN = (((1,), (0,)), ((), ()))
NT = (((1,), (1,)), ((), ()))


def exchange(x, axes):
    return lax.all_to_all(x, axes, split_axis=0, concat_axis=0, tiled=True)


def swap(x, axis):
    return lax.ppermute(x, axis, [(0, 1), (1, 0)])


def halves(x):
    hi = x.astype(jnp.bfloat16)
    lo = (x - hi.astype(jnp.float32)).astype(jnp.bfloat16)
    return hi, lo


def product(a, b, dims=NN):
    dot = lambda x, y: lax.dot_general(x, y, dims, preferred_element_type=jnp.float32)
    return dot(a[0], b[0]) + (dot(a[0], b[1]) + dot(a[1], b[0]))


def grams(left, values, live):
    whole = halves(left)
    left = halves(left * live)
    return product(left, values), product(left, whole, NT)


def packed(gram):
    parts = gram[:32, :32], gram[:32, 32:], gram[32:, 32:]
    rest = jnp.concatenate([p[24:] for p in parts], axis=0)
    return jnp.concatenate([p[:24] for p in parts] + [rest], axis=1)


def unpacked(rows):
    a, b, c = (
        jnp.concatenate([rows[:, 32 * i : 32 * i + 32], rows[8 * i : 8 * i + 8, 96:]], axis=0) for i in range(3)
    )
    return jnp.concatenate([jnp.concatenate([a, b], axis=1), jnp.concatenate([b.T, c], axis=1)], axis=0)


def prepare_kernel(blk, values, w, parts, turned, w_mine, listed):
    for d in range(2):
        for j in range(CAP):
            listed[CAP * d + j] = blk[d, j]
    w_mine[...] = w[...]
    for j in range(CAP):
        block = values[j * BS : (j + 1) * BS, :]
        parts[j, 0], parts[j, 1] = halves(block)
        turned[j, 0], turned[j, 1] = halves(block.T)


def both_of(parts, j):
    return parts[j, 0], parts[j, 1]


def live_of(blk, j):
    return jnp.where(blk[j] >= 0, 1.0, 0.0).astype(jnp.float32)


def block_of(blk, d, j):
    return jnp.maximum(blk[CAP * d + j], 0)


def w_pair_kernel(mine, theirs, out):
    first = lax.axis_index("zh") == 0
    low = jnp.where(first, mine[...], theirs[...])
    high = jnp.where(first, theirs[...], mine[...])
    both = jnp.concatenate([low, high], axis=0)
    for q in range(NP):
        out[q] = both


def read_list(table, q, listed):
    for j in range(CAP):
        table[q * CAP + j] = jnp.maximum(listed[:, j : j + 1].astype(jnp.int32)[0, 0], 0)


def w_slot(w_got, j, blk, w_slots):
    at = pl.multiple_of(block_of(blk, 0, j) * BS, BS)
    for q in range(NP):
        w_slots[j, 4 * q : 4 * q + 4, :] = w_got[q, :, pl.ds(at, BS)]
    return w_slots[j]


def h1_terms_kernel(blk, w0, h, values, w_own, out, w_slots):
    for j in range(CAP):
        upper, gram = grams(w_slot(w0, j, blk, w_slots), both_of(values, j), live_of(blk, j))
        for side in range(2):
            at = 128 * j + RANK * side
            out[at : at + RANK, :] = upper[:, COLS * side : COLS * (side + 1)]
        out[256 + 24 * j : 280 + 24 * j, :] = packed(gram)
    for q in range(NH):
        at = 304 + 16 * (q % 2) + 4 * (q // 2)
        out[at : at + 4, :] = h[:, COLS * q : COLS * (q + 1)]
    lane = lax.broadcasted_iota(jnp.int32, (8, COLS), 1)
    out[336:344, :] = jnp.where(lane == 0, blk[CAP], blk[CAP + 1]).astype(jnp.float32)
    plane = lax.axis_index(PLANE)
    for b in range(NB):
        w_own[b] = w0[plane, :, b * BS : (b + 1) * BS]


def h1_build_kernel(pair, out, lists):
    core = lax.axis_index("core")
    out[:, :88, :] = jnp.zeros((NQ, 88, COLS), jnp.float32)
    for i in range(2):
        read_list(lists, i, pair[i, 336:337, :])
        for j in range(CAP):
            q = lists[CAP * i + j]
            at = pl.multiple_of(128 * j + RANK * core, 8)
            out[q, :64, :] = out[q, :64, :] + pair[i, pl.ds(at, RANK), :]
            out[q, 64:88, :] = out[q, 64:88, :] + pair[i, 256 + 24 * j : 280 + 24 * j, :]
        side = pair[i, pl.ds(pl.multiple_of(304 + 16 * core, 8), 16), :]
        for q in range(NQ):
            out[q, 88 + 4 * i : 92 + 4 * i, :] = side[4 * q : 4 * q + 4]
            out[q, 96 + 4 * i : 100 + 4 * i, :] = pair[i, 336:340, :]


def h1_collect_kernel(got, out):
    total = got[0, :88, :]
    for q in range(1, NQ):
        total = total + got[q, :88, :]
    out[:88, :] = total
    for q in range(NQ):
        out[88 + 8 * q : 96 + 8 * q, :] = got[q, 88:96, :]


def h1_lists_kernel(w0, got, w_all, cols):
    w_arrange_kernel(w0, w_all)
    for q in range(NQ):
        for i in range(2):
            read_list(cols, 2 * q + i, got[q, 96 + 4 * i : 97 + 4 * i, :])


def h1_update_kernel(mine, theirs, out):
    total = mine[:88, :] + theirs[:88, :]
    gram = unpacked(total[64:])
    first = lax.axis_index("z4") == 0
    low = jnp.where(first, mine[88:, :], theirs[88:, :])
    high = jnp.where(first, theirs[88:, :], mine[88:, :])
    pairs = []
    for k in range(16):
        pairs += [low[2 * k : 2 * k + 2], high[2 * k : 2 * k + 2]]
    old = jnp.concatenate(pairs, axis=0)
    new = old * total[:64] / product(halves(gram), halves(old))
    for q in range(NQ):
        out[q] = new


def whole_block(h_all, b):
    return jnp.concatenate([h_all[0, b], h_all[1, b]], axis=1)


def send_grams(out, terms):
    rows = out.shape[1]
    both = jnp.concatenate([gram for _, gram in terms], axis=1)
    for q in range(out.shape[0]):
        for j in range(CAP):
            out[q, :, BS * j : BS * (j + 1)] = terms[j][0][rows * q : rows * (q + 1), :]
        out[q, :, CAP * BS : CAP * (BS + RANK)] = both[rows * q : rows * (q + 1), :]


def w1_terms_kernel(blk, h_all, values, out):
    terms = []
    for j in range(CAP):
        h_slot = whole_block(h_all, block_of(blk, 1, j))
        terms.append(grams(h_slot, both_of(values, j), live_of(blk, j)))
    send_grams(out, terms)
    lane = lax.broadcasted_iota(jnp.int32, (4, TAB), 1)
    listed = jnp.where(lane == 0, blk[0], blk[1]).astype(jnp.float32)
    for q in range(NP):
        out[q, :, CAP * (BS + RANK) :] = listed


def w2_terms_kernel(blk, h_got, values, out):
    terms = []
    for j in range(CAP):
        h_slot = h_got[:, 8 * j : 8 * j + 8, :].reshape(RANK, BS)
        terms.append(grams(h_slot, both_of(values, j), live_of(blk, j)))
    send_grams(out, terms)


def h2_terms_kernel(blk, w_got, values, out, w_slots):
    terms = []
    for j in range(CAP):
        terms.append(grams(w_slot(w_got, j, blk, w_slots), both_of(values, j), live_of(blk, j)))
    send_grams(out, terms)


def gram_collect_kernel(table, got, out):
    rows = out.shape[1]
    out[...] = jnp.zeros(out.shape, out.dtype)
    half = lax.broadcasted_iota(jnp.int32, (rows, CAP * RANK), 1) // RANK
    for q in range(got.shape[0]):
        grams = got[q, :, CAP * BS : CAP * (BS + RANK)]
        turned = jnp.concatenate([grams[:, RANK:], grams[:, :RANK]], axis=1)
        for j in range(CAP):
            b = table[q * CAP + j]
            out[b] = out[b] + got[q, :, BS * j : BS * (j + 1)]
            side = b % 2
            at = pl.ds(pl.multiple_of(b // 2 * CAP * RANK, CAP * RANK), CAP * RANK)
            mine = jnp.where(side == j, grams, turned)
            out[NB, :, at] = out[NB, :, at] + jnp.where(half == side, mine, 0.0)


def w1_collect_kernel(got, out, rows):
    for q in range(NP):
        read_list(rows, q, got[q, 0:1, CAP * (BS + RANK) :])
    gram_collect_kernel(rows, got, out)


def owned(own, whole, mine, theirs, b):
    rows = own.shape[0]
    gram = mine[NB, :, RANK * b : RANK * (b + 1)] + theirs[NB, :, RANK * b : RANK * (b + 1)]
    high = gram.astype(jnp.bfloat16).astype(jnp.float32)
    gram = jnp.concatenate([high, gram - high], axis=0).astype(jnp.bfloat16)
    whole = halves(whole)
    most = lax.dot_general(gram, whole[0], NN, preferred_element_type=jnp.float32)
    rest = lax.dot_general(gram, whole[1], NN, preferred_element_type=jnp.float32)
    return own * (mine[b] + theirs[b]) / (most[:rows] + (most[rows:] + rest[:rows]))


def w_arrange_kernel(w0, w_all):
    for b in range(NB):
        for q in range(NP):
            w_all[b, 4 * q : 4 * q + 4, :] = w0[q, :, b * BS : (b + 1) * BS]


def w1_update_kernel(own, w_all, mine, theirs, new, out):
    for b in range(NB):
        rows = owned(own[b], w_all[b], mine, theirs, b)
        new[b] = rows
        for q in range(NP):
            out[q, :, b * BS : (b + 1) * BS] = rows


def h2_update_kernel(table, h_all, mine, theirs, final, out, new):
    first = lax.axis_index("z4") == 0
    at = pl.ds(pl.multiple_of(8 * lax.axis_index(HALF), 8), 8)
    for b in range(NB):
        own = jnp.concatenate([h_all[0, b, at, :], h_all[1, b, at, :]], axis=1)
        rows = owned(own, whole_block(h_all, b), mine, theirs, b)
        new[b] = rows
        for high in range(2):
            pair = rows[4 * high : 4 * high + 4]
            final[2 * high : 2 * high + 2, b * BS : (b + 1) * BS] = jnp.where(first, pair[0:2], pair[2:4])
    for q in range(NH):
        for j in range(CAP):
            out[q, 8 * j : 8 * (j + 1), :] = new[table[q * CAP + j]]


def w2_collect_kernel(table, got, mine, out, total):
    gram_collect_kernel(table, got, total)
    first = lax.axis_index("zh") == 0
    low, high = total[:, 0:2, :], total[:, 2:4, :]
    mine[...] = jnp.where(first, low, high)
    out[...] = jnp.where(first, high, low)


def last_w_kernel(own, w_all, mine, theirs, final):
    first = lax.axis_index("zh") == 0
    for b in range(NB):
        rows = jnp.where(first, own[b, 0:2, :], own[b, 2:4, :])
        final[:, b * BS : (b + 1) * BS] = owned(rows, w_all[b], mine, theirs, b)


def call(body, scalars, arrays, outs, tables=(), scratch=(), counts=(), last=False, dtypes=None):
    smem = pl.BlockSpec(memory_space=pltpu.SMEM)
    vmem = pl.BlockSpec(memory_space=pltpu.VMEM)
    kind = jax.ShapeDtypeStruct if last else pltpu.VMEM
    return pl.pallas_call(
        body,
        in_specs=[smem] * len(scalars) + [vmem] * len(arrays),
        out_specs=[vmem] * len(outs) + [smem] * len(tables),
        out_shape=[kind(*s) for s in zip(outs, dtypes or [jnp.float32] * len(outs))] + [pltpu.SMEM(s, jnp.int32) for s in tables],
        scratch_shapes=[pltpu.VMEM(s, jnp.float32) for s in scratch] + [pltpu.SMEM((n,), jnp.int32) for n in counts],
    )(
        *(pltpu.with_memory_space_constraint(a, pltpu.SMEM) for a in scalars),
        *(pltpu.with_memory_space_constraint(a, pltpu.VMEM) for a in arrays),
    )


def per_device(blocks, observed, w_factor, h_factor):
    w_other = swap(w_factor, "zh")
    values, turned, w_mine, blk = call(
        prepare_kernel,
        (blocks[0, 0],),
        (observed[0, 0], w_factor),
        [(CAP, 2, BS, BS), (CAP, 2, BS, BS), w_factor.shape],
        dtypes=[jnp.bfloat16, jnp.bfloat16, jnp.float32],
        tables=[(2 * CAP,)],
    )
    (w_pair,) = call(w_pair_kernel, (), (w_mine, w_other), [(NP, 4, NB * BS)])
    w_got = exchange(w_pair, PLANE)

    w_own, sent = call(
        h1_terms_kernel, (blk,), (w_got, h_factor, values), [(NB, 4, BS), (344, COLS)], scratch=[(CAP, RANK, BS)]
    )
    pair = lax.all_gather(sent, "core", axis=0)
    (sent,) = call(h1_build_kernel, (), (pair,), [(NQ, 104, COLS)], counts=(2 * CAP,))
    got = exchange(sent, QUAD)
    (mine,) = call(h1_collect_kernel, (), (got,), [(120, COLS)])
    theirs = swap(mine, "z4")
    w_all, cols = call(h1_lists_kernel, (), (w_got, got), [(NB, RANK, BS)], tables=[(NH * CAP,)])
    (out,) = call(h1_update_kernel, (), (mine, theirs), [(NQ, RANK, COLS)])
    h_all = lax.all_gather(exchange(out, QUAD), "core", axis=0)

    wide = CAP * (BS + RANK)
    (sent,) = call(w1_terms_kernel, (blk,), (h_all, turned), [(NP, 4, wide + TAB)])
    got = exchange(sent, PLANE)
    mine, rows = call(w1_collect_kernel, (), (got,), [(NB + 1, 4, BS)], tables=[(NP * CAP,)])
    theirs = swap(mine, "zh")
    w_own, out = call(w1_update_kernel, (), (w_own, w_all, mine, theirs), [(NB, 4, BS), (NP, 4, NB * BS)])
    w_got = exchange(out, PLANE)

    (sent,) = call(h2_terms_kernel, (blk,), (w_got, values), [(NH, 8, wide)], scratch=[(CAP, RANK, BS)])
    got = exchange(sent, HALF)
    (mine,) = call(gram_collect_kernel, (cols,), (got,), [(NB + 1, 8, BS)])
    theirs = swap(mine, "z4")
    (w_all,) = call(w_arrange_kernel, (), (w_got,), [(NB, RANK, BS)])
    h_final, out = call(
        h2_update_kernel, (cols,), (h_all, mine, theirs), [(4, NB * BS), (NH, 16, BS)], scratch=[(NB, 8, BS)]
    )
    h_got = exchange(out, HALF)

    (sent,) = call(w2_terms_kernel, (blk,), (h_got, turned), [(NP, 4, wide)])
    got = exchange(sent, PLANE)
    mine, out = call(w2_collect_kernel, (rows,), (got,), [(NB + 1, 2, BS), (NB + 1, 2, BS)], scratch=[(NB + 1, 4, BS)])
    theirs = swap(out, "zh")
    (w_final,) = call(last_w_kernel, (), (w_own, w_all, mine, theirs), [(2, NB * BS)], last=True)
    return w_final, h_final


def solution(mesh):
    fine = Mesh(mesh.devices.reshape(2, 2, 2, 2, 2, 4, 4), FINE)
    tex = ("z4",) + HALF
    smp = ("zh",) + PLANE
    in_specs = (P(tex, smp, None, None), P(tex, smp, None, None), P(smp, tex), P(tex, smp))
    out_specs = (P(smp, tex), P(tex, smp))
    return jax.shard_map(per_device, mesh=fine, in_specs=in_specs, out_specs=out_specs, check_vma=False)
```
